128 devices in a mesh: gx: 16 (over z, x), yz: 8 (over y, core).
Axes of the slice: x: 4, y: 4, z: 4, core: 2. Of those that a mesh axis runs over, the one named last changes fastest.
Arguments:
- state: float32 [4, 512, 384, 256], P(None, 'gx', 'yz'), may hold values from -6 to 6
- mean_flow: float32 [512, 384, 256], P('gx', 'yz'), may hold values from 0.2 to 1.2
- face_cell: int32 [24576], P(('gx', 'yz')), may hold values from 0 to 50331647, as said below
- face_normal: float32 [3, 24576], P(None, ('gx', 'yz')), may hold values from -3 to 3
- face_pos: float32 [3, 24576], P(None, ('gx', 'yz')), may hold values from -2 to 2
- observer_pos: float32 [3, 512], replicated, may hold values from 4 to 12
- time_bin: int32 [24576, 512], P(('gx', 'yz')), may hold values from 0 to 63
Outputs:
- state_next: float32 [4, 512, 384, 256], P(None, 'gx', 'yz')
- signal: float32 [512, 64], P(('gx', 'yz'))
The draws below stay inside these ranges and needn't reach their ends.
Inputs may be any that keep to these rules, and one draw needn't show every extreme that they name: `face_cell`: face j is held by device j // 192 of gx+yz, and its cell, numbered (x 384 + y) * 256 + z, lies in that device's block of grid cells.
All inputs are finite; a program needn't handle non-finite values.
Results may differ from the reference program's by a relative error of at most 0.000084.
Values sent between devices are 32-bit elements; how exact they have to be, the bound alone decides.
A program may use at most 192 MiB of HBM per device.

```python
import jax
import jax.numpy as jnp
from jax import lax

CX = 32
CY = 48
NZ = 256
FACES_DEV = 192
OBS = 512
BINS = 64
NX = 512
NY = 384
FACES = 24576
N_YZ = 8


def draw_face_cell(key, part):
    faces = jnp.arange(FACES, dtype=jnp.int32)
    device = faces // FACES_DEV
    column = device // N_YZ
    group = device % N_YZ
    key_x, key_y, key_z = jax.random.split(key, 3)
    along_x = jax.random.randint(key_x, (FACES,), 0, CX, dtype=jnp.int32)
    along_y = jax.random.randint(key_y, (FACES,), 0, CY, dtype=jnp.int32)
    along_z = jax.random.randint(key_z, (FACES,), 0, NZ, dtype=jnp.int32)
    cell = ((column * CX + along_x) * (CY * N_YZ) + group * CY + along_y) * NZ + along_z
    return cell.astype(jnp.int32)


def with_ends(entries, own_key, least, top_value):
    spot = [jax.random.randint(jax.random.fold_in(own_key, axis), (), 0, length) for axis, length in enumerate(entries.shape)]
    main_axis = entries.shape.index(max(entries.shape))
    beside = spot[:main_axis] + [(spot[main_axis] + 1) % entries.shape[main_axis]] + spot[main_axis + 1:]
    return entries.at[tuple(spot)].set(least).at[tuple(beside)].set(top_value)


def block_scale(stream_key, shape, pieces, least, high):
    loudness = 1.0
    for dim, shards_of in pieces:
        heights = jax.random.uniform(jax.random.fold_in(jax.random.fold_in(stream_key, 6), dim), (shards_of,), jnp.float32, least / len(pieces), high / len(pieces))
        loudness = loudness * jnp.repeat(jnp.exp(heights), shape[dim] // shards_of).reshape((-1,) + (1,) * (len(shape) - 1 - dim))
    return loudness


def bell_draw(own_key, extent, width, limit, shards=(), kind=jnp.bfloat16):
    factor_of = block_scale(own_key, extent, shards, -0.22, 0.18) if shards else 1.0
    array = jax.random.normal(own_key, extent, jnp.float32) * width * factor_of
    return jnp.minimum(jnp.maximum(array, -limit), limit).astype(kind)


def setup_inputs(seed: int = 0) -> dict:
    key_list = jax.random.split(jax.random.key(seed), 8)
    state = bell_draw(key_list[0], (4, NX, NY, NZ), 1.0, 6.0, ((1, 16), (2, 8)), jnp.float32)
    mean_flow = jnp.clip(0.2 + 1 * jax.random.uniform(key_list[1], (NX, NY, NZ), jnp.float32) ** block_scale(key_list[1], (NX, NY, NZ), ((0, 16), (1, 8)), -0.2, 0.2), 0.2, 1.2)
    face_cell = draw_face_cell(jax.random.fold_in(key_list[7], 71), 0)
    face_normal = jnp.clip(jax.random.uniform(key_list[3], (3, FACES), jnp.float32, -3.0, 3.0) * block_scale(key_list[3], (3, FACES), ((1, 128),), -0.4, 0.0), -3.0, 3.0)
    face_pos = jnp.clip(jax.random.uniform(key_list[4], (3, FACES), jnp.float32, -2.0, 2.0) * block_scale(key_list[4], (3, FACES), ((1, 128),), -0.4, 0.0), -2.0, 2.0)
    observer_pos = jnp.clip(jax.random.uniform(key_list[5], (3, OBS), jnp.float32, 4.0, 12.0), 4.0, 12.0)
    time_bin = with_ends(jax.random.randint(key_list[6], (FACES, OBS), 0, BINS), jax.random.fold_in(key_list[6], 1), 0, BINS - 1).astype(jnp.int32)
    return dict(state=state, mean_flow=mean_flow, face_cell=face_cell, face_normal=face_normal, face_pos=face_pos, observer_pos=observer_pos, time_bin=time_bin)


time_step = 0.25
four_pi = 4.0 * 3.141592653589793

def diagonals(count, dtype):
    index = jnp.arange(count)
    third = jnp.full((count,), 1.0 / 3.0, dtype)
    quarter = jnp.asarray(0.25, dtype)
    lower = jnp.where(index == 1, quarter, third)
    lower = jnp.where(index == count - 2, quarter, lower)
    lower = jnp.where(index == count - 1, jnp.asarray(2.0, dtype), lower)
    lower = jnp.where(index == 0, jnp.asarray(0.0, dtype), lower)
    upper = jnp.where(index == 1, quarter, third)
    upper = jnp.where(index == count - 2, quarter, upper)
    upper = jnp.where(index == 0, jnp.asarray(2.0, dtype), upper)
    upper = jnp.where(index == count - 1, jnp.asarray(0.0, dtype), upper)
    return (lower, jnp.ones((count,), dtype), upper)

def compact_rhs(field, axis):
    count = field.shape[axis]
    widths = [(2, 2) if dimension == axis else (0, 0) for dimension in range(field.ndim)]
    padded = jnp.pad(field, widths)

    def take(first, last):
        return lax.slice_in_dim(padded, first, last, axis=axis)

    def plane(index):
        return lax.slice_in_dim(field, index, index + 1, axis=axis)
    inner = 7.0 / 9.0 * (take(3, count + 3) - take(1, count + 1)) + 1.0 / 36.0 * (take(4, count + 4) - take(0, count))
    first_row = 0.5 * (4.0 * plane(1) + plane(2) - 5.0 * plane(0))
    second_row = 0.75 * (plane(2) - plane(0))
    before_last = 0.75 * (plane(count - 1) - plane(count - 3))
    last_row = 0.5 * (5.0 * plane(count - 1) - 4.0 * plane(count - 2) - plane(count - 3))
    middle_rows = lax.slice_in_dim(inner, 2, count - 2, axis=axis)
    return jnp.concatenate([first_row, second_row, middle_rows, before_last, last_row], axis)

def compact_derivative(field, axis):
    moved = jnp.moveaxis(compact_rhs(field, axis), axis, 0)
    count = moved.shape[0]
    lower, middle, upper = diagonals(count, field.dtype)
    solved = lax.linalg.tridiagonal_solve(lower, middle, upper, moved.reshape(count, -1))
    return jnp.moveaxis(solved.reshape(moved.shape), 0, axis)

def explicit_y(field):
    count = field.shape[1]
    padded = jnp.pad(field, ((0, 0), (3, 3), (0, 0)))

    def take(shift):
        return padded[:, 3 + shift:3 + shift + count]
    return 0.75 * (take(1) - take(-1)) - 0.15 * (take(2) - take(-2)) + 1.0 / 60.0 * (take(3) - take(-3))

def reference(state, mean_flow, face_cell, face_normal, face_pos, observer_pos, time_bin):
    pressure, stream, lateral, vertical = (state[0], state[1], state[2], state[3])
    pressure_x = compact_derivative(pressure, 0)
    stream_x = compact_derivative(stream, 0)
    lateral_x = compact_derivative(lateral, 0)
    vertical_x = compact_derivative(vertical, 0)
    mean_x = compact_derivative(mean_flow, 0)
    pressure_y = explicit_y(pressure)
    lateral_y = explicit_y(lateral)
    mean_y = explicit_y(mean_flow)
    pressure_z = compact_derivative(pressure, 2)
    vertical_z = compact_derivative(vertical, 2)
    mean_z = compact_derivative(mean_flow, 2)
    pressure_rate = -(mean_flow * pressure_x + stream_x + lateral_y + vertical_z)
    stream_rate = -(mean_flow * stream_x + stream * mean_x + lateral * mean_y + vertical * mean_z + pressure_x)
    lateral_rate = -(mean_flow * lateral_x + pressure_y)
    vertical_rate = -(mean_flow * vertical_x + pressure_z)
    rates = jnp.stack([pressure_rate, stream_rate, lateral_rate, vertical_rate])
    state_next = state + time_step * rates
    face_rates = rates.reshape(4, -1)[:, face_cell]
    face_pressure = state_next[0].reshape(-1)[face_cell]
    normal_rate = face_normal[0] * face_rates[1] + face_normal[1] * face_rates[2] + face_normal[2] * face_rates[3]
    offset_x = observer_pos[0][None, :] - face_pos[0][:, None]
    offset_y = observer_pos[1][None, :] - face_pos[1][:, None]
    offset_z = observer_pos[2][None, :] - face_pos[2][:, None]
    distance = jnp.sqrt(offset_x * offset_x + offset_y * offset_y + offset_z * offset_z)
    normal_r = (face_normal[0][:, None] * offset_x + face_normal[1][:, None] * offset_y + face_normal[2][:, None] * offset_z) / distance
    contribution = (normal_rate[:, None] + (face_rates[0][:, None] + face_pressure[:, None] / distance) * normal_r) / (four_pi * distance)
    slots = jnp.arange(OBS, dtype=jnp.int32)[None, :] * BINS + time_bin
    signal = jnp.zeros((OBS * BINS,), contribution.dtype).at[slots.reshape(-1)].add(contribution.reshape(-1))
    return (state_next, signal.reshape(OBS, BINS))
```

```python
import functools

import jax
import jax.numpy as jnp
import numpy as np
from jax import lax
from jax.experimental import pallas as pl
from jax.experimental.pallas import tpu as pltpu
from jax.sharding import PartitionSpec as P

CX, CY, NZ = 32, 48, 256
FACES_DEV, OBS, BINS = 192, 512, 64
N_GX, N_YZ = 16, 8
TIME_STEP = 0.25
INV_FOUR_PI = 1.0 / (4.0 * 3.141592653589793)
MESH = pl.DeviceIdType.MESH
F32, BF16 = jnp.float32, jnp.bfloat16

LAM = (-1.0 + np.sqrt(1.0 - 4.0 / 9.0)) / (2.0 / 3.0)
CC, DD = 25.0 / 12.0, -1.0 / 12.0
CL = CC * LAM
KK = DD / CL


def operator(n):
    a = np.eye(n)
    b = np.zeros((n, n))
    for i in range(n):
        if i == 0:
            a[0, 1] = 2.0
            b[0, :3] = (-2.5, 2.0, 0.5)
        elif i == n - 1:
            a[i, i - 1] = 2.0
            b[i, n - 3 :] = (-0.5, -2.0, 2.5)
        elif i in (1, n - 2):
            a[i, i - 1] = a[i, i + 1] = 0.25
            b[i, i + 1], b[i, i - 1] = 0.75, -0.75
        else:
            a[i, i - 1] = a[i, i + 1] = 1.0 / 3.0
            b[i, i + 1], b[i, i - 1] = 7.0 / 9.0, -7.0 / 9.0
            b[i, i + 2], b[i, i - 2] = 1.0 / 36.0, -1.0 / 36.0
    return np.linalg.solve(a, b)


def closure(n, total):
    lag = np.arange(n)[:, None] - np.arange(n)[None, :]
    inside = np.where(
        lag == 0, 0.0, np.sign(lag) * (CC * LAM ** np.abs(lag) + DD * (np.abs(lag) == 1))
    )
    rest = operator(total)[:n, :n] - inside
    factors = np.stack([CC * LAM ** (np.arange(n) + 1.0), DD * (np.arange(n) == 0)], 1)
    return np.linalg.lstsq(factors, rest, rcond=None)[0]


def split2(x):
    hi = x.astype(BF16)
    return hi, (x - hi.astype(F32)).astype(BF16)


def dot3(a, b):
    return (
        jnp.dot(a[0], b[0], preferred_element_type=F32)
        + jnp.dot(a[1], b[0], preferred_element_type=F32)
        + jnp.dot(a[0], b[1], preferred_element_type=F32)
    )


def kernel(
    ends, state, mean, face_cell, normal, pos, obs, tbin, dz, table, table_s_in,
    nxt, sig,
    fld, grd, hal, tsum, stg, geo, tbp, face_v, normal_v, pos_v, obs_v, tbin_v, dz_v, table_v,
    rows_v, binned, packed, recv_a, send_b, recv_b, table_s, cell_s,
    ld_sem, in_sem, xs_sem, xr_sem, ys_sem, yr_sem, as_sem, ar_sem, bs_sem, br_sem,
):
    gx = lax.axis_index("gx")
    yz = lax.axis_index("yz")

    order = (0, 2, 4, 1, 3)
    loads = {}
    for f in order:
        src = mean if f == 4 else state.at[f]
        for t in range(2):
            c = pltpu.make_async_copy(
                src.at[:, :, pl.ds(128 * t, 128)], fld.at[f, :, t, pl.ds(8, CY), :], ld_sem.at[f, t]
            )
            c.start()
            loads[f, t] = c
    small = []
    for k, (s, d) in enumerate((
        (dz, dz_v), (table, table_v), (table_s_in, table_s), (face_cell, cell_s),
        (face_cell, face_v), (normal, normal_v), (pos, pos_v), (obs, obs_v), (tbin, tbin_v),
    )):
        c = pltpu.make_async_copy(s, d, in_sem.at[k])
        c.start()
        small.append(c)

    barrier = pltpu.get_barrier_semaphore()
    for k in range(1, N_GX):
        pl.semaphore_signal(barrier, inc=1, device_id=(lax.rem(gx + k, N_GX), yz), device_id_type=MESH)
    for k in range(1, N_YZ):
        pl.semaphore_signal(barrier, inc=1, device_id=(gx, lax.rem(yz + k, N_YZ)), device_id_type=MESH)
    pl.semaphore_wait(barrier, N_GX + N_YZ - 2)

    has_left, has_right = gx > 0, gx < N_GX - 1
    has_low, has_high = yz > 0, yz < N_YZ - 1
    right, left = (lax.rem(gx + 1, N_GX), yz), (lax.rem(gx + N_GX - 1, N_GX), yz)
    high, low = (gx, lax.rem(yz + 1, N_YZ)), (gx, lax.rem(yz + N_YZ - 1, N_YZ))

    def xcopy(src, dst, way, k):
        return pltpu.make_async_remote_copy(
            src_ref=src, dst_ref=dst, send_sem=xs_sem.at[way, k], recv_sem=xr_sem.at[way, k],
            device_id=(right, left)[way], device_id_type=MESH,
        )

    xc = ([], [])
    for way, plane in ((0, CX - 1), (1, 0)):
        xc[way].append(xcopy(state.at[:, plane], hal.at[pl.ds(0, 4), 2 + way], way, 0))
        xc[way].append(xcopy(mean.at[plane], hal.at[4, 2 + way], way, 1))
        for f in range(5):
            xc[way].append(xcopy(tsum.at[way, f], hal.at[f, way], way, 2 + f))
    sends = (has_right, has_left)
    gets = (has_left, has_right)
    for way in range(2):
        @pl.when(sends[way])
        def _():
            xc[way][0].start()
            xc[way][1].start()

    yc = ([], [])
    for k, f in enumerate((0, 2, 4)):
        for way, (first, there) in enumerate(((8 + CY - 3, 5), (8, 8 + CY))):
            yc[way].append(pltpu.make_async_remote_copy(
                src_ref=fld.at[f, :, :, pl.ds(first, 3), :], dst_ref=fld.at[f, :, :, pl.ds(there, 3), :],
                send_sem=ys_sem.at[way, k], recv_sem=yr_sem.at[way, k],
                device_id=(high, low)[way], device_id_type=MESH,
            ))
    ysends = (has_high, has_low)
    ygets = (has_low, has_high)

    for n_done, f in enumerate(order):
        loads[f, 0].wait()
        loads[f, 1].wait()
        if f in (0, 2, 4):
            for way in range(2):
                @pl.when(ysends[way])
                def _():
                    yc[way][f // 2].start()

        def sweep(t, _):
            zero = jnp.zeros((CY, 128), F32)
            acc, edge = zero, zero
            for i in range(CX):
                grd[f, i, t] = edge
                v = fld[f, i, t, pl.ds(8, CY), :]
                acc = LAM * acc + v
                edge = acc + KK * v
            tsum[0, f, :, pl.ds(pl.multiple_of(128 * t, 128), 128)] = acc
            acc, edge = zero, zero
            for i in reversed(range(CX)):
                grd[f, i, t] = CL * (grd[f, i, t] - edge)
                v = fld[f, i, t, pl.ds(8, CY), :]
                acc = LAM * acc + v
                edge = acc + KK * v
            tsum[1, f, :, pl.ds(pl.multiple_of(128 * t, 128), 128)] = acc
            return 0

        lax.fori_loop(0, 2, sweep, 0)
        for way in range(2):
            @pl.when(sends[way])
            def _():
                xc[way][2 + f].start()

    for way, there in ((0, jnp.logical_not(has_left)), (1, jnp.logical_not(has_right))):
        @pl.when(there)
        def _():
            def close(n, _):
                f, t = n // 2, n % 2
                one = jnp.zeros((CY, 128), F32)
                two = jnp.zeros((CY, 128), F32)
                for i in range(CX):
                    v = fld[f, i if way == 0 else CX - 1 - i, t, pl.ds(8, CY), :]
                    one = one + float(ends[0, i]) * v
                    two = two + float(ends[1, i]) * v
                lanes = pl.ds(pl.multiple_of(128 * t, 128), 128)
                hal[f, way, :, lanes] = one
                hal[f, 2 + way, :, lanes] = two
                return 0

            lax.fori_loop(0, 10, close, 0)
    for way, there, row in ((0, jnp.logical_not(has_low), 5), (1, jnp.logical_not(has_high), 8 + CY)):
        @pl.when(there)
        def _():
            for f in (0, 2, 4):
                fld[f, :, :, pl.ds(row, 3), :] = jnp.zeros((CX, 2, 3, 128), F32)

    for c in small:
        c.wait()
    for way in range(2):
        @pl.when(ygets[way])
        def _():
            for k in range(3):
                yc[way][k].wait_recv()

    dz_hi, dz_lo = dz_v[0], dz_v[1]
    step = 4

    def local(n, _):
        x0 = n * step
        zs = []
        for f in (0, 3, 4):
            v = fld[f, pl.ds(x0, step), :, pl.ds(8, CY), :]
            v = jnp.concatenate([v[:, 0], v[:, 1]], axis=-1).reshape(step * CY, NZ)
            zs.append(dot3(split2(v), (dz_hi, dz_lo)))
        for j in range(step):
            for t in range(2):
                x = x0 + j
                at = lambda f, s=0: fld[f, x, t, pl.ds(8 + s, CY), :]
                pz, wz, mz = (a[j * CY : (j + 1) * CY, 128 * t : 128 * t + 128] for a in zs)

                def dy(f):
                    return (
                        0.75 * (at(f, 1) - at(f, -1)) - 0.15 * (at(f, 2) - at(f, -2))
                        + (1.0 / 60.0) * (at(f, 3) - at(f, -3))
                    )

                px, ux, vx, wx, mx = (grd[f, x, t] for f in range(5))
                m, u, v, w = at(4), at(1), at(2), at(3)
                grd[0, x, t] = m * px + ux + dy(2) + wz
                grd[1, x, t] = m * ux + u * mx + v * dy(4) + w * mz + px
                grd[2, x, t] = m * vx + dy(0)
                grd[3, x, t] = m * wx + pz
        return 0

    lax.fori_loop(0, CX // step, local, 0)

    def gather(n, _):
        for k in range(8):
            j = n * 8 + k
            cell = cell_s[0, j]
            line = lax.shift_right_logical(cell, 8)
            x = lax.shift_right_logical(lax.shift_right_logical(line, 7) * 21846, 16)
            y = line - CY * lax.shift_right_logical(lax.shift_right_logical(line, 4) * 21846, 16)
            x = x & (CX - 1)
            t = lax.shift_right_logical(cell, 7) & 1
            for q in range(4):
                stg[q, pl.ds(j, 1), :] = grd[q, x, t, pl.ds(y, 1), :]
            for q, f in ((4, 0), (5, 1), (6, 4)):
                stg[q, pl.ds(j, 1), :] = fld[f, x, t, pl.ds(8 + y, 1), :]
        return 0

    lax.fori_loop(0, FACES_DEV // 8, gather, 0)

    cell = face_v[...]
    line = lax.shift_right_logical(cell, 8)
    fx = lax.shift_right_logical(lax.shift_right_logical(line, 7) * 21846, 16)
    fy = line - CY * lax.shift_right_logical(lax.shift_right_logical(line, 4) * 21846, 16)
    fx = fx & (CX - 1)
    fz = cell & 255
    rows_v[...] = jnp.zeros((16, 256), F32)
    rows_v[pl.ds(0, 3), pl.ds(0, FACES_DEV)] = pos_v[...]
    rows_v[pl.ds(3, 3), pl.ds(0, FACES_DEV)] = normal_v[...]
    rows_v[pl.ds(6, 1), pl.ds(0, FACES_DEV)] = fx.astype(F32)
    rows_v[pl.ds(7, 1), pl.ds(0, FACES_DEV)] = fy.astype(F32)
    rows_v[pl.ds(8, 1), pl.ds(0, FACES_DEV)] = fz.astype(F32)
    cols = rows_v[...].T
    col = lambda k: cols[:FACES_DEV, k : k + 1]
    xcol, ycol, zcol = col(6), col(7), col(8)
    lane = lax.broadcasted_iota(jnp.int32, (FACES_DEV, 128), 1).astype(F32)
    zlane = zcol - jnp.where(zcol >= 128.0, 128.0, 0.0)
    zmask = zlane == lane
    pick = lambda a: jnp.sum(jnp.where(zmask, a, 0.0), axis=1, keepdims=True)
    face0 = [pick(stg[q]) for q in range(7)]
    xmask = xcol == lane
    coef = [
        jnp.sum(jnp.where(xmask, table_v[pl.ds(k, 1), :], 0.0), axis=1, keepdims=True) for k in range(4)
    ]
    wide = lax.broadcasted_iota(jnp.int32, (FACES_DEV, 4 * CY), 1)
    part = (wide >= CY).astype(jnp.int32) + (wide >= 2 * CY).astype(jnp.int32) + (wide >= 3 * CY).astype(jnp.int32)
    hit = (wide - CY * part).astype(F32) == ycol
    weight = jnp.where(
        hit,
        jnp.where(part == 0, coef[0], jnp.where(part == 1, coef[1], jnp.where(part == 2, coef[2], coef[3]))),
        0.0,
    )
    weight = split2(weight)

    to = lax.broadcasted_iota(jnp.int32, (OBS, OBS), 1)
    source = (
        32 * (lax.shift_right_logical(to, 1) & 15) + 4 * (lax.shift_right_logical(to, 5) & 7)
        + 2 * (to & 1) + lax.shift_right_logical(to, 8)
    )
    perm = jnp.where(lax.broadcasted_iota(jnp.int32, (OBS, OBS), 0) == source, 1.0, 0.0).astype(BF16)
    tbp[...] = jnp.dot(tbin_v[...].astype(F32).astype(BF16), perm, preferred_element_type=F32)
    whole = obs_v[...]
    o_hi = whole.astype(BF16)
    rest = whole - o_hi.astype(F32)
    o_mid = rest.astype(BF16)
    o_lo = (rest - o_mid.astype(F32)).astype(BF16)
    seen = (
        jnp.dot(o_hi, perm, preferred_element_type=F32)
        + jnp.dot(o_mid, perm, preferred_element_type=F32)
        + jnp.dot(o_lo, perm, preferred_element_type=F32)
    )
    for t in range(4):
        lanes = slice(128 * t, 128 * t + 128)
        dx = seen[0:1, lanes] - col(0)
        dy_ = seen[1:2, lanes] - col(1)
        dz_ = seen[2:3, lanes] - col(2)
        inv = lax.rsqrt(dx * dx + dy_ * dy_ + dz_ * dz_)
        nr = (col(3) * dx + col(4) * dy_ + col(5) * dz_) * inv
        q1 = INV_FOUR_PI * inv
        geo[0, :, lanes] = q1
        geo[1, :, lanes] = q1 * nr
        geo[2, :, lanes] = q1 * nr * inv

    for way in range(2):
        @pl.when(gets[way])
        def _():
            for k in range(7):
                xc[way][k].wait_recv()
    near = []
    for f in range(5):
        near.append(dot3(weight, split2(hal[f].reshape(4 * CY, NZ))))
    fp, fu, fm = face0[4], face0[5], face0[6]
    add0 = fm * near[0] + near[1]
    adda = (
        col(3) * (fm * near[1] + fu * near[4] + near[0])
        + (col(4) * fm) * near[2] + (col(5) * fm) * near[3]
    )
    zwide = lax.broadcasted_iota(jnp.int32, (FACES_DEV, NZ), 1).astype(F32) == zcol
    pickw = lambda a: jnp.sum(jnp.where(zwide, a, 0.0), axis=1, keepdims=True)
    rate0 = -(face0[0] + pickw(add0))
    ratea = -(col(3) * face0[1] + col(4) * face0[2] + col(5) * face0[3] + pickw(adda))
    pnext = fp + TIME_STEP * rate0
    for t in range(4):
        lanes = slice(128 * t, 128 * t + 128)
        geo[0, :, lanes] = ratea * geo[0, :, lanes] + rate0 * geo[1, :, lanes] + pnext * geo[2, :, lanes]

    def one_bin(b, _):
        want = b.astype(F32)
        for t in range(4):
            acc = jnp.zeros((8, 128), F32)
            for g in range(FACES_DEV // 8):
                rows = pl.ds(8 * g, 8)
                lanes = pl.ds(128 * t, 128)
                acc = acc + jnp.where(tbp[rows, lanes] == want, geo[0, rows, lanes], 0.0)
            binned[t, pl.ds(b, 1), :] = jnp.sum(acc, axis=0, keepdims=True)
        return 0

    lax.fori_loop(0, BINS, one_bin, 0)
    for t in range(2):
        both = jnp.concatenate([binned[t], binned[2 + t]], axis=0)
        packed[pl.ds(128 * t, 128), :] = both.T

    ac = []
    for k in range(1, N_YZ):
        peer = lax.rem(yz + k, N_YZ)
        c = pltpu.make_async_remote_copy(
            src_ref=packed.at[pl.ds(pl.multiple_of(32 * peer, 32), 32), :], dst_ref=recv_a.at[k - 1],
            send_sem=as_sem.at[k - 1], recv_sem=ar_sem.at[k - 1], device_id=(gx, peer), device_id_type=MESH,
        )
        c.start()
        ac.append(c)

    def finish(x, _):
        ca, cb = table_s[0, x], table_s[1, x]
        for t in range(2):
            for h in range(2):
                lanes = pl.ds(128 * t, 128)
                ys = pl.ds(24 * h, 24)
                px, ux, vx, wx, mx = (ca * hal[f, 0, ys, lanes] + cb * hal[f, 1, ys, lanes] for f in range(5))
                p, u, v, w, m = (fld[f, x, t, pl.ds(8 + 24 * h, 24), :] for f in range(5))
                n0, n1, n2, n3 = (grd[q, x, t, ys, :] for q in range(4))
                nxt[0, x, ys, lanes] = p - TIME_STEP * (n0 + m * px + ux)
                nxt[1, x, ys, lanes] = u - TIME_STEP * (n1 + m * ux + u * mx + px)
                nxt[2, x, ys, lanes] = v - TIME_STEP * (n2 + m * vx)
                nxt[3, x, ys, lanes] = w - TIME_STEP * (n3 + m * wx)
        return 0

    def edges():
        for x, k, sign in ((0, 2, DD), (CX - 1, 3, -DD)):
            for t in range(2):
                lanes = pl.ds(128 * t, 128)
                px, ux, vx, wx, mx = ((-TIME_STEP * sign) * hal[f, k, :, lanes] for f in range(5))
                u, m = fld[1, x, t, pl.ds(8, CY), :], fld[4, x, t, pl.ds(8, CY), :]
                nxt[0, x, :, lanes] += m * px + ux
                nxt[1, x, :, lanes] += m * ux + u * mx + px
                nxt[2, x, :, lanes] += m * vx
                nxt[3, x, :, lanes] += m * wx

    lax.fori_loop(0, CX // 2, finish, 0)

    total = packed[pl.ds(pl.multiple_of(32 * yz, 32), 32), :]
    for k in range(N_YZ - 1):
        ac[k].wait_recv()
        total = total + recv_a[k]
    for g in range(N_GX):
        send_b[g] = total[2 * g : 2 * g + 2]
    bc = []
    for k in range(1, N_GX):
        peer = lax.rem(gx + k, N_GX)
        c = pltpu.make_async_remote_copy(
            src_ref=send_b.at[peer], dst_ref=recv_b.at[k - 1],
            send_sem=bs_sem.at[k - 1], recv_sem=br_sem.at[k - 1], device_id=(peer, yz), device_id_type=MESH,
        )
        c.start()
        bc.append(c)

    lax.fori_loop(CX // 2, CX, finish, 0)
    edges()

    total = send_b[gx]
    for k in range(N_GX - 1):
        bc[k].wait_recv()
        total = total + recv_b[k]
    for h in range(2):
        for h2 in range(2):
            sig[pl.ds(2 * h + h2, 1), :] = total[h : h + 1, BINS * h2 : BINS * h2 + BINS]

    for way in range(2):
        @pl.when(sends[way])
        def _():
            for c in xc[way]:
                c.wait_send()

        @pl.when(ysends[way])
        def _():
            for c in yc[way]:
                c.wait_send()
    for c in ac + bc:
        c.wait_send()


def per_device(state, mean_flow, face_cell, face_normal, face_pos, observer_pos, time_bin):
    n = np.arange(CX)
    table = np.zeros((8, 128), np.float32)
    table[0, :CX] = CC * LAM ** (n + 1.0)
    table[1, :CX] = -CC * LAM ** (CX - n * 1.0)
    table[2, 0] = DD
    table[3, CX - 1] = -DD
    dz = operator(NZ).T.astype(np.float32)
    dz = jnp.stack(split2(jnp.asarray(dz)))
    ends = closure(CX, CX * N_GX)
    anywhere = pl.BlockSpec(memory_space=pl.ANY)
    vm = pltpu.VMEM
    dma = pltpu.SemaphoreType.DMA
    nxt, sig = pl.pallas_call(
        functools.partial(kernel, ends),
        out_shape=(
            jax.ShapeDtypeStruct((4, CX, CY, NZ), F32),
            jax.ShapeDtypeStruct((4, BINS), F32),
        ),
        in_specs=[anywhere] * 10,
        out_specs=(pl.BlockSpec(memory_space=pltpu.VMEM), pl.BlockSpec(memory_space=pltpu.VMEM)),
        scratch_shapes=[
            vm((5, CX, 2, 64, 128), F32),
            vm((5, CX, 2, CY, 128), F32),
            vm((5, 4, CY, NZ), F32),
            vm((2, 5, CY, NZ), F32),
            vm((7, FACES_DEV, 128), F32),
            vm((3, FACES_DEV, OBS), F32),
            vm((FACES_DEV, OBS), F32),
            vm((1, FACES_DEV), jnp.int32),
            vm((3, FACES_DEV), F32),
            vm((3, FACES_DEV), F32),
            vm((3, OBS), F32),
            vm((FACES_DEV, OBS), jnp.int32),
            vm((2, NZ, NZ), BF16),
            vm((8, 128), F32),
            vm((16, 256), F32),
            vm((4, BINS, 128), F32),
            vm((256, 128), F32),
            vm((N_YZ - 1, 32, 128), F32),
            vm((N_GX, 2, 128), F32),
            vm((N_GX - 1, 2, 128), F32),
            pltpu.SMEM((4, 128), F32),
            pltpu.SMEM((1, FACES_DEV), jnp.int32),
            dma((5, 2)), dma((9,)), dma((2, 7)), dma((2, 7)), dma((2, 3)), dma((2, 3)),
            dma((N_YZ - 1,)), dma((N_YZ - 1,)), dma((N_GX - 1,)), dma((N_GX - 1,)),
        ],
        compiler_params=pltpu.CompilerParams(
            collective_id=0, has_side_effects=True, vmem_limit_bytes=63000 * 1024
        ),
    )(
        state, mean_flow, face_cell.reshape(1, FACES_DEV), face_normal, face_pos, observer_pos, time_bin,
        dz, jnp.asarray(table), jnp.asarray(table[:4]),
    )
    return nxt, sig


def solution(mesh):
    return jax.shard_map(
        per_device,
        mesh=mesh,
        in_specs=(
            P(None, "gx", "yz", None),
            P("gx", "yz", None),
            P(("gx", "yz")),
            P(None, ("gx", "yz")),
            P(None, ("gx", "yz")),
            P(),
            P(("gx", "yz"), None),
        ),
        out_specs=(P(None, "gx", "yz", None), P(("gx", "yz"), None)),
        check_vma=False,
    )
```

```python
import functools

import jax
import jax.numpy as jnp
import numpy as np
from jax import lax
from jax.experimental import pallas as pl
from jax.experimental.pallas import tpu as pltpu
from jax.sharding import PartitionSpec as P

CX, CY, NZ = 32, 48, 256
FACES_DEV, OBS, BINS = 192, 512, 64
N_GX, N_YZ = 16, 8
TIME_STEP = 0.25
INV_FOUR_PI = 1.0 / (4.0 * 3.141592653589793)
MESH = pl.DeviceIdType.MESH
F32, BF16 = jnp.float32, jnp.bfloat16

LAM = (-1.0 + np.sqrt(1.0 - 4.0 / 9.0)) / (2.0 / 3.0)
CC, DD = 25.0 / 12.0, -1.0 / 12.0
EDGE = DD / CC


def operator(n):
    a = np.eye(n)
    b = np.zeros((n, n))
    for i in range(n):
        if i == 0:
            a[0, 1] = 2.0
            b[0, :3] = (-2.5, 2.0, 0.5)
        elif i == n - 1:
            a[i, i - 1] = 2.0
            b[i, n - 3 :] = (-0.5, -2.0, 2.5)
        elif i in (1, n - 2):
            a[i, i - 1] = a[i, i + 1] = 0.25
            b[i, i + 1], b[i, i - 1] = 0.75, -0.75
        else:
            a[i, i - 1] = a[i, i + 1] = 1.0 / 3.0
            b[i, i + 1], b[i, i - 1] = 7.0 / 9.0, -7.0 / 9.0
            b[i, i + 2], b[i, i - 2] = 1.0 / 36.0, -1.0 / 36.0
    return np.linalg.solve(a, b)


def closure(n, total):
    lag = np.arange(n)[:, None] - np.arange(n)[None, :]
    inside = np.where(
        lag == 0, 0.0, np.sign(lag) * (CC * LAM ** np.abs(lag) + DD * (np.abs(lag) == 1))
    )
    rest = operator(total)[:n, :n] - inside
    factors = np.stack([CC * LAM ** (np.arange(n) + 1.0), DD * (np.arange(n) == 0)], 1)
    weights = np.linalg.lstsq(factors, rest, rcond=None)[0]
    scale = weights[:, 12] / LAM**12
    return np.concatenate([weights[:, :4] - scale[:, None] * LAM ** np.arange(4.0), scale[:, None]], 1)


def split2(x):
    hi = x.astype(BF16)
    return hi, (x - hi.astype(F32)).astype(BF16)


class Marks:
    def __init__(self):
        self.scope = None

    def __call__(self, name):
        if self.scope is not None:
            self.scope.__exit__(None, None, None)
        self.scope = None if name is None else jax.named_scope(name)
        if self.scope is not None:
            self.scope.__enter__()


def dot3(a, b):
    return (
        jnp.dot(a[0], b[0], preferred_element_type=F32)
        + jnp.dot(a[1], b[0], preferred_element_type=F32)
        + jnp.dot(a[0], b[1], preferred_element_type=F32)
    )


def kernel(
    ends, state, mean, face_cell, normal, pos, obs, tbin, dz, table, table_s_in, had,
    nxt, sig,
    fld, grd, zed, hal, tsum, stg, geo, sgn, face_v, normal_v, pos_v, obs_v, tbin_v, dz_v, table_v, had_v,
    rows_v, seen_v, binned, packed, recv_a, send_b, recv_b, table_s, cell_s,
    ld_sem, in_sem, xs_sem, xr_sem, ys_sem, yr_sem, as_sem, ar_sem, bs_sem, br_sem,
):
    mark = Marks()
    gx = lax.axis_index("gx")
    yz = lax.axis_index("yz")

    mark("start")
    order = (0, 4, 2, 3, 1)
    small = []
    for k, (s, d) in enumerate((
        (obs, obs_v), (tbin, tbin_v), (dz, dz_v), (table, table_v), (table_s_in, table_s),
        (face_cell, cell_s), (face_cell, face_v), (normal, normal_v), (pos, pos_v), (had, had_v),
    )):
        c = pltpu.make_async_copy(s, d, in_sem.at[k])
        c.start()
        small.append(c)

    loads = {}
    for f in order:
        src = mean if f == 4 else state.at[f]
        for t in range(2):
            c = pltpu.make_async_copy(
                src.at[:, :, pl.ds(128 * t, 128)], fld.at[f, :, t, pl.ds(8, CY), :], ld_sem.at[f, t]
            )
            c.start()
            loads[f, t] = c
    mark("barrier")
    barrier = pltpu.get_barrier_semaphore()
    for k in range(1, N_GX):
        pl.semaphore_signal(barrier, inc=1, device_id=(lax.rem(gx + k, N_GX), yz), device_id_type=MESH)
    for k in range(1, N_YZ):
        pl.semaphore_signal(barrier, inc=1, device_id=(gx, lax.rem(yz + k, N_YZ)), device_id_type=MESH)
    mark("observers")
    to = lax.broadcasted_iota(jnp.int32, (OBS, OBS), 1)
    source = (
        32 * (lax.shift_right_logical(to, 1) & 15) + 4 * (lax.shift_right_logical(to, 5) & 7)
        + 2 * (to & 1) + lax.shift_right_logical(to, 8)
    )
    perm = jnp.where(lax.broadcasted_iota(jnp.int32, (OBS, OBS), 0) == source, 1.0, 0.0).astype(BF16)
    small[0].wait()
    small[1].wait()
    which = jnp.dot(tbin_v[...].astype(F32).astype(BF16), perm, preferred_element_type=F32).astype(jnp.int32)
    for k in range(6):
        sgn[k] = jnp.where((which & (1 << k)) == 0, 1.0, -1.0)
    whole = obs_v[...]
    o_hi = whole.astype(BF16)
    rest = whole - o_hi.astype(F32)
    o_mid = rest.astype(BF16)
    o_lo = (rest - o_mid.astype(F32)).astype(BF16)
    seen_v[pl.ds(0, 3), :] = (
        jnp.dot(o_hi, perm, preferred_element_type=F32)
        + jnp.dot(o_mid, perm, preferred_element_type=F32)
        + jnp.dot(o_lo, perm, preferred_element_type=F32)
    )
    mark("barrier_wait")
    pl.semaphore_wait(barrier, N_GX + N_YZ - 2)

    mark("issue")
    has_left, has_right = gx > 0, gx < N_GX - 1
    has_low, has_high = yz > 0, yz < N_YZ - 1
    right, left = (lax.rem(gx + 1, N_GX), yz), (lax.rem(gx + N_GX - 1, N_GX), yz)
    high, low = (gx, lax.rem(yz + 1, N_YZ)), (gx, lax.rem(yz + N_YZ - 1, N_YZ))

    def xcopy(src, dst, way, k):
        return pltpu.make_async_remote_copy(
            src_ref=src, dst_ref=dst, send_sem=xs_sem.at[way, k], recv_sem=xr_sem.at[way, k],
            device_id=(right, left)[way], device_id_type=MESH,
        )

    xc = ([], [])
    for way, plane in ((0, CX - 1), (1, 0)):
        xc[way].append(xcopy(state.at[:, plane], hal.at[pl.ds(0, 4), 2 + way], way, 0))
        xc[way].append(xcopy(mean.at[plane], hal.at[4, 2 + way], way, 1))
        for f in range(5):
            xc[way].append(xcopy(tsum.at[way, f], hal.at[f, way], way, 2 + f))
    sends = (has_right, has_left)
    gets = (has_left, has_right)
    for way in range(2):
        @pl.when(sends[way])
        def _():
            xc[way][0].start()
            xc[way][1].start()

    yc = ([], [])
    for k, f in enumerate((0, 2, 4)):
        for way, (first, there) in enumerate(((8 + CY - 3, 5), (8, 8 + CY))):
            yc[way].append(pltpu.make_async_remote_copy(
                src_ref=fld.at[f, :, :, pl.ds(first, 3), :], dst_ref=fld.at[f, :, :, pl.ds(there, 3), :],
                send_sem=ys_sem.at[way, k], recv_sem=yr_sem.at[way, k],
                device_id=(high, low)[way], device_id_type=MESH,
            ))
    ysends = (has_high, has_low)
    ygets = (has_low, has_high)

    mark("sweeps")
    small[2].wait()

    def along_z(j):
        q = j // 4
        x0 = 8 * (j - 4 * q)
        f = jnp.where(q == 0, 0, 5 - q)
        v = fld[f, pl.ds(x0, 8), :, pl.ds(8, CY), :]
        v = jnp.concatenate([v[:, 0], v[:, 1]], axis=-1).reshape(8 * CY, NZ)
        hi, lo = split2(v)
        out = jnp.dot(jnp.concatenate([hi, lo, hi], axis=1), dz_v[...], preferred_element_type=F32)
        zed[q, pl.ds(x0, 8)] = out.reshape(8, CY, NZ)

    jobs = 0
    for f, per_half in zip(order, (1, 1, 1, 2, 1)):
        loads[f, 0].wait()
        loads[f, 1].wait()
        if f in (0, 2, 4):
            for way in range(2):
                @pl.when(ysends[way])
                def _():
                    yc[way][f // 2].start()

        def sweep(t, _, f=f, per_half=per_half, jobs=jobs):
            zero = jnp.zeros((CY, 128), F32)
            at = lambda i: fld[f, i, t, pl.ds(8, CY), :] if 0 <= i < CX else zero
            up, down, v_old, w_old = zero, zero, zero, zero
            v, w = at(0), at(CX - 1)
            for i in range(CX):
                if i * per_half // CX != (i - 1) * per_half // CX:
                    along_z(jobs + per_half * t + i * per_half // CX)
                k = CX - 1 - i
                v_new, w_new = at(i + 1), at(k - 1)
                if i < CX // 2:
                    grd[f, i, t, pl.ds(0, CY), :] = up
                    grd[f, k, t, pl.ds(0, CY), :] = down
                else:
                    grd[f, i, t, pl.ds(0, CY), :] = (up - grd[f, i, t, pl.ds(0, CY), :]) + EDGE * (v_old - v_new)
                    grd[f, k, t, pl.ds(0, CY), :] = (grd[f, k, t, pl.ds(0, CY), :] - down) + EDGE * (w_new - w_old)
                up_sum, down_sum = up + v, down + w
                up, down = LAM * up_sum, LAM * down_sum
                v_old, v, w_old, w = v, v_new, w, w_new
            lanes = pl.ds(pl.multiple_of(128 * t, 128), 128)
            tsum[0, f, :, lanes] = up_sum
            tsum[1, f, :, lanes] = down_sum
            return 0

        lax.fori_loop(0, 2, sweep, 0)
        jobs += 2 * per_half
        for way in range(2):
            @pl.when(sends[way])
            def _():
                xc[way][2 + f].start()

    mark("ends")
    for way, there in ((0, jnp.logical_not(has_left)), (1, jnp.logical_not(has_right))):
        @pl.when(there)
        def _():
            def close(n, _):
                f, t = n // 2, n % 2
                lanes = pl.ds(pl.multiple_of(128 * t, 128), 128)
                far = tsum[1 - way, f, :, lanes]
                one, two = float(ends[0, 4]) * far, float(ends[1, 4]) * far
                for i in range(4):
                    v = fld[f, i if way == 0 else CX - 1 - i, t, pl.ds(8, CY), :]
                    one = one + float(ends[0, i]) * v
                    two = two + float(ends[1, i]) * v
                hal[f, way, :, lanes] = one
                hal[f, 2 + way, :, lanes] = two
                return 0

            lax.fori_loop(0, 10, close, 0)
    for way, there, row in ((0, jnp.logical_not(has_low), 5), (1, jnp.logical_not(has_high), 8 + CY)):
        @pl.when(there)
        def _():
            for f in (0, 2, 4):
                fld[f, :, :, pl.ds(row, 3), :] = jnp.zeros((CX, 2, 3, 128), F32)

    mark("wait_y")
    for c in small[3:]:
        c.wait()
    for way in range(2):
        @pl.when(ygets[way])
        def _():
            for k in range(3):
                yc[way][k].wait_recv()

    mark("local")
    def local(n, _):
        for j in range(2):
            for t in range(2):
                x = 2 * n + j
                at = lambda f, s=0: fld[f, x, t, pl.ds(8 + s, CY), :]
                pz, mz, wz = (zed[q, x, :, 128 * t : 128 * t + 128] for q in range(3))

                def dy(f):
                    return (
                        0.75 * (at(f, 1) - at(f, -1)) - 0.15 * (at(f, 2) - at(f, -2))
                        + (1.0 / 60.0) * (at(f, 3) - at(f, -3))
                    )

                px, ux, vx, wx, mx = (grd[f, x, t, pl.ds(0, CY), :] for f in range(5))
                m, u, v, w = at(4), at(1), at(2), at(3)
                cm = CC * m
                grd[0, x, t, pl.ds(0, CY), :] = cm * px + CC * ux + dy(2) + wz
                grd[1, x, t, pl.ds(0, CY), :] = cm * ux + CC * (u * mx + px) + v * dy(4) + w * mz
                grd[2, x, t, pl.ds(0, CY), :] = cm * vx + dy(0)
                grd[3, x, t, pl.ds(0, CY), :] = cm * wx + pz
        return 0

    lax.fori_loop(0, CX // 2, local, 0)

    mark("gather")
    corner = gx * (CX * CY * N_YZ) + yz * CY
    grd_rows = grd.reshape(5, CX * 2 * 64, 128)
    fld_rows = fld.reshape(5, CX * 2 * 64, 128)

    def gather(n, _):
        for k in range(8):
            j = n * 8 + k
            cell = cell_s[0, j]
            line = jnp.maximum(lax.shift_right_logical(cell, 8) - corner, 0)
            x = lax.shift_right_logical(lax.shift_right_logical(line, 7) * 86, 8)
            row = line - 256 * x + (lax.shift_right_logical(cell, 1) & 64)
            for q in range(4):
                stg[q, pl.ds(j, 1), :] = grd_rows[q, pl.ds(row, 1), :]
            for q, f in ((4, 0), (5, 1), (6, 4)):
                stg[q, pl.ds(j, 1), :] = fld_rows[f, pl.ds(row + 8, 1), :]
        return 0

    lax.fori_loop(0, FACES_DEV // 8, gather, 0)

    mark("columns")
    cell = face_v[...]
    line = lax.shift_right_logical(cell, 8)
    fx = lax.shift_right_logical(lax.shift_right_logical(line, 7) * 21846, 16)
    fy = line - CY * lax.shift_right_logical(lax.shift_right_logical(line, 4) * 21846, 16)
    fx = fx & (CX - 1)
    fz = cell & 255
    rows_v[...] = jnp.zeros((16, 256), F32)
    rows_v[pl.ds(0, 3), pl.ds(0, FACES_DEV)] = pos_v[...]
    rows_v[pl.ds(3, 3), pl.ds(0, FACES_DEV)] = normal_v[...]
    rows_v[pl.ds(6, 1), pl.ds(0, FACES_DEV)] = fx.astype(F32)
    rows_v[pl.ds(7, 1), pl.ds(0, FACES_DEV)] = fy.astype(F32)
    rows_v[pl.ds(8, 1), pl.ds(0, FACES_DEV)] = fz.astype(F32)
    cols = rows_v[...].T
    col = lambda k: cols[:FACES_DEV, k : k + 1]
    xcol, ycol, zcol = col(6), col(7), col(8)
    lane = lax.broadcasted_iota(jnp.int32, (FACES_DEV, 128), 1).astype(F32)
    zlane = zcol - jnp.where(zcol >= 128.0, 128.0, 0.0)
    zmask = zlane == lane
    pick = lambda a: jnp.sum(jnp.where(zmask, a, 0.0), axis=1, keepdims=True)
    face0 = [pick(stg[q]) for q in range(7)]
    xmask = xcol == lane
    coef = [
        jnp.sum(jnp.where(xmask, table_v[pl.ds(k, 1), :], 0.0), axis=1, keepdims=True) for k in range(4)
    ]
    wide = lax.broadcasted_iota(jnp.int32, (FACES_DEV, 4 * CY), 1)
    part = (wide >= CY).astype(jnp.int32) + (wide >= 2 * CY).astype(jnp.int32) + (wide >= 3 * CY).astype(jnp.int32)
    hit = (wide - CY * part).astype(F32) == ycol
    weight = jnp.where(
        hit,
        jnp.where(part == 0, coef[0], jnp.where(part == 1, coef[1], jnp.where(part == 2, coef[2], coef[3]))),
        0.0,
    )
    hi, lo = split2(weight)
    weight = jnp.concatenate([hi, lo, hi], axis=1)

    mark("geometry")
    for t in range(4):
        lanes = slice(128 * t, 128 * t + 128)
        dx = seen_v[0:1, lanes] - col(0)
        dy_ = seen_v[1:2, lanes] - col(1)
        dz_ = seen_v[2:3, lanes] - col(2)
        inv = lax.rsqrt(dx * dx + dy_ * dy_ + dz_ * dz_)
        nr = (col(3) * dx + col(4) * dy_ + col(5) * dz_) * inv
        q1 = INV_FOUR_PI * inv
        geo[0, :, lanes] = q1
        geo[1, :, lanes] = q1 * nr
        geo[2, :, lanes] = q1 * nr * inv

    mark("wait_x")
    for way in range(2):
        @pl.when(gets[way])
        def _():
            for c in xc[way]:
                c.wait_recv()
    mark("near")
    near = []
    for f in range(5):
        hi, lo = split2(hal[f].reshape(4 * CY, NZ))
        near.append(jnp.dot(weight, jnp.concatenate([hi, hi, lo], axis=0), preferred_element_type=F32))
    fp, fu, fm = face0[4], face0[5], face0[6]
    add0 = fm * near[0] + near[1]
    adda = (
        col(3) * (fm * near[1] + fu * near[4] + near[0])
        + (col(4) * fm) * near[2] + (col(5) * fm) * near[3]
    )
    zwide = lax.broadcasted_iota(jnp.int32, (FACES_DEV, NZ), 1).astype(F32) == zcol
    pickw = lambda a: jnp.sum(jnp.where(zwide, a, 0.0), axis=1, keepdims=True)
    rate0 = -(face0[0] + pickw(add0))
    ratea = -(col(3) * face0[1] + col(4) * face0[2] + col(5) * face0[3] + pickw(adda))
    pnext = fp + TIME_STEP * rate0
    for t in range(4):
        lanes = slice(128 * t, 128 * t + 128)
        geo[0, :, lanes] = ratea * geo[0, :, lanes] + rate0 * geo[1, :, lanes] + pnext * geo[2, :, lanes]

    mark("bins")
    def patterns(n, _):
        t = n // 8
        block = n - 8 * t
        lanes = pl.ds(pl.multiple_of(128 * t, 128), 128)
        after = block + 1
        bit = jnp.where(after % 2 == 1, 3, jnp.where(after % 4 == 2, 4, 5))
        acc = [jnp.zeros((8, 128), F32)] * 8
        for g in range(FACES_DEV // 8):
            rows = pl.ds(8 * g, 8)
            what = geo[0, rows, lanes]
            geo[0, rows, lanes] = what * sgn[bit, rows, lanes]
            low = [sgn[k, rows, lanes] for k in range(3)]
            for k in range(8):
                if k:
                    what = what * low[0 if k % 2 else (1 if k % 4 else 2)]
                acc[k] = acc[k] + what
        for k in range(8):
            binned[t, pl.ds(pl.multiple_of(64 * block, 8) + 8 * k, 8), :] = acc[k]
        return 0

    lax.fori_loop(0, 32, patterns, 0)
    mark("pack")

    def folded(t):
        out = binned[t, pl.ds(0, BINS, stride=8), :]
        for k in range(1, 8):
            out = out + binned[t, pl.ds(k, BINS, stride=8), :]
        return out

    for t in range(2):
        both = jnp.concatenate([folded(t), folded(2 + t)], axis=0).T
        hi = both.astype(BF16)
        rest = both - hi.astype(F32)
        mid = rest.astype(BF16)
        lo = (rest - mid.astype(F32)).astype(BF16)
        had = had_v[...]
        packed[pl.ds(128 * t, 128), :] = (
            jnp.dot(hi, had, preferred_element_type=F32)
            + jnp.dot(mid, had, preferred_element_type=F32)
            + jnp.dot(lo, had, preferred_element_type=F32)
        )

    ac = []
    for k in range(1, N_YZ):
        peer = lax.rem(yz + k, N_YZ)
        c = pltpu.make_async_remote_copy(
            src_ref=packed.at[pl.ds(pl.multiple_of(32 * peer, 32), 32), :], dst_ref=recv_a.at[k - 1],
            send_sem=as_sem.at[k - 1], recv_sem=ar_sem.at[k - 1], device_id=(gx, peer), device_id_type=MESH,
        )
        c.start()
        ac.append(c)

    mark("finish_a")
    def finish(x, _):
        ca, cb = table_s[0, x], table_s[1, x]
        for t in range(2):
            for h in range(2):
                lanes = pl.ds(128 * t, 128)
                ys = pl.ds(24 * h, 24)
                px, ux, vx, wx, mx = (ca * hal[f, 0, ys, lanes] + cb * hal[f, 1, ys, lanes] for f in range(5))
                p, u, v, w, m = (fld[f, x, t, pl.ds(8 + 24 * h, 24), :] for f in range(5))
                n0, n1, n2, n3 = (grd[q, x, t, ys, :] for q in range(4))
                nxt[0, x, ys, lanes] = p - TIME_STEP * (n0 + m * px + ux)
                nxt[1, x, ys, lanes] = u - TIME_STEP * (n1 + m * ux + u * mx + px)
                nxt[2, x, ys, lanes] = v - TIME_STEP * (n2 + m * vx)
                nxt[3, x, ys, lanes] = w - TIME_STEP * (n3 + m * wx)
        return 0

    def edges():
        for x, k, sign in ((0, 2, DD), (CX - 1, 3, -DD)):
            for t in range(2):
                lanes = pl.ds(128 * t, 128)
                px, ux, vx, wx, mx = ((-TIME_STEP * sign) * hal[f, k, :, lanes] for f in range(5))
                u, m = fld[1, x, t, pl.ds(8, CY), :], fld[4, x, t, pl.ds(8, CY), :]
                nxt[0, x, :, lanes] += m * px + ux
                nxt[1, x, :, lanes] += m * ux + u * mx + px
                nxt[2, x, :, lanes] += m * vx
                nxt[3, x, :, lanes] += m * wx

    lax.fori_loop(0, CX // 2, finish, 0)

    mark("wait_a")
    total = packed[pl.ds(pl.multiple_of(32 * yz, 32), 32), :]
    for k in range(N_YZ - 1):
        ac[k].wait_recv()
        total = total + recv_a[k]
    for g in range(N_GX):
        send_b[g] = total[2 * g : 2 * g + 2]
    bc = []
    for k in range(1, N_GX):
        peer = lax.rem(gx + k, N_GX)
        c = pltpu.make_async_remote_copy(
            src_ref=send_b.at[peer], dst_ref=recv_b.at[k - 1],
            send_sem=bs_sem.at[k - 1], recv_sem=br_sem.at[k - 1], device_id=(peer, yz), device_id_type=MESH,
        )
        c.start()
        bc.append(c)

    mark("finish_b")
    lax.fori_loop(CX // 2, CX, finish, 0)
    edges()

    mark("wait_b")
    total = send_b[gx]
    for k in range(N_GX - 1):
        bc[k].wait_recv()
        total = total + recv_b[k]
    for h in range(2):
        for h2 in range(2):
            sig[pl.ds(2 * h + h2, 1), :] = total[h : h + 1, BINS * h2 : BINS * h2 + BINS]

    mark("drain")
    for way in range(2):
        @pl.when(sends[way])
        def _():
            for c in xc[way]:
                c.wait_send()

        @pl.when(ysends[way])
        def _():
            for c in yc[way]:
                c.wait_send()
    for c in ac + bc:
        c.wait_send()
    mark(None)


def per_device(state, mean_flow, face_cell, face_normal, face_pos, observer_pos, time_bin):
    n = np.arange(CX)
    table = np.zeros((8, 128), np.float32)
    table[0, :CX] = CC * LAM ** (n + 1.0)
    table[1, :CX] = -CC * LAM ** (CX - n * 1.0)
    table[2, 0] = DD
    table[3, CX - 1] = -DD
    dz = operator(NZ).T.astype(np.float32)
    dz_hi, dz_lo = split2(jnp.asarray(dz))
    dz = jnp.concatenate([dz_hi, dz_hi, dz_lo], axis=0)
    ends = closure(CX, CX * N_GX)
    gray = np.arange(BINS) // 8 * 8
    gray = (gray ^ (gray >> 1) & 56) + ((n := np.arange(BINS) % 8) ^ (n >> 1))
    common = gray[:, None] & np.arange(BINS)[None, :]
    parity = sum((common >> k) & 1 for k in range(6)) % 2
    had = np.kron(np.eye(2), (1.0 - 2.0 * parity) / BINS).astype(np.float32)
    anywhere = pl.BlockSpec(memory_space=pltpu.HBM)
    vm = pltpu.VMEM
    dma = pltpu.SemaphoreType.DMA
    nxt, sig = pl.pallas_call(
        functools.partial(kernel, ends),
        out_shape=(
            vm((4, CX, CY, NZ), F32),
            vm((4, BINS), F32),
        ),
        in_specs=[anywhere] * 11,
        out_specs=(pl.BlockSpec(memory_space=pltpu.VMEM), pl.BlockSpec(memory_space=pltpu.VMEM)),
        scratch_shapes=[
            vm((5, CX, 2, 64, 128), F32),
            vm((5, CX, 2, 64, 128), F32),
            vm((3, CX, CY, NZ), F32),
            vm((5, 4, CY, NZ), F32),
            vm((2, 5, CY, NZ), F32),
            vm((7, FACES_DEV, 128), F32),
            vm((3, FACES_DEV, OBS), F32),
            vm((6, FACES_DEV, OBS), F32),
            vm((1, FACES_DEV), jnp.int32),
            vm((3, FACES_DEV), F32),
            vm((3, FACES_DEV), F32),
            vm((3, OBS), F32),
            vm((FACES_DEV, OBS), jnp.int32),
            vm((3 * NZ, NZ), BF16),
            vm((8, 128), F32),
            vm((128, 128), BF16),
            vm((16, 256), F32),
            vm((8, OBS), F32),
            vm((4, 8 * BINS, 128), F32),
            vm((256, 128), F32),
            vm((N_YZ - 1, 32, 128), F32),
            vm((N_GX, 2, 128), F32),
            vm((N_GX - 1, 2, 128), F32),
            pltpu.SMEM((4, 128), F32),
            pltpu.SMEM((1, FACES_DEV), jnp.int32),
            dma((5, 2)), dma((10,)), dma((2, 7)), dma((2, 7)), dma((2, 3)), dma((2, 3)),
            dma((N_YZ - 1,)), dma((N_YZ - 1,)), dma((N_GX - 1,)), dma((N_GX - 1,)),
        ],
        compiler_params=pltpu.CompilerParams(
            collective_id=0, has_side_effects=True, vmem_limit_bytes=57 * 2**20 + 2**19
        ),
    )(
        state, mean_flow, face_cell.reshape(1, FACES_DEV), face_normal, face_pos, observer_pos, time_bin,
        dz, jnp.asarray(table), jnp.asarray(table[:4]), jnp.asarray(had, BF16),
    )
    return nxt, sig


def solution(mesh):
    return jax.shard_map(
        per_device,
        mesh=mesh,
        in_specs=(
            P(None, "gx", "yz", None),
            P("gx", "yz", None),
            P(("gx", "yz")),
            P(None, ("gx", "yz")),
            P(None, ("gx", "yz")),
            P(),
            P(("gx", "yz"), None),
        ),
        out_specs=(P(None, "gx", "yz", None), P(("gx", "yz"), None)),
        check_vma=False,
    )
```

```python
import functools

import jax
import jax.numpy as jnp
import numpy as np
from jax import lax
from jax.experimental import pallas as pl
from jax.experimental.pallas import tpu as pltpu
from jax.sharding import PartitionSpec as P

CX, CY, NZ = 32, 48, 256
FACES_DEV, OBS, BINS = 192, 512, 64
N_GX, N_YZ = 16, 8
TIME_STEP = 0.25
INV_FOUR_PI = 1.0 / (4.0 * 3.141592653589793)
MESH = pl.DeviceIdType.MESH
F32, BF16 = jnp.float32, jnp.bfloat16

LAM = (-1.0 + np.sqrt(1.0 - 4.0 / 9.0)) / (2.0 / 3.0)
CC, DD = 25.0 / 12.0, -1.0 / 12.0
EDGE = DD / CC


def operator(n):
    a = np.eye(n)
    b = np.zeros((n, n))
    for i in range(n):
        if i == 0:
            a[0, 1] = 2.0
            b[0, :3] = (-2.5, 2.0, 0.5)
        elif i == n - 1:
            a[i, i - 1] = 2.0
            b[i, n - 3 :] = (-0.5, -2.0, 2.5)
        elif i in (1, n - 2):
            a[i, i - 1] = a[i, i + 1] = 0.25
            b[i, i + 1], b[i, i - 1] = 0.75, -0.75
        else:
            a[i, i - 1] = a[i, i + 1] = 1.0 / 3.0
            b[i, i + 1], b[i, i - 1] = 7.0 / 9.0, -7.0 / 9.0
            b[i, i + 2], b[i, i - 2] = 1.0 / 36.0, -1.0 / 36.0
    return np.linalg.solve(a, b)


def closure(n, total):
    lag = np.arange(n)[:, None] - np.arange(n)[None, :]
    inside = np.where(
        lag == 0, 0.0, np.sign(lag) * (CC * LAM ** np.abs(lag) + DD * (np.abs(lag) == 1))
    )
    rest = operator(total)[:n, :n] - inside
    factors = np.stack([CC * LAM ** (np.arange(n) + 1.0), DD * (np.arange(n) == 0)], 1)
    weights = np.linalg.lstsq(factors, rest, rcond=None)[0]
    scale = weights[:, 12] / LAM**12
    return np.concatenate([weights[:, :4] - scale[:, None] * LAM ** np.arange(4.0), scale[:, None]], 1)


def split2(x):
    hi = x.astype(BF16)
    return hi, (x - hi.astype(F32)).astype(BF16)


class Marks:
    def __init__(self):
        self.scope = None

    def __call__(self, name):
        if self.scope is not None:
            self.scope.__exit__(None, None, None)
        self.scope = None if name is None else jax.named_scope(name)
        if self.scope is not None:
            self.scope.__enter__()


def dot3(a, b):
    return (
        jnp.dot(a[0], b[0], preferred_element_type=F32)
        + jnp.dot(a[1], b[0], preferred_element_type=F32)
        + jnp.dot(a[0], b[1], preferred_element_type=F32)
    )


def kernel(
    ends, state, mean, face_cell, normal, pos, obs, tbin, dz, table, table_s_in, had,
    nxt, sig,
    fld, grd, zed, hal, tsum, stg, geo, sgn, face_v, normal_v, pos_v, obs_v, tbin_v, dz_v, table_v, had_v,
    rows_v, seen_v, binned, packed, recv_a, send_b, recv_b, table_s, cell_s,
    ld_sem, in_sem, xs_sem, xr_sem, ys_sem, yr_sem, as_sem, ar_sem, bs_sem, br_sem, near_sem,
):
    mark = Marks()
    gx = lax.axis_index("gx")
    yz = lax.axis_index("yz")

    mark("barrier")
    barrier = pltpu.get_barrier_semaphore()
    def tell(sem, along, step):
        here, count = (gx, N_GX) if along == "gx" else (yz, N_YZ)
        for sign in (1, -1):
            there = here + sign * step

            @pl.when(there < count if sign > 0 else there >= 0)
            def _():
                to = (there, yz) if along == "gx" else (gx, there)
                pl.semaphore_signal(sem, inc=1, device_id=to, device_id_type=MESH)

    def told(sem, *pairs):
        total = 0
        for along, step in pairs:
            here, count = (gx, N_GX) if along == "gx" else (yz, N_YZ)
            total = total + (here >= step).astype(jnp.int32) + (here < count - step).astype(jnp.int32)
        pl.semaphore_wait(sem, total)

    tell(barrier, "gx", 1)
    tell(barrier, "yz", 1)
    mark("start")
    order = (0, 4, 2, 3, 1)
    small = []
    for k, (s, d) in enumerate((
        (obs, obs_v), (tbin, tbin_v), (dz, dz_v), (table, table_v), (table_s_in, table_s),
        (face_cell, cell_s), (face_cell, face_v), (normal, normal_v), (pos, pos_v), (had, had_v),
    )):
        c = pltpu.make_async_copy(s, d, in_sem.at[k])
        c.start()
        small.append(c)

    loads = {}
    for f in order:
        src = mean if f == 4 else state.at[f]
        for t in range(2):
            c = pltpu.make_async_copy(
                src.at[:, :, pl.ds(128 * t, 128)], fld.at[f, :, t, pl.ds(8, CY), :], ld_sem.at[f, t]
            )
            c.start()
            loads[f, t] = c
    mark("barrier_wait")
    told(barrier, ("gx", 1), ("yz", 1))

    mark("issue")
    has_left, has_right = gx > 0, gx < N_GX - 1
    has_low, has_high = yz > 0, yz < N_YZ - 1
    right, left = (lax.rem(gx + 1, N_GX), yz), (lax.rem(gx + N_GX - 1, N_GX), yz)
    high, low = (gx, lax.rem(yz + 1, N_YZ)), (gx, lax.rem(yz + N_YZ - 1, N_YZ))

    def xcopy(src, dst, way, k):
        return pltpu.make_async_remote_copy(
            src_ref=src, dst_ref=dst, send_sem=xs_sem.at[way, k], recv_sem=xr_sem.at[way, k],
            device_id=(right, left)[way], device_id_type=MESH,
        )

    xc = ([], [])
    for way, plane in ((0, CX - 1), (1, 0)):
        xc[way].append(xcopy(state.at[:, plane], hal.at[pl.ds(0, 4), 2 + way], way, 0))
        xc[way].append(xcopy(mean.at[plane], hal.at[4, 2 + way], way, 1))
        for f in range(5):
            xc[way].append(xcopy(tsum.at[way, f], hal.at[f, way], way, 2 + f))
    tell(near_sem.at[0], "gx", 1)
    tell(near_sem.at[0], "yz", 1)
    sends = (has_right, has_left)
    gets = (has_left, has_right)
    for way in range(2):
        @pl.when(sends[way])
        def _():
            xc[way][0].start()
            xc[way][1].start()

    yc = ([], [])
    for k, f in enumerate((0, 2, 4)):
        for way, (first, there) in enumerate(((8 + CY - 3, 5), (8, 8 + CY))):
            yc[way].append(pltpu.make_async_remote_copy(
                src_ref=fld.at[f, :, :, pl.ds(first, 3), :], dst_ref=fld.at[f, :, :, pl.ds(there, 3), :],
                send_sem=ys_sem.at[way, k], recv_sem=yr_sem.at[way, k],
                device_id=(high, low)[way], device_id_type=MESH,
            ))
    ysends = (has_high, has_low)
    ygets = (has_low, has_high)

    mark("observers")
    to = lax.broadcasted_iota(jnp.int32, (OBS, OBS), 1)
    source = (
        32 * (lax.shift_right_logical(to, 1) & 15) + 4 * (lax.shift_right_logical(to, 5) & 7)
        + 2 * (to & 1) + lax.shift_right_logical(to, 8)
    )
    perm = jnp.where(lax.broadcasted_iota(jnp.int32, (OBS, OBS), 0) == source, 1.0, 0.0).astype(BF16)
    small[0].wait()
    small[1].wait()
    which = jnp.dot(tbin_v[...].astype(F32).astype(BF16), perm, preferred_element_type=F32).astype(jnp.int32)
    for k in range(6):
        sgn[k] = jnp.where((which & (1 << k)) == 0, 1.0, -1.0)
    whole = obs_v[...]
    o_hi = whole.astype(BF16)
    rest = whole - o_hi.astype(F32)
    o_mid = rest.astype(BF16)
    o_lo = (rest - o_mid.astype(F32)).astype(BF16)
    seen_v[pl.ds(0, 3), :] = (
        jnp.dot(o_hi, perm, preferred_element_type=F32)
        + jnp.dot(o_mid, perm, preferred_element_type=F32)
        + jnp.dot(o_lo, perm, preferred_element_type=F32)
    )
    mark("columns")
    for c in small[3:]:
        c.wait()
    cell = face_v[...]
    line = lax.shift_right_logical(cell, 8)
    fx = lax.shift_right_logical(lax.shift_right_logical(line, 7) * 21846, 16)
    fy = line - CY * lax.shift_right_logical(lax.shift_right_logical(line, 4) * 21846, 16)
    fx = fx & (CX - 1)
    fz = cell & 255
    rows_v[...] = jnp.zeros((16, 256), F32)
    rows_v[pl.ds(0, 3), pl.ds(0, FACES_DEV)] = pos_v[...]
    rows_v[pl.ds(3, 3), pl.ds(0, FACES_DEV)] = normal_v[...]
    rows_v[pl.ds(6, 1), pl.ds(0, FACES_DEV)] = fx.astype(F32)
    rows_v[pl.ds(7, 1), pl.ds(0, FACES_DEV)] = fy.astype(F32)
    rows_v[pl.ds(8, 1), pl.ds(0, FACES_DEV)] = fz.astype(F32)
    cols = rows_v[...].T
    col = lambda k: cols[:FACES_DEV, k : k + 1]
    xcol, ycol, zcol = col(6), col(7), col(8)
    lane = lax.broadcasted_iota(jnp.int32, (FACES_DEV, 128), 1).astype(F32)
    zlane = zcol - jnp.where(zcol >= 128.0, 128.0, 0.0)
    zmask = zlane == lane
    pick = lambda a: jnp.sum(jnp.where(zmask, a, 0.0), axis=1, keepdims=True)
    xmask = xcol == lane
    coef = [
        jnp.sum(jnp.where(xmask, table_v[pl.ds(k, 1), :], 0.0), axis=1, keepdims=True) for k in range(4)
    ]
    upper = lane >= CY
    hit = jnp.where(upper, lane - CY, lane) == ycol
    weights = [
        jnp.where(hit, jnp.where(upper, coef[2 * k + 1], coef[2 * k]), 0.0) for k in range(2)
    ]
    mark("geometry")
    for t in range(4):
        lanes = slice(128 * t, 128 * t + 128)
        dx = seen_v[0:1, lanes] - col(0)
        dy_ = seen_v[1:2, lanes] - col(1)
        dz_ = seen_v[2:3, lanes] - col(2)
        inv = lax.rsqrt(dx * dx + dy_ * dy_ + dz_ * dz_)
        nr = (col(3) * dx + col(4) * dy_ + col(5) * dz_) * inv
        q1 = INV_FOUR_PI * inv
        geo[0, :, lanes] = q1
        geo[1, :, lanes] = q1 * nr
        geo[2, :, lanes] = q1 * nr * inv

    mark("wait_load")
    for f in order[:3]:
        loads[f, 0].wait()
        loads[f, 1].wait()
        for way in range(2):
            @pl.when(ysends[way])
            def _():
                yc[way][f // 2].start()

    mark("sweeps")
    small[2].wait()

    def along_z(j):
        q = j // 2
        x0 = 16 * (j - 2 * q)
        f = jnp.where(q == 0, 0, 5 - q)
        v = fld[f, pl.ds(x0, 16), :, pl.ds(8, CY), :]
        v = jnp.concatenate([v[:, 0], v[:, 1]], axis=-1).reshape(16 * CY, NZ)
        hi, lo = split2(v)
        out = jnp.dot(jnp.concatenate([hi, lo, hi], axis=1), dz_v[...], preferred_element_type=F32)
        zed[q, pl.ds(x0, 16)] = out.reshape(16, CY, NZ)

    jobs = 0
    for f, per_half in zip(order, (1, 1, 0, 1, 0)):
        if f not in (0, 2, 4):
            loads[f, 0].wait()
            loads[f, 1].wait()

        def sweep(t, _, f=f, per_half=per_half, jobs=jobs):
            zero = jnp.zeros((CY, 128), F32)
            at = lambda i: fld[f, i, t, pl.ds(8, CY), :] if 0 <= i < CX else zero
            up, down, v_old, w_old = zero, zero, zero, zero
            v, w = at(0), at(CX - 1)
            for i in range(CX):
                if i * per_half // CX != (i - 1) * per_half // CX:
                    along_z(jobs + per_half * t + i * per_half // CX)
                k = CX - 1 - i
                v_new, w_new = at(i + 1), at(k - 1)
                if i < CX // 2:
                    grd[f, i, t, pl.ds(0, CY), :] = up
                    grd[f, k, t, pl.ds(0, CY), :] = down
                else:
                    grd[f, i, t, pl.ds(0, CY), :] = (up - grd[f, i, t, pl.ds(0, CY), :]) + EDGE * (v_old - v_new)
                    grd[f, k, t, pl.ds(0, CY), :] = (grd[f, k, t, pl.ds(0, CY), :] - down) + EDGE * (w_new - w_old)
                up_sum, down_sum = up + v, down + w
                up, down = LAM * up_sum, LAM * down_sum
                v_old, v, w_old, w = v, v_new, w, w_new
            lanes = pl.ds(pl.multiple_of(128 * t, 128), 128)
            tsum[0, f, :, lanes] = up_sum
            tsum[1, f, :, lanes] = down_sum
            return 0

        lax.fori_loop(0, 2, sweep, 0)
        jobs += 2 * per_half
        for way in range(2):
            @pl.when(sends[way])
            def _():
                xc[way][2 + f].start()

    told(near_sem.at[0], ("gx", 1), ("yz", 1))
    tell(near_sem.at[1], "yz", 2)
    tell(near_sem.at[2], "gx", 2)
    mark("ends")
    for way, there in ((0, jnp.logical_not(has_left)), (1, jnp.logical_not(has_right))):
        @pl.when(there)
        def _():
            def close(n, _):
                f, t = n // 2, n % 2
                lanes = pl.ds(pl.multiple_of(128 * t, 128), 128)
                far = tsum[1 - way, f, :, lanes]
                one, two = float(ends[0, 4]) * far, float(ends[1, 4]) * far
                for i in range(4):
                    v = fld[f, i if way == 0 else CX - 1 - i, t, pl.ds(8, CY), :]
                    one = one + float(ends[0, i]) * v
                    two = two + float(ends[1, i]) * v
                hal[f, way, :, lanes] = one
                hal[f, 2 + way, :, lanes] = two
                return 0

            lax.fori_loop(0, 10, close, 0)
    for way, there, row in ((0, jnp.logical_not(has_low), 5), (1, jnp.logical_not(has_high), 8 + CY)):
        @pl.when(there)
        def _():
            for f in (0, 2, 4):
                fld[f, :, :, pl.ds(row, 3), :] = jnp.zeros((CX, 2, 3, 128), F32)

    mark("wait_y")
    for way in range(2):
        @pl.when(ygets[way])
        def _():
            for k in range(3):
                yc[way][k].wait_recv()

    mark("local")
    def local(n, _):
        for j in range(2):
            for t in range(2):
                x = 2 * n + j
                at = lambda f, s=0: fld[f, x, t, pl.ds(8 + s, CY), :]
                pz, mz, wz = (zed[q, x, :, 128 * t : 128 * t + 128] for q in range(3))

                def dy(f):
                    return (
                        0.75 * (at(f, 1) - at(f, -1)) - 0.15 * (at(f, 2) - at(f, -2))
                        + (1.0 / 60.0) * (at(f, 3) - at(f, -3))
                    )

                px, ux, vx, wx, mx = (grd[f, x, t, pl.ds(0, CY), :] for f in range(5))
                m, u, v, w = at(4), at(1), at(2), at(3)
                cm = CC * m
                grd[0, x, t, pl.ds(0, CY), :] = cm * px + CC * ux + dy(2) + wz
                grd[1, x, t, pl.ds(0, CY), :] = cm * ux + CC * (u * mx + px) + v * dy(4) + w * mz
                grd[2, x, t, pl.ds(0, CY), :] = cm * vx + dy(0)
                grd[3, x, t, pl.ds(0, CY), :] = cm * wx + pz
        return 0

    lax.fori_loop(0, CX // 2, local, 0)

    mark("gather")
    corner = gx * (CX * CY * N_YZ) + yz * CY
    grd_rows = grd.reshape(5, CX * 2 * 64, 128)
    fld_rows = fld.reshape(5, CX * 2 * 64, 128)

    def gather(n, _):
        for k in range(8):
            j = n * 8 + k
            cell = cell_s[0, j]
            line = jnp.maximum(lax.shift_right_logical(cell, 8) - corner, 0)
            x = lax.shift_right_logical(lax.shift_right_logical(line, 7) * 86, 8)
            row = line - 256 * x + (lax.shift_right_logical(cell, 1) & 64)
            for q in range(4):
                stg[q, pl.ds(j, 1), :] = grd_rows[q, pl.ds(row, 1), :]
            for q, f in ((4, 0), (5, 1), (6, 4)):
                stg[q, pl.ds(j, 1), :] = fld_rows[f, pl.ds(row + 8, 1), :]
        return 0

    lax.fori_loop(0, FACES_DEV // 8, gather, 0)

    told(near_sem.at[1], ("yz", 2))
    tell(near_sem.at[3], "yz", 4)
    mark("picks")
    face0 = [pick(stg[q]) for q in range(7)]
    fp, fu, fm = face0[4], face0[5], face0[6]
    fn = [col(3 + k) for k in range(3)]
    to0 = (fm, jnp.ones_like(fm))
    toa = (fn[0], fn[0] * fm, fn[1] * fm, fn[2] * fm, fn[0] * fu)

    def left_of(k, scales):
        out = []
        for scale in scales:
            hi, lo = split2(weights[k] * scale)
            out += [hi, lo, hi]
        return jnp.concatenate(out, axis=1)

    lefts = [(left_of(k, to0), left_of(k, toa)) for k in range(2)]

    mark("wait_x")
    for way in range(2):
        @pl.when(gets[way])
        def _():
            xc[way][0].wait_recv()
            xc[way][1].wait_recv()

    zwide = lax.broadcasted_iota(jnp.int32, (FACES_DEV, NZ), 1).astype(F32) == zcol
    pad = jnp.zeros((128 - 2 * CY, NZ), BF16)

    def at_faces(k):
        right = []
        for f in range(5):
            hi, lo = split2(hal[f, pl.ds(2 * k, 2)].reshape(2 * CY, NZ))
            right += [hi, pad, hi, pad, lo, pad]
        return [
            jnp.dot(a, jnp.concatenate(right[: 6 * n], axis=0), preferred_element_type=F32)
            for a, n in zip(lefts[k], (2, 5))
        ]

    edge0, edgea = at_faces(1)
    mark("wait_t")
    for way in range(2):
        @pl.when(gets[way])
        def _():
            for c in xc[way][2:]:
                c.wait_recv()
    mark("near")
    add0, adda = at_faces(0)
    pickw = lambda a: jnp.sum(jnp.where(zwide, a, 0.0), axis=1, keepdims=True)
    add0, adda = add0 + edge0, adda + edgea
    rate0 = -(face0[0] + pickw(add0))
    ratea = -(col(3) * face0[1] + col(4) * face0[2] + col(5) * face0[3] + pickw(adda))
    pnext = fp + TIME_STEP * rate0
    for t in range(4):
        lanes = slice(128 * t, 128 * t + 128)
        geo[0, :, lanes] = ratea * geo[0, :, lanes] + rate0 * geo[1, :, lanes] + pnext * geo[2, :, lanes]

    def patterns(n, _):
        t = n // 8
        block = n - 8 * t
        lanes = pl.ds(pl.multiple_of(128 * t, 128), 128)
        after = block + 1
        bit = jnp.where(after % 2 == 1, 3, jnp.where(after % 4 == 2, 4, 5))
        acc = [jnp.zeros((8, 128), F32)] * 8
        for g in range(FACES_DEV // 8):
            rows = pl.ds(8 * g, 8)
            what = geo[0, rows, lanes]
            geo[0, rows, lanes] = what * sgn[bit, rows, lanes]
            low = [sgn[k, rows, lanes] for k in range(3)]
            for k in range(8):
                if k:
                    what = what * low[0 if k % 2 else (1 if k % 4 else 2)]
                acc[k] = acc[k] + what
        for k in range(8):
            binned[t, pl.ds(pl.multiple_of(64 * block, 8) + 8 * k, 8), :] = acc[k]
        return 0

    def folded(t):
        out = binned[t, pl.ds(0, BINS, stride=8), :]
        for k in range(1, 8):
            out = out + binned[t, pl.ds(k, BINS, stride=8), :]
        return out

    mark("near_wait")
    told(near_sem.at[2], ("gx", 2))
    tell(near_sem.at[4], "gx", 4)
    mark("bins")
    lax.fori_loop(0, 32, patterns, 0, unroll=2)
    mark("pack")
    had = had_v[...]
    for t in range(2):
        both = jnp.concatenate([folded(t), folded(2 + t)], axis=0).T
        hi = both.astype(BF16)
        rest = both - hi.astype(F32)
        mid = rest.astype(BF16)
        lo = (rest - mid.astype(F32)).astype(BF16)
        packed[pl.ds(128 * t, 128), :] = (
            jnp.dot(hi, had, preferred_element_type=F32)
            + jnp.dot(mid, had, preferred_element_type=F32)
            + jnp.dot(lo, had, preferred_element_type=F32)
        )
    told(near_sem.at[4], ("gx", 4))
    tell(near_sem.at[5], "gx", 8)
    told(near_sem.at[3], ("yz", 4))
    ac = []
    for k in range(1, N_YZ):
        peer = lax.rem(yz + k, N_YZ)
        c = pltpu.make_async_remote_copy(
            src_ref=packed.at[pl.ds(pl.multiple_of(32 * peer, 32), 32), :], dst_ref=recv_a.at[k - 1],
            send_sem=as_sem.at[k - 1], recv_sem=ar_sem.at[k - 1], device_id=(gx, peer), device_id_type=MESH,
        )
        c.start()
        ac.append(c)

    mark("finish_a")
    def finish(x, _):
        ca, cb = table_s[0, x], table_s[1, x]
        for t in range(2):
            for h in range(2):
                lanes = pl.ds(128 * t, 128)
                ys = pl.ds(24 * h, 24)
                px, ux, vx, wx, mx = (ca * hal[f, 0, ys, lanes] + cb * hal[f, 1, ys, lanes] for f in range(5))
                p, u, v, w, m = (fld[f, x, t, pl.ds(8 + 24 * h, 24), :] for f in range(5))
                n0, n1, n2, n3 = (grd[q, x, t, ys, :] for q in range(4))
                nxt[0, x, ys, lanes] = p - TIME_STEP * (n0 + m * px + ux)
                nxt[1, x, ys, lanes] = u - TIME_STEP * (n1 + m * ux + u * mx + px)
                nxt[2, x, ys, lanes] = v - TIME_STEP * (n2 + m * vx)
                nxt[3, x, ys, lanes] = w - TIME_STEP * (n3 + m * wx)
        return 0

    def edges():
        for x, k, sign in ((0, 2, DD), (CX - 1, 3, -DD)):
            for t in range(2):
                lanes = pl.ds(128 * t, 128)
                px, ux, vx, wx, mx = ((-TIME_STEP * sign) * hal[f, k, :, lanes] for f in range(5))
                u, m = fld[1, x, t, pl.ds(8, CY), :], fld[4, x, t, pl.ds(8, CY), :]
                nxt[0, x, :, lanes] += m * px + ux
                nxt[1, x, :, lanes] += m * ux + u * mx + px
                nxt[2, x, :, lanes] += m * vx
                nxt[3, x, :, lanes] += m * wx

    lax.fori_loop(0, CX // 2, finish, 0)

    mark("wait_a")
    total = packed[pl.ds(pl.multiple_of(32 * yz, 32), 32), :]
    for k in range(N_YZ - 1):
        ac[k].wait_recv()
        total = total + recv_a[k]
    for g in range(N_GX):
        send_b[g] = total[2 * g : 2 * g + 2]
    mark("far_wait")
    told(near_sem.at[5], ("gx", 8))
    bc = []
    for k in range(1, N_GX):
        peer = lax.rem(gx + k, N_GX)
        c = pltpu.make_async_remote_copy(
            src_ref=send_b.at[peer], dst_ref=recv_b.at[k - 1],
            send_sem=bs_sem.at[k - 1], recv_sem=br_sem.at[k - 1], device_id=(peer, yz), device_id_type=MESH,
        )
        c.start()
        bc.append(c)

    mark("finish_b")
    lax.fori_loop(CX // 2, CX, finish, 0)
    edges()

    mark("wait_b")
    total = send_b[gx]
    for k in range(N_GX - 1):
        bc[k].wait_recv()
        total = total + recv_b[k]
    for h in range(2):
        for h2 in range(2):
            sig[pl.ds(2 * h + h2, 1), :] = total[h : h + 1, BINS * h2 : BINS * h2 + BINS]

    mark("drain")
    for way in range(2):
        @pl.when(sends[way])
        def _():
            for c in xc[way]:
                c.wait_send()

        @pl.when(ysends[way])
        def _():
            for c in yc[way]:
                c.wait_send()
    for c in ac + bc:
        c.wait_send()
    mark(None)


def per_device(state, mean_flow, face_cell, face_normal, face_pos, observer_pos, time_bin):
    n = np.arange(CX)
    table = np.zeros((8, 128), np.float32)
    table[0, :CX] = CC * LAM ** (n + 1.0)
    table[1, :CX] = -CC * LAM ** (CX - n * 1.0)
    table[2, 0] = DD
    table[3, CX - 1] = -DD
    dz = operator(NZ).T.astype(np.float32)
    dz_hi, dz_lo = split2(jnp.asarray(dz))
    dz = jnp.concatenate([dz_hi, dz_hi, dz_lo], axis=0)
    ends = closure(CX, CX * N_GX)
    gray = np.arange(BINS) // 8 * 8
    gray = (gray ^ (gray >> 1) & 56) + ((n := np.arange(BINS) % 8) ^ (n >> 1))
    common = gray[:, None] & np.arange(BINS)[None, :]
    parity = sum((common >> k) & 1 for k in range(6)) % 2
    had = np.kron(np.eye(2), (1.0 - 2.0 * parity) / BINS).astype(np.float32)
    anywhere = pl.BlockSpec(memory_space=pltpu.HBM)
    vm = pltpu.VMEM
    dma = pltpu.SemaphoreType.DMA
    nxt, sig = pl.pallas_call(
        functools.partial(kernel, ends),
        out_shape=(
            vm((4, CX, CY, NZ), F32),
            vm((4, BINS), F32),
        ),
        in_specs=[anywhere] * 11,
        out_specs=(pl.BlockSpec(memory_space=pltpu.VMEM), pl.BlockSpec(memory_space=pltpu.VMEM)),
        scratch_shapes=[
            vm((5, CX, 2, 64, 128), F32),
            vm((5, CX, 2, 64, 128), F32),
            vm((3, CX, CY, NZ), F32),
            vm((5, 4, CY, NZ), F32),
            vm((2, 5, CY, NZ), F32),
            vm((7, FACES_DEV, 128), F32),
            vm((3, FACES_DEV, OBS), F32),
            vm((6, FACES_DEV, OBS), F32),
            vm((1, FACES_DEV), jnp.int32),
            vm((3, FACES_DEV), F32),
            vm((3, FACES_DEV), F32),
            vm((3, OBS), F32),
            vm((FACES_DEV, OBS), jnp.int32),
            vm((3 * NZ, NZ), BF16),
            vm((8, 128), F32),
            vm((128, 128), BF16),
            vm((16, 256), F32),
            vm((8, OBS), F32),
            vm((4, 8 * BINS, 128), F32),
            vm((256, 128), F32),
            vm((N_YZ, 32, 128), F32),
            vm((N_GX, 2, 128), F32),
            vm((N_GX - 1, 2, 128), F32),
            pltpu.SMEM((4, 128), F32),
            pltpu.SMEM((1, FACES_DEV), jnp.int32),
            dma((5, 2)), dma((10,)), dma((2, 7)), dma((2, 7)), dma((2, 3)), dma((2, 3)),
            dma((N_YZ,)), dma((N_YZ,)), dma((N_GX - 1,)), dma((N_GX - 1,)), pltpu.SemaphoreType.REGULAR((6,)),
        ],
        compiler_params=pltpu.CompilerParams(
            collective_id=0, has_side_effects=True, vmem_limit_bytes=57 * 2**20 + 2**19
        ),
    )(
        state, mean_flow, face_cell.reshape(1, FACES_DEV), face_normal, face_pos, observer_pos, time_bin,
        dz, jnp.asarray(table), jnp.asarray(table[:4]), jnp.asarray(had, BF16),
    )

    def write_out(nxt_ref, sig_ref, nxt_out, sig_out, sem):
        copies = [pltpu.make_async_copy(sig_ref, sig_out, sem.at[4])]
        copies += [pltpu.make_async_copy(nxt_ref.at[k], nxt_out.at[k], sem.at[k]) for k in range(4)]
        for c in copies:
            c.start()
        for c in copies:
            c.wait()

    return pl.pallas_call(
        write_out,
        out_shape=(
            jax.ShapeDtypeStruct((4, CX, CY, NZ), F32),
            jax.ShapeDtypeStruct((4, BINS), F32),
        ),
        in_specs=[pl.BlockSpec(memory_space=pltpu.VMEM)] * 2,
        out_specs=(anywhere, anywhere),
        scratch_shapes=[dma((5,))],
        compiler_params=pltpu.CompilerParams(vmem_limit_bytes=2**20),
    )(pltpu.with_memory_space_constraint(nxt, pltpu.VMEM), pltpu.with_memory_space_constraint(sig, pltpu.VMEM))


def solution(mesh):
    return jax.shard_map(
        per_device,
        mesh=mesh,
        in_specs=(
            P(None, "gx", "yz", None),
            P("gx", "yz", None),
            P(("gx", "yz")),
            P(None, ("gx", "yz")),
            P(None, ("gx", "yz")),
            P(),
            P(("gx", "yz"), None),
        ),
        out_specs=(P(None, "gx", "yz", None), P(("gx", "yz"), None)),
        check_vma=False,
    )
```

```python
import functools

import jax
import jax.numpy as jnp
import numpy as np
from jax import lax
from jax.experimental import pallas as pl
from jax.experimental.pallas import tpu as pltpu
from jax.sharding import PartitionSpec as P

CX, CY, NZ = 32, 48, 256
FACES_DEV, OBS, BINS = 192, 512, 64
N_GX, N_YZ = 16, 8
TIME_STEP = 0.25
INV_FOUR_PI = 1.0 / (4.0 * 3.141592653589793)
MESH = pl.DeviceIdType.MESH
F32, BF16 = jnp.float32, jnp.bfloat16

LAM = (-1.0 + np.sqrt(1.0 - 4.0 / 9.0)) / (2.0 / 3.0)
CC, DD = 25.0 / 12.0, -1.0 / 12.0
EDGE = DD / CC


def operator(n):
    a = np.eye(n)
    b = np.zeros((n, n))
    for i in range(n):
        if i == 0:
            a[0, 1] = 2.0
            b[0, :3] = (-2.5, 2.0, 0.5)
        elif i == n - 1:
            a[i, i - 1] = 2.0
            b[i, n - 3 :] = (-0.5, -2.0, 2.5)
        elif i in (1, n - 2):
            a[i, i - 1] = a[i, i + 1] = 0.25
            b[i, i + 1], b[i, i - 1] = 0.75, -0.75
        else:
            a[i, i - 1] = a[i, i + 1] = 1.0 / 3.0
            b[i, i + 1], b[i, i - 1] = 7.0 / 9.0, -7.0 / 9.0
            b[i, i + 2], b[i, i - 2] = 1.0 / 36.0, -1.0 / 36.0
    return np.linalg.solve(a, b)


def closure(n, total):
    lag = np.arange(n)[:, None] - np.arange(n)[None, :]
    inside = np.where(
        lag == 0, 0.0, np.sign(lag) * (CC * LAM ** np.abs(lag) + DD * (np.abs(lag) == 1))
    )
    rest = operator(total)[:n, :n] - inside
    factors = np.stack([CC * LAM ** (np.arange(n) + 1.0), DD * (np.arange(n) == 0)], 1)
    weights = np.linalg.lstsq(factors, rest, rcond=None)[0]
    scale = weights[:, 12] / LAM**12
    return np.concatenate([weights[:, :4] - scale[:, None] * LAM ** np.arange(4.0), scale[:, None]], 1)


def split2(x):
    hi = x.astype(BF16)
    return hi, (x - hi.astype(F32)).astype(BF16)


class Marks:
    def __init__(self):
        self.scope = None

    def __call__(self, name):
        if self.scope is not None:
            self.scope.__exit__(None, None, None)
        self.scope = None if name is None else jax.named_scope(name)
        if self.scope is not None:
            self.scope.__enter__()


def dot3(a, b):
    return (
        jnp.dot(a[0], b[0], preferred_element_type=F32)
        + jnp.dot(a[1], b[0], preferred_element_type=F32)
        + jnp.dot(a[0], b[1], preferred_element_type=F32)
    )


def kernel(
    ends, state, mean, face_cell, normal, pos, obs, tbin, dz, table, table_s_in, had,
    nxt, sig,
    fld, grd, zed, hal, tsum, stg, geo, sgn, face_v, normal_v, pos_v, obs_v, tbin_v, dz_v, table_v, had_v,
    rows_v, seen_v, binned, packed, recv_a, send_b, recv_b, table_s, cell_s,
    ld_sem, in_sem, xs_sem, xr_sem, ys_sem, yr_sem, as_sem, ar_sem, bs_sem, br_sem, near_sem,
):
    mark = Marks()
    gx = lax.axis_index("gx")
    yz = lax.axis_index("yz")

    mark("barrier")
    barrier = pltpu.get_barrier_semaphore()
    def tell(sem, along, step):
        here, count = (gx, N_GX) if along == "gx" else (yz, N_YZ)
        for sign in (1, -1):
            there = here + sign * step

            @pl.when(there < count if sign > 0 else there >= 0)
            def _():
                to = (there, yz) if along == "gx" else (gx, there)
                pl.semaphore_signal(sem, inc=1, device_id=to, device_id_type=MESH)

    def told(sem, *pairs):
        total = 0
        for along, step in pairs:
            here, count = (gx, N_GX) if along == "gx" else (yz, N_YZ)
            total = total + (here >= step).astype(jnp.int32) + (here < count - step).astype(jnp.int32)
        pl.semaphore_wait(sem, total)

    tell(barrier, "gx", 1)
    tell(barrier, "yz", 1)
    mark("start")
    order = (0, 4, 2, 3, 1)
    small = []
    for k, (s, d) in enumerate((
        (obs, obs_v), (tbin, tbin_v), (dz, dz_v), (table, table_v), (table_s_in, table_s),
        (face_cell, cell_s), (face_cell, face_v), (normal, normal_v), (pos, pos_v), (had, had_v),
    )):
        c = pltpu.make_async_copy(s, d, in_sem.at[k])
        c.start()
        small.append(c)

    loads = {}
    for f in order:
        src = mean if f == 4 else state.at[f]
        for t in range(2):
            c = pltpu.make_async_copy(
                src.at[:, :, pl.ds(128 * t, 128)], fld.at[f, :, t, pl.ds(8, CY), :], ld_sem.at[f, t]
            )
            c.start()
            loads[f, t] = c
    mark("barrier_wait")
    told(barrier, ("gx", 1), ("yz", 1))

    mark("issue")
    has_left, has_right = gx > 0, gx < N_GX - 1
    has_low, has_high = yz > 0, yz < N_YZ - 1
    right, left = (lax.rem(gx + 1, N_GX), yz), (lax.rem(gx + N_GX - 1, N_GX), yz)
    high, low = (gx, lax.rem(yz + 1, N_YZ)), (gx, lax.rem(yz + N_YZ - 1, N_YZ))

    def xcopy(src, dst, way, k):
        return pltpu.make_async_remote_copy(
            src_ref=src, dst_ref=dst, send_sem=xs_sem.at[way, k], recv_sem=xr_sem.at[way, k],
            device_id=(right, left)[way], device_id_type=MESH,
        )

    planes, sums = ([], []), ([], [])
    for way, plane in ((0, CX - 1), (1, 0)):
        planes[way].append(xcopy(state.at[:, plane], hal.at[pl.ds(0, 4), 2 + way], way, 0))
        planes[way].append(xcopy(mean.at[plane], hal.at[4, 2 + way], way, 0))
        for f in range(5):
            sums[way].append(xcopy(tsum.at[way, f], hal.at[f, way], way, 1 + f // 4))
    all_planes = [xcopy(tsum.at[way], hal.at[:, 2 + way], way, 0) for way in range(2)]
    all_sums = [
        (xcopy(tsum.at[way, pl.ds(0, 4)], hal.at[pl.ds(0, 4), way], way, 1), sums[way][4]) for way in range(2)
    ]
    tell(near_sem.at[0], "gx", 1)
    tell(near_sem.at[0], "yz", 1)
    sends = (has_right, has_left)
    gets = (has_left, has_right)
    for way in range(2):
        @pl.when(sends[way])
        def _():
            planes[way][0].start()
            planes[way][1].start()

    yc = ([], [])
    for k, f in enumerate((0, 2, 4)):
        for way, (first, there) in enumerate(((8 + CY - 3, 5), (8, 8 + CY))):
            yc[way].append(pltpu.make_async_remote_copy(
                src_ref=fld.at[f, :, :, pl.ds(first, 3), :], dst_ref=fld.at[f, :, :, pl.ds(there, 3), :],
                send_sem=ys_sem.at[way, k], recv_sem=yr_sem.at[way, k],
                device_id=(high, low)[way], device_id_type=MESH,
            ))
    ysends = (has_high, has_low)
    ygets = (has_low, has_high)

    mark("observers")
    to = lax.broadcasted_iota(jnp.int32, (OBS, OBS), 1)
    source = (
        32 * (to & 15) + 4 * (lax.shift_right_logical(to, 4) & 7)
        + 2 * lax.shift_right_logical(to, 8) + (lax.shift_right_logical(to, 7) & 1)
    )
    perm = jnp.where(lax.broadcasted_iota(jnp.int32, (OBS, OBS), 0) == source, 1.0, 0.0).astype(BF16)
    small[0].wait()
    small[1].wait()
    which = jnp.dot(tbin_v[...].astype(F32).astype(BF16), perm, preferred_element_type=F32).astype(jnp.int32)
    for k in range(6):
        sgn[k] = jnp.where((which & (1 << k)) == 0, 1.0, -1.0)
    whole = obs_v[...]
    o_hi = whole.astype(BF16)
    rest = whole - o_hi.astype(F32)
    o_mid = rest.astype(BF16)
    o_lo = (rest - o_mid.astype(F32)).astype(BF16)
    seen_v[pl.ds(0, 3), :] = (
        jnp.dot(o_hi, perm, preferred_element_type=F32)
        + jnp.dot(o_mid, perm, preferred_element_type=F32)
        + jnp.dot(o_lo, perm, preferred_element_type=F32)
    )
    mark("columns")
    for c in small[3:]:
        c.wait()
    cell = face_v[...]
    line = lax.shift_right_logical(cell, 8)
    fx = lax.shift_right_logical(lax.shift_right_logical(line, 7) * 21846, 16)
    fy = line - CY * lax.shift_right_logical(lax.shift_right_logical(line, 4) * 21846, 16)
    fx = fx & (CX - 1)
    fz = cell & 255
    rows_v[...] = jnp.zeros((16, 256), F32)
    rows_v[pl.ds(0, 3), pl.ds(0, FACES_DEV)] = pos_v[...]
    rows_v[pl.ds(3, 3), pl.ds(0, FACES_DEV)] = normal_v[...]
    rows_v[pl.ds(6, 1), pl.ds(0, FACES_DEV)] = fx.astype(F32)
    rows_v[pl.ds(7, 1), pl.ds(0, FACES_DEV)] = fy.astype(F32)
    rows_v[pl.ds(8, 1), pl.ds(0, FACES_DEV)] = fz.astype(F32)
    cols = rows_v[...].T
    col = lambda k: cols[:FACES_DEV, k : k + 1]
    xcol, ycol, zcol = col(6), col(7), col(8)
    lane = lax.broadcasted_iota(jnp.int32, (FACES_DEV, 128), 1).astype(F32)
    zlane = zcol - jnp.where(zcol >= 128.0, 128.0, 0.0)
    zmask = zlane == lane
    pick = lambda a: jnp.sum(jnp.where(zmask, a, 0.0), axis=1, keepdims=True)
    xmask = xcol == lane
    coef = [
        jnp.sum(jnp.where(xmask, table_v[pl.ds(k, 1), :], 0.0), axis=1, keepdims=True) for k in range(4)
    ]
    upper = lane >= CY
    hit = jnp.where(upper, lane - CY, lane) == ycol
    weights = [
        jnp.where(hit, jnp.where(upper, coef[2 * k + 1], coef[2 * k]), 0.0) for k in range(2)
    ]
    mark("geometry")
    for t in range(4):
        lanes = slice(128 * t, 128 * t + 128)
        dx = seen_v[0:1, lanes] - col(0)
        dy_ = seen_v[1:2, lanes] - col(1)
        dz_ = seen_v[2:3, lanes] - col(2)
        inv = lax.rsqrt(dx * dx + dy_ * dy_ + dz_ * dz_)
        nr = (col(3) * dx + col(4) * dy_ + col(5) * dz_) * inv
        q1 = INV_FOUR_PI * inv
        geo[0, :, lanes] = q1
        geo[1, :, lanes] = q1 * nr
        geo[2, :, lanes] = q1 * nr * inv

    mark("wait_load")
    for f in order[:3]:
        loads[f, 0].wait()
        loads[f, 1].wait()
        for way in range(2):
            @pl.when(ysends[way])
            def _():
                yc[way][f // 2].start()

    mark("sweeps")
    small[2].wait()

    def along_z(j):
        q = j // 2
        x0 = 16 * (j - 2 * q)
        f = jnp.where(q == 0, 0, q + 2)
        v = fld[f, pl.ds(x0, 16), :, pl.ds(8, CY), :]
        v = jnp.concatenate([v[:, 0], v[:, 1]], axis=-1).reshape(16 * CY, NZ)
        hi, lo = split2(v)
        out = jnp.dot(jnp.concatenate([hi, lo, hi], axis=1), dz_v[...], preferred_element_type=F32)
        zed[q, pl.ds(x0, 16)] = out.reshape(16, CY, NZ)

    jobs = 0
    for f, per_half in zip((0, 3, 2, 1, 4), (1, 1, 1, 0, 0)):
        if f not in (0, 2, 4):
            loads[f, 0].wait()
            loads[f, 1].wait()

        def sweep(t, _, f=f, per_half=per_half, jobs=jobs):
            zero = jnp.zeros((CY, 128), F32)
            at = lambda i: fld[f, i, t, pl.ds(8, CY), :] if 0 <= i < CX else zero
            up, down, v_old, w_old = zero, zero, zero, zero
            v, w = at(0), at(CX - 1)
            for i in range(CX):
                if i * per_half // CX != (i - 1) * per_half // CX:
                    along_z(jobs + per_half * t + i * per_half // CX)
                k = CX - 1 - i
                v_new, w_new = at(i + 1), at(k - 1)
                if i < CX // 2:
                    grd[f, i, t, pl.ds(0, CY), :] = up
                    grd[f, k, t, pl.ds(0, CY), :] = down
                else:
                    grd[f, i, t, pl.ds(0, CY), :] = (up - grd[f, i, t, pl.ds(0, CY), :]) + EDGE * (v_old - v_new)
                    grd[f, k, t, pl.ds(0, CY), :] = (grd[f, k, t, pl.ds(0, CY), :] - down) + EDGE * (w_new - w_old)
                up_sum, down_sum = up + v, down + w
                up, down = LAM * up_sum, LAM * down_sum
                v_old, v, w_old, w = v, v_new, w, w_new
            lanes = pl.ds(pl.multiple_of(128 * t, 128), 128)
            tsum[0, f, :, lanes] = up_sum
            tsum[1, f, :, lanes] = down_sum
            return 0

        lax.fori_loop(0, 2, sweep, 0)
        if f == 0:
            told(near_sem.at[0], ("gx", 1), ("yz", 1))
            tell(near_sem.at[1], "yz", 2)
            tell(near_sem.at[2], "gx", 2)
        jobs += 2 * per_half
        for way in range(2):
            @pl.when(sends[way])
            def _():
                sums[way][f].start()

    mark("ends")
    for way, there in ((0, jnp.logical_not(has_left)), (1, jnp.logical_not(has_right))):
        @pl.when(there)
        def _():
            def close(n, _):
                f, t = n // 2, n % 2
                lanes = pl.ds(pl.multiple_of(128 * t, 128), 128)
                far = tsum[1 - way, f, :, lanes]
                one, two = float(ends[0, 4]) * far, float(ends[1, 4]) * far
                for i in range(4):
                    v = fld[f, i if way == 0 else CX - 1 - i, t, pl.ds(8, CY), :]
                    one = one + float(ends[0, i]) * v
                    two = two + float(ends[1, i]) * v
                hal[f, way, :, lanes] = one
                hal[f, 2 + way, :, lanes] = two
                return 0

            lax.fori_loop(0, 10, close, 0)
    for way, there, row in ((0, jnp.logical_not(has_low), 5), (1, jnp.logical_not(has_high), 8 + CY)):
        @pl.when(there)
        def _():
            for f in (0, 2, 4):
                fld[f, :, :, pl.ds(row, 3), :] = jnp.zeros((CX, 2, 3, 128), F32)

    mark("wait_y")
    for way in range(2):
        @pl.when(ygets[way])
        def _():
            for k in range(3):
                yc[way][k].wait_recv()

    mark("local")
    def local(n, _):
        for j in range(2):
            for t in range(2):
                x = 2 * n + j
                at = lambda f, s=0: fld[f, x, t, pl.ds(8 + s, CY), :]
                pz, wz, mz = (zed[q, x, :, 128 * t : 128 * t + 128] for q in range(3))

                def dy(f):
                    return (
                        0.75 * (at(f, 1) - at(f, -1)) - 0.15 * (at(f, 2) - at(f, -2))
                        + (1.0 / 60.0) * (at(f, 3) - at(f, -3))
                    )

                px, ux, vx, wx, mx = (grd[f, x, t, pl.ds(0, CY), :] for f in range(5))
                m, u, v, w = at(4), at(1), at(2), at(3)
                cm = CC * m
                grd[0, x, t, pl.ds(0, CY), :] = cm * px + CC * ux + dy(2) + wz
                grd[1, x, t, pl.ds(0, CY), :] = cm * ux + CC * (u * mx + px) + v * dy(4) + w * mz
                grd[2, x, t, pl.ds(0, CY), :] = cm * vx + dy(0)
                grd[3, x, t, pl.ds(0, CY), :] = cm * wx + pz
        return 0

    lax.fori_loop(0, CX // 2, local, 0)

    mark("gather")
    corner = gx * (CX * CY * N_YZ) + yz * CY
    grd_rows = grd.reshape(5, CX * 2 * 64, 128)
    fld_rows = fld.reshape(5, CX * 2 * 64, 128)

    def gather(n, _):
        for k in range(8):
            j = n * 8 + k
            cell = cell_s[0, j]
            line = jnp.maximum(lax.shift_right_logical(cell, 8) - corner, 0)
            x = lax.shift_right_logical(lax.shift_right_logical(line, 7) * 86, 8)
            row = line - 256 * x + (lax.shift_right_logical(cell, 1) & 64)
            for q in range(4):
                stg[q, pl.ds(j, 1), :] = grd_rows[q, pl.ds(row, 1), :]
            for q, f in ((4, 0), (5, 1), (6, 4)):
                stg[q, pl.ds(j, 1), :] = fld_rows[f, pl.ds(row + 8, 1), :]
        return 0

    lax.fori_loop(0, FACES_DEV // 8, gather, 0)

    told(near_sem.at[1], ("yz", 2))
    tell(near_sem.at[3], "yz", 4)
    told(near_sem.at[2], ("gx", 2))
    tell(near_sem.at[4], "gx", 4)
    mark("picks")
    face0 = [pick(stg[q]) for q in range(7)]
    fp, fu, fm = face0[4], face0[5], face0[6]
    fn = [col(3 + k) for k in range(3)]
    to0 = (fm, jnp.ones_like(fm))
    toa = (fn[0], fn[0] * fm, fn[1] * fm, fn[2] * fm, fn[0] * fu)

    def left_of(k, scales):
        out = []
        for scale in scales:
            hi, lo = split2(weights[k] * scale)
            out += [hi, lo, hi]
        return jnp.concatenate(out, axis=1)

    lefts = [(left_of(k, to0), left_of(k, toa[:4]), left_of(k, toa[4:])) for k in range(2)]

    mark("wait_x")
    for way in range(2):
        @pl.when(gets[way])
        def _():
            all_planes[way].wait_recv()

    zwide = lax.broadcasted_iota(jnp.int32, (FACES_DEV, NZ), 1).astype(F32) == zcol
    pad = jnp.zeros((128 - 2 * CY, NZ), BF16)

    def rights(k, fields):
        out = []
        for f in fields:
            hi, lo = split2(hal[f, pl.ds(2 * k, 2)].reshape(2 * CY, NZ))
            out += [hi, pad, hi, pad, lo, pad]
        return out

    def times(a, right):
        return jnp.dot(a, jnp.concatenate(right, axis=0), preferred_element_type=F32)

    def most_at_faces(k):
        right = rights(k, range(4))
        return times(lefts[k][0], right[:12]), times(lefts[k][1], right)

    add0, adda = most_at_faces(1)
    adda = adda + times(lefts[1][2], rights(1, (4,)))
    mark("wait_t")
    for way in range(2):
        @pl.when(gets[way])
        def _():
            all_sums[way][0].wait_recv()
    more0, morea = most_at_faces(0)
    add0, adda = add0 + more0, adda + morea
    mark("wait_u")
    for way in range(2):
        @pl.when(gets[way])
        def _():
            all_sums[way][1].wait_recv()
    mark("near")
    adda = adda + times(lefts[0][2], rights(0, (4,)))
    pickw = lambda a: jnp.sum(jnp.where(zwide, a, 0.0), axis=1, keepdims=True)
    rate0 = -(face0[0] + pickw(add0))
    ratea = -(col(3) * face0[1] + col(4) * face0[2] + col(5) * face0[3] + pickw(adda))
    pnext = fp + TIME_STEP * rate0
    for t in range(4):
        lanes = slice(128 * t, 128 * t + 128)
        geo[0, :, lanes] = ratea * geo[0, :, lanes] + rate0 * geo[1, :, lanes] + pnext * geo[2, :, lanes]

    def patterns(n, _):
        t = n // 8
        block = n - 8 * t
        lanes = pl.ds(pl.multiple_of(128 * t, 128), 128)
        after = block + 1
        bit = jnp.where(after % 2 == 1, 3, jnp.where(after % 4 == 2, 4, 5))
        acc = [jnp.zeros((8, 128), F32)] * 8
        for g in range(FACES_DEV // 8):
            rows = pl.ds(8 * g, 8)
            what = geo[0, rows, lanes]
            geo[0, rows, lanes] = what * sgn[bit, rows, lanes]
            low = [sgn[k, rows, lanes] for k in range(3)]
            for k in range(8):
                if k:
                    what = what * low[0 if k % 2 else (1 if k % 4 else 2)]
                acc[k] = acc[k] + what
        for k in range(8):
            binned[t, pl.ds(pl.multiple_of(64 * block, 8) + 8 * k, 8), :] = acc[k]
        return 0

    def folded(t):
        out = binned[t, pl.ds(0, BINS, stride=8), :]
        for k in range(1, 8):
            out = out + binned[t, pl.ds(k, BINS, stride=8), :]
        return out

    mark("near_wait")
    told(near_sem.at[4], ("gx", 4))
    tell(near_sem.at[5], "gx", 8)
    def acopy(half, k):
        peer = lax.rem(yz + k, N_YZ)
        return pltpu.make_async_remote_copy(
            src_ref=packed.at[half, pl.ds(pl.multiple_of(16 * peer, 16), 16), :], dst_ref=recv_a.at[half, k - 1],
            send_sem=as_sem.at[half], recv_sem=ar_sem.at[half], device_id=(gx, peer), device_id_type=MESH,
        )

    def bcopy(k):
        peer = lax.rem(gx + k, N_GX)
        return pltpu.make_async_remote_copy(
            src_ref=send_b.at[peer], dst_ref=recv_b.at[k - 1],
            send_sem=bs_sem, recv_sem=br_sem, device_id=(peer, yz), device_id_type=MESH,
        )

    def whole(ref, send_sem, recv_sem, to):
        return pltpu.make_async_remote_copy(
            src_ref=ref, dst_ref=ref, send_sem=send_sem, recv_sem=recv_sem, device_id=to, device_id_type=MESH,
        )

    awhole = [whole(recv_a.at[half], as_sem.at[half], ar_sem.at[half], high) for half in range(2)]
    bwhole = whole(recv_b, bs_sem, br_sem, right)

    told(near_sem.at[3], ("yz", 4))
    for half in range(2):
        mark(f"bins{half}")
        lax.fori_loop(16 * half, 16 * half + 16, patterns, 0, unroll=2)
        mark(f"pack{half}")
        had = had_v[...]
        both = jnp.concatenate([folded(2 * half), folded(2 * half + 1)], axis=0).T
        hi = both.astype(BF16)
        rest = both - hi.astype(F32)
        mid = rest.astype(BF16)
        lo = (rest - mid.astype(F32)).astype(BF16)
        packed[half] = (
            jnp.dot(hi, had, preferred_element_type=F32)
            + jnp.dot(mid, had, preferred_element_type=F32)
            + jnp.dot(lo, had, preferred_element_type=F32)
        )
        for k in (4, 3, 5, 2, 6, 1, 7):
            acopy(half, k).start()

    mark("finish_a")
    def finish(x, _):
        ca, cb = table_s[0, x], table_s[1, x]
        for t in range(2):
            for h in range(2):
                lanes = pl.ds(128 * t, 128)
                ys = pl.ds(24 * h, 24)
                px, ux, vx, wx, mx = (ca * hal[f, 0, ys, lanes] + cb * hal[f, 1, ys, lanes] for f in range(5))
                p, u, v, w, m = (fld[f, x, t, pl.ds(8 + 24 * h, 24), :] for f in range(5))
                n0, n1, n2, n3 = (grd[q, x, t, ys, :] for q in range(4))
                nxt[0, x, ys, lanes] = p - TIME_STEP * (n0 + m * px + ux)
                nxt[1, x, ys, lanes] = u - TIME_STEP * (n1 + m * ux + u * mx + px)
                nxt[2, x, ys, lanes] = v - TIME_STEP * (n2 + m * vx)
                nxt[3, x, ys, lanes] = w - TIME_STEP * (n3 + m * wx)
        return 0

    def edges():
        for x, k, sign in ((0, 2, DD), (CX - 1, 3, -DD)):
            for t in range(2):
                lanes = pl.ds(128 * t, 128)
                px, ux, vx, wx, mx = ((-TIME_STEP * sign) * hal[f, k, :, lanes] for f in range(5))
                u, m = fld[1, x, t, pl.ds(8, CY), :], fld[4, x, t, pl.ds(8, CY), :]
                nxt[0, x, :, lanes] += m * px + ux
                nxt[1, x, :, lanes] += m * ux + u * mx + px
                nxt[2, x, :, lanes] += m * vx
                nxt[3, x, :, lanes] += m * wx

    lax.fori_loop(0, CX // 2, finish, 0)

    mark("wait_a")
    for half in range(2):
        awhole[half].wait_recv()
        total = packed[half, pl.ds(pl.multiple_of(16 * yz, 16), 16), :]
        for k in range(N_YZ - 1):
            total = total + recv_a[half, k]
        for g in range(N_GX):
            send_b[g, pl.ds(half, 1), :] = total[g : g + 1]
    mark("far_wait")
    told(near_sem.at[5], ("gx", 8))
    hops = lambda k: min(k // 4, 4 - k // 4) + min(k % 4, 4 - k % 4)
    for k in sorted(range(1, N_GX), key=hops, reverse=True):
        bcopy(k).start()

    mark("finish_b")
    lax.fori_loop(CX // 2, CX, finish, 0)
    edges()

    mark("wait_b")
    bwhole.wait_recv()
    total = send_b[gx]
    for k in range(N_GX - 1):
        total = total + recv_b[k]
    for h in range(2):
        for h2 in range(2):
            sig[pl.ds(2 * h + h2, 1), :] = total[h : h + 1, BINS * h2 : BINS * h2 + BINS]

    mark("drain")
    for way in range(2):
        @pl.when(sends[way])
        def _():
            for c in (all_planes[way], *all_sums[way]):
                c.wait_send()

        @pl.when(ysends[way])
        def _():
            for c in yc[way]:
                c.wait_send()
    for c in (*awhole, bwhole):
        c.wait_send()
    mark(None)


def per_device(state, mean_flow, face_cell, face_normal, face_pos, observer_pos, time_bin):
    n = np.arange(CX)
    table = np.zeros((8, 128), np.float32)
    table[0, :CX] = CC * LAM ** (n + 1.0)
    table[1, :CX] = -CC * LAM ** (CX - n * 1.0)
    table[2, 0] = DD
    table[3, CX - 1] = -DD
    dz = operator(NZ).T.astype(np.float32)
    dz_hi, dz_lo = split2(jnp.asarray(dz))
    dz = jnp.concatenate([dz_hi, dz_hi, dz_lo], axis=0)
    ends = closure(CX, CX * N_GX)
    gray = np.arange(BINS) // 8 * 8
    gray = (gray ^ (gray >> 1) & 56) + ((n := np.arange(BINS) % 8) ^ (n >> 1))
    common = gray[:, None] & np.arange(BINS)[None, :]
    parity = sum((common >> k) & 1 for k in range(6)) % 2
    had = np.kron(np.eye(2), (1.0 - 2.0 * parity) / BINS).astype(np.float32)
    anywhere = pl.BlockSpec(memory_space=pltpu.HBM)
    vm = pltpu.VMEM
    dma = pltpu.SemaphoreType.DMA
    nxt, sig = pl.pallas_call(
        functools.partial(kernel, ends),
        out_shape=(
            vm((4, CX, CY, NZ), F32),
            vm((4, BINS), F32),
        ),
        in_specs=[anywhere] * 11,
        out_specs=(pl.BlockSpec(memory_space=pltpu.VMEM), pl.BlockSpec(memory_space=pltpu.VMEM)),
        scratch_shapes=[
            vm((5, CX, 2, 64, 128), F32),
            vm((5, CX, 2, 64, 128), F32),
            vm((3, CX, CY, NZ), F32),
            vm((5, 4, CY, NZ), F32),
            vm((2, 5, CY, NZ), F32),
            vm((7, FACES_DEV, 128), F32),
            vm((3, FACES_DEV, OBS), F32),
            vm((6, FACES_DEV, OBS), F32),
            vm((1, FACES_DEV), jnp.int32),
            vm((3, FACES_DEV), F32),
            vm((3, FACES_DEV), F32),
            vm((3, OBS), F32),
            vm((FACES_DEV, OBS), jnp.int32),
            vm((3 * NZ, NZ), BF16),
            vm((8, 128), F32),
            vm((128, 128), BF16),
            vm((16, 256), F32),
            vm((8, OBS), F32),
            vm((4, 8 * BINS, 128), F32),
            vm((2, 128, 128), F32),
            vm((2, N_YZ - 1, 16, 128), F32),
            vm((N_GX, 2, 128), F32),
            vm((N_GX - 1, 2, 128), F32),
            pltpu.SMEM((4, 128), F32),
            pltpu.SMEM((1, FACES_DEV), jnp.int32),
            dma((5, 2)), dma((10,)), dma((2, 3)), dma((2, 3)), dma((2, 3)), dma((2, 3)),
            dma((2,)), dma((2,)), dma(()), dma(()), pltpu.SemaphoreType.REGULAR((6,)),
        ],
        compiler_params=pltpu.CompilerParams(
            collective_id=0, has_side_effects=True, vmem_limit_bytes=57 * 2**20 + 2**19
        ),
    )(
        state, mean_flow, face_cell.reshape(1, FACES_DEV), face_normal, face_pos, observer_pos, time_bin,
        dz, jnp.asarray(table), jnp.asarray(table[:4]), jnp.asarray(had, BF16),
    )

    def write_out(nxt_ref, sig_ref, nxt_out, sig_out, sem):
        copies = [pltpu.make_async_copy(sig_ref, sig_out, sem.at[4])]
        copies += [pltpu.make_async_copy(nxt_ref.at[k], nxt_out.at[k], sem.at[k]) for k in range(4)]
        for c in copies:
            c.start()
        for c in copies:
            c.wait()

    return pl.pallas_call(
        write_out,
        out_shape=(
            jax.ShapeDtypeStruct((4, CX, CY, NZ), F32),
            jax.ShapeDtypeStruct((4, BINS), F32),
        ),
        in_specs=[pl.BlockSpec(memory_space=pltpu.VMEM)] * 2,
        out_specs=(anywhere, anywhere),
        scratch_shapes=[dma((5,))],
        compiler_params=pltpu.CompilerParams(vmem_limit_bytes=2**20),
    )(pltpu.with_memory_space_constraint(nxt, pltpu.VMEM), pltpu.with_memory_space_constraint(sig, pltpu.VMEM))


def solution(mesh):
    return jax.shard_map(
        per_device,
        mesh=mesh,
        in_specs=(
            P(None, "gx", "yz", None),
            P("gx", "yz", None),
            P(("gx", "yz")),
            P(None, ("gx", "yz")),
            P(None, ("gx", "yz")),
            P(),
            P(("gx", "yz"), None),
        ),
        out_specs=(P(None, "gx", "yz", None), P(("gx", "yz"), None)),
        check_vma=False,
    )
```

```python
import functools

import jax
import jax.numpy as jnp
import numpy as np
from jax import lax
from jax.experimental import pallas as pl
from jax.experimental.pallas import tpu as pltpu
from jax.sharding import PartitionSpec as P

CX, CY, NZ = 32, 48, 256
FACES_DEV, OBS, BINS = 192, 512, 64
N_GX, N_YZ = 16, 8
TIME_STEP = 0.25
INV_FOUR_PI = 1.0 / (4.0 * 3.141592653589793)
MESH = pl.DeviceIdType.MESH
F32, BF16 = jnp.float32, jnp.bfloat16

LAM = (-1.0 + np.sqrt(1.0 - 4.0 / 9.0)) / (2.0 / 3.0)
CC, DD = 25.0 / 12.0, -1.0 / 12.0
EDGE = DD / CC


def operator(n):
    a = np.eye(n)
    b = np.zeros((n, n))
    for i in range(n):
        if i == 0:
            a[0, 1] = 2.0
            b[0, :3] = (-2.5, 2.0, 0.5)
        elif i == n - 1:
            a[i, i - 1] = 2.0
            b[i, n - 3 :] = (-0.5, -2.0, 2.5)
        elif i in (1, n - 2):
            a[i, i - 1] = a[i, i + 1] = 0.25
            b[i, i + 1], b[i, i - 1] = 0.75, -0.75
        else:
            a[i, i - 1] = a[i, i + 1] = 1.0 / 3.0
            b[i, i + 1], b[i, i - 1] = 7.0 / 9.0, -7.0 / 9.0
            b[i, i + 2], b[i, i - 2] = 1.0 / 36.0, -1.0 / 36.0
    return np.linalg.solve(a, b)


def closure(n, total):
    lag = np.arange(n)[:, None] - np.arange(n)[None, :]
    inside = np.where(
        lag == 0, 0.0, np.sign(lag) * (CC * LAM ** np.abs(lag) + DD * (np.abs(lag) == 1))
    )
    rest = operator(total)[:n, :n] - inside
    factors = np.stack([CC * LAM ** (np.arange(n) + 1.0), DD * (np.arange(n) == 0)], 1)
    weights = np.linalg.lstsq(factors, rest, rcond=None)[0]
    scale = weights[:, 12] / LAM**12
    return np.concatenate([weights[:, :4] - scale[:, None] * LAM ** np.arange(4.0), scale[:, None]], 1)


def split2(x):
    hi = x.astype(BF16)
    return hi, (x - hi.astype(F32)).astype(BF16)


class Marks:
    def __init__(self):
        self.scope = None

    def __call__(self, name):
        if self.scope is not None:
            self.scope.__exit__(None, None, None)
        self.scope = None if name is None else jax.named_scope(name)
        if self.scope is not None:
            self.scope.__enter__()


def dot3(a, b):
    return (
        jnp.dot(a[0], b[0], preferred_element_type=F32)
        + jnp.dot(a[1], b[0], preferred_element_type=F32)
        + jnp.dot(a[0], b[1], preferred_element_type=F32)
    )


def kernel(
    ends, state, mean, face_cell, normal, pos, obs, tbin, dz, table, table_s_in, had,
    nxt, sig,
    fld, grd, zed, hal, tsum, stg, geo, sgn, face_v, normal_v, pos_v, obs_v, tbin_v, dz_v, table_v, had_v,
    rows_v, seen_v, binned, packed, recv_a, send_b, recv_b, table_s, cell_s,
    ld_sem, in_sem, xs_sem, xr_sem, ys_sem, yr_sem, as_sem, ar_sem, bs_sem, br_sem, near_sem,
):
    mark = Marks()
    gx = lax.axis_index("gx")
    yz = lax.axis_index("yz")

    mark("barrier")
    barrier = pltpu.get_barrier_semaphore()
    def tell(sem, along, step):
        here, count = (gx, N_GX) if along == "gx" else (yz, N_YZ)
        for sign in (1, -1):
            there = here + sign * step

            @pl.when(there < count if sign > 0 else there >= 0)
            def _():
                to = (there, yz) if along == "gx" else (gx, there)
                pl.semaphore_signal(sem, inc=1, device_id=to, device_id_type=MESH)

    def told(sem, *pairs):
        total = 0
        for along, step in pairs:
            here, count = (gx, N_GX) if along == "gx" else (yz, N_YZ)
            total = total + (here >= step).astype(jnp.int32) + (here < count - step).astype(jnp.int32)
        pl.semaphore_wait(sem, total)

    tell(barrier, "gx", 1)
    tell(barrier, "yz", 1)
    mark("start")
    order = (0, 4, 2, 3, 1)
    small = []
    for k, (s, d) in enumerate((
        (obs, obs_v), (tbin, tbin_v), (dz, dz_v), (table, table_v), (table_s_in, table_s),
        (face_cell, cell_s), (face_cell, face_v), (normal, normal_v), (pos, pos_v), (had, had_v),
    )):
        c = pltpu.make_async_copy(s, d, in_sem.at[k])
        c.start()
        small.append(c)

    loads = {}
    for f in order:
        src = mean if f == 4 else state.at[f]
        for t in range(2):
            c = pltpu.make_async_copy(
                src.at[:, :, pl.ds(128 * t, 128)], fld.at[f, :, t, pl.ds(8, CY), :], ld_sem.at[f, t]
            )
            c.start()
            loads[f, t] = c
    mark("barrier_wait")
    told(barrier, ("gx", 1), ("yz", 1))

    mark("issue")
    has_left, has_right = gx > 0, gx < N_GX - 1
    has_low, has_high = yz > 0, yz < N_YZ - 1
    right, left = (lax.rem(gx + 1, N_GX), yz), (lax.rem(gx + N_GX - 1, N_GX), yz)
    high, low = (gx, lax.rem(yz + 1, N_YZ)), (gx, lax.rem(yz + N_YZ - 1, N_YZ))

    def xcopy(src, dst, way, k):
        return pltpu.make_async_remote_copy(
            src_ref=src, dst_ref=dst, send_sem=xs_sem.at[way, k], recv_sem=xr_sem.at[way, k],
            device_id=(right, left)[way], device_id_type=MESH,
        )

    planes, sums = ([], []), ([], [])
    for way, plane in ((0, CX - 1), (1, 0)):
        planes[way].append(xcopy(state.at[:, plane], hal.at[pl.ds(0, 4), 2 + way], way, 0))
        planes[way].append(xcopy(mean.at[plane], hal.at[4, 2 + way], way, 0))
        for f in range(5):
            sums[way].append(xcopy(tsum.at[way, f], hal.at[f, way], way, 1 + f // 4))
    all_planes = [xcopy(tsum.at[way], hal.at[:, 2 + way], way, 0) for way in range(2)]
    all_sums = [
        (xcopy(tsum.at[way, pl.ds(0, 4)], hal.at[pl.ds(0, 4), way], way, 1), sums[way][4]) for way in range(2)
    ]
    tell(near_sem.at[0], "gx", 1)
    tell(near_sem.at[0], "yz", 1)
    sends = (has_right, has_left)
    gets = (has_left, has_right)
    for way in range(2):
        @pl.when(sends[way])
        def _():
            planes[way][0].start()
            planes[way][1].start()


    yc = ([], [])
    for k, f in enumerate((0, 2, 4)):
        for way, (first, there) in enumerate(((8 + CY - 3, 5), (8, 8 + CY))):
            yc[way].append(pltpu.make_async_remote_copy(
                src_ref=fld.at[f, :, :, pl.ds(first, 3), :], dst_ref=fld.at[f, :, :, pl.ds(there, 3), :],
                send_sem=ys_sem.at[way], recv_sem=yr_sem.at[way],
                device_id=(high, low)[way], device_id_type=MESH,
            ))
    yall = [
        pltpu.make_async_remote_copy(
            src_ref=fld.at[pl.ds(0, 3), :, :, pl.ds(row, 3), :], dst_ref=fld.at[pl.ds(0, 3), :, :, pl.ds(row, 3), :],
            send_sem=ys_sem.at[way], recv_sem=yr_sem.at[way], device_id=(high, low)[way], device_id_type=MESH,
        )
        for way, row in ((0, 5), (1, 8 + CY))
    ]
    ysends = (has_high, has_low)
    ygets = (has_low, has_high)

    def send_y(f):
        loads[f, 0].wait()
        loads[f, 1].wait()
        for way in range(2):
            @pl.when(ysends[way])
            def _():
                yc[way][f // 2].start()

    mark("observers")
    to = lax.broadcasted_iota(jnp.int32, (OBS, OBS), 1)
    source = (
        32 * (to & 15) + 4 * (lax.shift_right_logical(to, 4) & 7)
        + 2 * lax.shift_right_logical(to, 8) + (lax.shift_right_logical(to, 7) & 1)
    )
    perm = jnp.where(lax.broadcasted_iota(jnp.int32, (OBS, OBS), 0) == source, 1.0, 0.0).astype(BF16)
    small[0].wait()
    small[1].wait()
    which = jnp.dot(tbin_v[...].astype(F32).astype(BF16), perm, preferred_element_type=F32).astype(jnp.int32)
    for k in range(6):
        sgn[k] = jnp.where((which & (1 << k)) == 0, 1.0, -1.0)
    whole = obs_v[...]
    o_hi = whole.astype(BF16)
    rest = whole - o_hi.astype(F32)
    o_mid = rest.astype(BF16)
    o_lo = (rest - o_mid.astype(F32)).astype(BF16)
    seen_v[pl.ds(0, 3), :] = (
        jnp.dot(o_hi, perm, preferred_element_type=F32)
        + jnp.dot(o_mid, perm, preferred_element_type=F32)
        + jnp.dot(o_lo, perm, preferred_element_type=F32)
    )
    send_y(0)
    mark("columns")
    for c in small[3:]:
        c.wait()
    cell = face_v[...]
    line = lax.shift_right_logical(cell, 8)
    fx = lax.shift_right_logical(lax.shift_right_logical(line, 7) * 21846, 16)
    fy = line - CY * lax.shift_right_logical(lax.shift_right_logical(line, 4) * 21846, 16)
    fx = fx & (CX - 1)
    fz = cell & 255
    rows_v[...] = jnp.zeros((16, 256), F32)
    rows_v[pl.ds(0, 3), pl.ds(0, FACES_DEV)] = pos_v[...]
    rows_v[pl.ds(3, 3), pl.ds(0, FACES_DEV)] = normal_v[...]
    rows_v[pl.ds(6, 1), pl.ds(0, FACES_DEV)] = fx.astype(F32)
    rows_v[pl.ds(7, 1), pl.ds(0, FACES_DEV)] = fy.astype(F32)
    rows_v[pl.ds(8, 1), pl.ds(0, FACES_DEV)] = fz.astype(F32)
    cols = rows_v[...].T
    col = lambda k: cols[:FACES_DEV, k : k + 1]
    xcol, ycol, zcol = col(6), col(7), col(8)
    lane = lax.broadcasted_iota(jnp.int32, (FACES_DEV, 128), 1).astype(F32)
    zlane = zcol - jnp.where(zcol >= 128.0, 128.0, 0.0)
    zmask = zlane == lane
    pick = lambda a: jnp.sum(jnp.where(zmask, a, 0.0), axis=1, keepdims=True)
    xmask = xcol == lane
    coef = [
        jnp.sum(jnp.where(xmask, table_v[pl.ds(k, 1), :], 0.0), axis=1, keepdims=True) for k in range(4)
    ]
    upper = lane >= CY
    hit = jnp.where(upper, lane - CY, lane) == ycol
    weights = [
        jnp.where(hit, jnp.where(upper, coef[2 * k + 1], coef[2 * k]), 0.0) for k in range(2)
    ]
    send_y(4)
    mark("geometry")
    for t in range(4):
        lanes = slice(128 * t, 128 * t + 128)
        dx = seen_v[0:1, lanes] - col(0)
        dy_ = seen_v[1:2, lanes] - col(1)
        dz_ = seen_v[2:3, lanes] - col(2)
        inv = lax.rsqrt(dx * dx + dy_ * dy_ + dz_ * dz_)
        nr = (col(3) * dx + col(4) * dy_ + col(5) * dz_) * inv
        q1 = INV_FOUR_PI * inv
        geo[0, :, lanes] = q1
        geo[1, :, lanes] = q1 * nr
        geo[2, :, lanes] = q1 * nr * inv

    send_y(2)
    mark("sweeps")
    small[2].wait()

    def along_z(j):
        q = j // 2
        x0 = 16 * (j - 2 * q)
        f = jnp.where(q == 0, 0, q + 2)
        v = fld[f, pl.ds(x0, 16), :, pl.ds(8, CY), :]
        v = jnp.concatenate([v[:, 0], v[:, 1]], axis=-1).reshape(16 * CY, NZ)
        hi, lo = split2(v)
        out = jnp.dot(jnp.concatenate([hi, lo, hi], axis=1), dz_v[...], preferred_element_type=F32)
        zed[q, pl.ds(x0, 16)] = out.reshape(16, CY, NZ)

    jobs = 0
    for f, per_half in zip((0, 3, 2, 1, 4), (1, 1, 1, 0, 0)):
        if f not in (0, 2, 4):
            loads[f, 0].wait()
            loads[f, 1].wait()

        def sweep(t, _, f=f, per_half=per_half, jobs=jobs):
            zero = jnp.zeros((CY, 128), F32)
            at = lambda i: fld[f, i, t, pl.ds(8, CY), :] if 0 <= i < CX else zero
            up, down, v_old, w_old = zero, zero, zero, zero
            v, w = at(0), at(CX - 1)
            for i in range(CX):
                if i * per_half // CX != (i - 1) * per_half // CX:
                    along_z(jobs + per_half * t + i * per_half // CX)
                k = CX - 1 - i
                v_new, w_new = at(i + 1), at(k - 1)
                if i < CX // 2:
                    grd[f, i, t, pl.ds(0, CY), :] = up
                    grd[f, k, t, pl.ds(0, CY), :] = down
                else:
                    grd[f, i, t, pl.ds(0, CY), :] = (up - grd[f, i, t, pl.ds(0, CY), :]) + EDGE * (v_old - v_new)
                    grd[f, k, t, pl.ds(0, CY), :] = (grd[f, k, t, pl.ds(0, CY), :] - down) + EDGE * (w_new - w_old)
                up_sum, down_sum = up + v, down + w
                up, down = LAM * up_sum, LAM * down_sum
                v_old, v, w_old, w = v, v_new, w, w_new
            lanes = pl.ds(pl.multiple_of(128 * t, 128), 128)
            tsum[0, f, :, lanes] = up_sum
            tsum[1, f, :, lanes] = down_sum
            return 0

        lax.fori_loop(0, 2, sweep, 0)
        if f == 0:
            told(near_sem.at[0], ("gx", 1), ("yz", 1))
            tell(near_sem.at[1], "yz", 2)
            tell(near_sem.at[2], "gx", 2)
        jobs += 2 * per_half
        for way in range(2):
            @pl.when(sends[way])
            def _():
                sums[way][f].start()

    mark("ends")
    for way, there in ((0, jnp.logical_not(has_left)), (1, jnp.logical_not(has_right))):
        @pl.when(there)
        def _():
            def close(n, _):
                f, t = n // 2, n % 2
                lanes = pl.ds(pl.multiple_of(128 * t, 128), 128)
                far = tsum[1 - way, f, :, lanes]
                one, two = float(ends[0, 4]) * far, float(ends[1, 4]) * far
                for i in range(4):
                    v = fld[f, i if way == 0 else CX - 1 - i, t, pl.ds(8, CY), :]
                    one = one + float(ends[0, i]) * v
                    two = two + float(ends[1, i]) * v
                hal[f, way, :, lanes] = one
                hal[f, 2 + way, :, lanes] = two
                return 0

            lax.fori_loop(0, 10, close, 0)
    for way, there, row in ((0, jnp.logical_not(has_low), 5), (1, jnp.logical_not(has_high), 8 + CY)):
        @pl.when(there)
        def _():
            for f in (0, 2, 4):
                fld[f, :, :, pl.ds(row, 3), :] = jnp.zeros((CX, 2, 3, 128), F32)

    mark("wait_y")
    for way in range(2):
        @pl.when(ygets[way])
        def _():
            yall[way].wait_recv()

    mark("local")
    def local(n, _):
        for j in range(2):
            for t in range(2):
                x = 2 * n + j
                at = lambda f, s=0: fld[f, x, t, pl.ds(8 + s, CY), :]
                pz, wz, mz = (zed[q, x, :, 128 * t : 128 * t + 128] for q in range(3))

                def dy(f):
                    return (
                        0.75 * (at(f, 1) - at(f, -1)) - 0.15 * (at(f, 2) - at(f, -2))
                        + (1.0 / 60.0) * (at(f, 3) - at(f, -3))
                    )

                px, ux, vx, wx, mx = (grd[f, x, t, pl.ds(0, CY), :] for f in range(5))
                m, u, v, w = at(4), at(1), at(2), at(3)
                cm = CC * m
                grd[0, x, t, pl.ds(0, CY), :] = cm * px + CC * ux + dy(2) + wz
                grd[1, x, t, pl.ds(0, CY), :] = cm * ux + CC * (u * mx + px) + v * dy(4) + w * mz
                grd[2, x, t, pl.ds(0, CY), :] = cm * vx + dy(0)
                grd[3, x, t, pl.ds(0, CY), :] = cm * wx + pz
        return 0

    lax.fori_loop(0, CX // 2, local, 0)

    mark("gather")
    corner = gx * (CX * CY * N_YZ) + yz * CY
    grd_rows = grd.reshape(5, CX * 2 * 64, 128)
    fld_rows = fld.reshape(5, CX * 2 * 64, 128)

    def gather(n, _):
        for k in range(8):
            j = n * 8 + k
            cell = cell_s[0, j]
            line = jnp.maximum(lax.shift_right_logical(cell, 8) - corner, 0)
            x = lax.shift_right_logical(lax.shift_right_logical(line, 7) * 86, 8)
            row = line - 256 * x + (lax.shift_right_logical(cell, 1) & 64)
            for q in range(4):
                stg[q, pl.ds(j, 1), :] = grd_rows[q, pl.ds(row, 1), :]
            for q, f in ((4, 0), (5, 1), (6, 4)):
                stg[q, pl.ds(j, 1), :] = fld_rows[f, pl.ds(row + 8, 1), :]
        return 0

    lax.fori_loop(0, FACES_DEV // 8, gather, 0)

    told(near_sem.at[1], ("yz", 2))
    tell(near_sem.at[3], "yz", 4)
    told(near_sem.at[2], ("gx", 2))
    tell(near_sem.at[4], "gx", 4)
    mark("picks")
    face0 = [pick(stg[q]) for q in range(7)]
    fp, fu, fm = face0[4], face0[5], face0[6]
    fn = [col(3 + k) for k in range(3)]
    to0 = (fm, jnp.ones_like(fm))
    toa = (fn[0], fn[0] * fm, fn[1] * fm, fn[2] * fm, fn[0] * fu)

    def left_of(k, scales):
        out = []
        for scale in scales:
            hi, lo = split2(weights[k] * scale)
            out += [hi, lo, hi]
        return jnp.concatenate(out, axis=1)

    lefts = [(left_of(k, to0), left_of(k, toa[:4]), left_of(k, toa[4:])) for k in range(2)]

    mark("wait_x")
    for way in range(2):
        @pl.when(gets[way])
        def _():
            all_planes[way].wait_recv()

    zwide = lax.broadcasted_iota(jnp.int32, (FACES_DEV, NZ), 1).astype(F32) == zcol
    pad = jnp.zeros((128 - 2 * CY, NZ), BF16)

    def rights(k, fields):
        out = []
        for f in fields:
            hi, lo = split2(hal[f, pl.ds(2 * k, 2)].reshape(2 * CY, NZ))
            out += [hi, pad, hi, pad, lo, pad]
        return out

    def times(a, right):
        return jnp.dot(a, jnp.concatenate(right, axis=0), preferred_element_type=F32)

    def most_at_faces(k):
        right = rights(k, range(4))
        return times(lefts[k][0], right[:12]), times(lefts[k][1], right)

    add0, adda = most_at_faces(1)
    adda = adda + times(lefts[1][2], rights(1, (4,)))
    mark("wait_t")
    for way in range(2):
        @pl.when(gets[way])
        def _():
            all_sums[way][0].wait_recv()
    more0, morea = most_at_faces(0)
    add0, adda = add0 + more0, adda + morea
    mark("wait_u")
    for way in range(2):
        @pl.when(gets[way])
        def _():
            all_sums[way][1].wait_recv()
    mark("near")
    adda = adda + times(lefts[0][2], rights(0, (4,)))
    pickw = lambda a: jnp.sum(jnp.where(zwide, a, 0.0), axis=1, keepdims=True)
    rate0 = -(face0[0] + pickw(add0))
    ratea = -(col(3) * face0[1] + col(4) * face0[2] + col(5) * face0[3] + pickw(adda))
    pnext = fp + TIME_STEP * rate0
    for t in range(4):
        lanes = slice(128 * t, 128 * t + 128)
        geo[0, :, lanes] = ratea * geo[0, :, lanes] + rate0 * geo[1, :, lanes] + pnext * geo[2, :, lanes]

    def patterns(n, _):
        t = n // 8
        block = n - 8 * t
        lanes = pl.ds(pl.multiple_of(128 * t, 128), 128)
        after = block + 1
        bit = jnp.where(after % 2 == 1, 3, jnp.where(after % 4 == 2, 4, 5))
        acc = [jnp.zeros((8, 128), F32)] * 8
        for g in range(FACES_DEV // 8):
            rows = pl.ds(8 * g, 8)
            what = geo[0, rows, lanes]
            geo[0, rows, lanes] = what * sgn[bit, rows, lanes]
            parts = [what]
            for k in range(3):
                sign = sgn[k, rows, lanes]
                parts += [part * sign for part in parts]
            acc = [a + part for a, part in zip(acc, parts)]
        for k in range(8):
            binned[t, pl.ds(pl.multiple_of(64 * block, 8) + 8 * k, 8), :] = acc[k]
        return 0

    def folded(t):
        out = binned[t, pl.ds(0, BINS, stride=8), :]
        for k in range(1, 8):
            out = out + binned[t, pl.ds(k, BINS, stride=8), :]
        return out

    def acopy(half, k):
        peer = lax.rem(yz + k, N_YZ)
        return pltpu.make_async_remote_copy(
            src_ref=packed.at[half, pl.ds(pl.multiple_of(16 * peer, 16), 16), :], dst_ref=recv_a.at[half, k - 1],
            send_sem=as_sem.at[half], recv_sem=ar_sem.at[half], device_id=(gx, peer), device_id_type=MESH,
        )

    def bcopy(k):
        peer = lax.rem(gx + k, N_GX)
        return pltpu.make_async_remote_copy(
            src_ref=send_b.at[peer], dst_ref=recv_b.at[k - 1],
            send_sem=bs_sem, recv_sem=br_sem, device_id=(peer, yz), device_id_type=MESH,
        )

    def whole(ref, send_sem, recv_sem, to):
        return pltpu.make_async_remote_copy(
            src_ref=ref, dst_ref=ref, send_sem=send_sem, recv_sem=recv_sem, device_id=to, device_id_type=MESH,
        )

    awhole = [whole(recv_a.at[half], as_sem.at[half], ar_sem.at[half], high) for half in range(2)]
    bwhole = whole(recv_b, bs_sem, br_sem, right)

    told(near_sem.at[3], ("yz", 4))
    for half in range(2):
        mark(f"bins{half}")
        lax.fori_loop(16 * half, 16 * half + 16, patterns, 0, unroll=4)
        mark(f"pack{half}")
        had = had_v[...]
        both = jnp.concatenate([folded(2 * half), folded(2 * half + 1)], axis=0).T
        hi = both.astype(BF16)
        rest = both - hi.astype(F32)
        mid = rest.astype(BF16)
        lo = (rest - mid.astype(F32)).astype(BF16)
        packed[half] = (
            jnp.dot(hi, had, preferred_element_type=F32)
            + jnp.dot(mid, had, preferred_element_type=F32)
            + jnp.dot(lo, had, preferred_element_type=F32)
        )
        for k in (4, 3, 5, 2, 6, 1, 7):
            acopy(half, k).start()
        if half == 0:
            told(near_sem.at[4], ("gx", 4))
            tell(near_sem.at[5], "gx", 8)

    mark("finish_a")
    def finish(x, _):
        ca, cb = table_s[0, x], table_s[1, x]
        for t in range(2):
            for h in range(2):
                lanes = pl.ds(128 * t, 128)
                ys = pl.ds(24 * h, 24)
                px, ux, vx, wx, mx = (ca * hal[f, 0, ys, lanes] + cb * hal[f, 1, ys, lanes] for f in range(5))
                p, u, v, w, m = (fld[f, x, t, pl.ds(8 + 24 * h, 24), :] for f in range(5))
                n0, n1, n2, n3 = (grd[q, x, t, ys, :] for q in range(4))
                nxt[0, x, ys, lanes] = p - TIME_STEP * (n0 + m * px + ux)
                nxt[1, x, ys, lanes] = u - TIME_STEP * (n1 + m * ux + u * mx + px)
                nxt[2, x, ys, lanes] = v - TIME_STEP * (n2 + m * vx)
                nxt[3, x, ys, lanes] = w - TIME_STEP * (n3 + m * wx)
        return 0

    def edges():
        for x, k, sign in ((0, 2, DD), (CX - 1, 3, -DD)):
            for t in range(2):
                lanes = pl.ds(128 * t, 128)
                px, ux, vx, wx, mx = ((-TIME_STEP * sign) * hal[f, k, :, lanes] for f in range(5))
                u, m = fld[1, x, t, pl.ds(8, CY), :], fld[4, x, t, pl.ds(8, CY), :]
                nxt[0, x, :, lanes] += m * px + ux
                nxt[1, x, :, lanes] += m * ux + u * mx + px
                nxt[2, x, :, lanes] += m * vx
                nxt[3, x, :, lanes] += m * wx

    lax.fori_loop(0, CX // 2, finish, 0)

    mark("wait_a")
    for half in range(2):
        awhole[half].wait_recv()
        total = packed[half, pl.ds(pl.multiple_of(16 * yz, 16), 16), :]
        for k in range(N_YZ - 1):
            total = total + recv_a[half, k]
        for g in range(N_GX):
            send_b[g, pl.ds(half, 1), :] = total[g : g + 1]
    mark("far_wait")
    told(near_sem.at[5], ("gx", 8))
    hops = lambda k: min(k // 4, 4 - k // 4) + min(k % 4, 4 - k % 4)
    for k in sorted(range(1, N_GX), key=hops, reverse=True):
        bcopy(k).start()

    mark("finish_b")
    lax.fori_loop(CX // 2, CX, finish, 0)
    edges()

    mark("wait_b")
    bwhole.wait_recv()
    total = send_b[gx]
    for k in range(N_GX - 1):
        total = total + recv_b[k]
    for h in range(2):
        for h2 in range(2):
            sig[pl.ds(2 * h + h2, 1), :] = total[h : h + 1, BINS * h2 : BINS * h2 + BINS]

    mark("drain")
    for way in range(2):
        @pl.when(sends[way])
        def _():
            for c in (all_planes[way], *all_sums[way]):
                c.wait_send()

        @pl.when(ysends[way])
        def _():
            yall[way].wait_send()
    for c in (*awhole, bwhole):
        c.wait_send()
    mark(None)


def per_device(state, mean_flow, face_cell, face_normal, face_pos, observer_pos, time_bin):
    n = np.arange(CX)
    table = np.zeros((8, 128), np.float32)
    table[0, :CX] = CC * LAM ** (n + 1.0)
    table[1, :CX] = -CC * LAM ** (CX - n * 1.0)
    table[2, 0] = DD
    table[3, CX - 1] = -DD
    dz = operator(NZ).T.astype(np.float32)
    dz_hi, dz_lo = split2(jnp.asarray(dz))
    dz = jnp.concatenate([dz_hi, dz_hi, dz_lo], axis=0)
    ends = closure(CX, CX * N_GX)
    gray = np.arange(BINS) // 8 * 8
    gray = (gray ^ (gray >> 1) & 56) + np.arange(BINS) % 8
    common = gray[:, None] & np.arange(BINS)[None, :]
    parity = sum((common >> k) & 1 for k in range(6)) % 2
    had = np.kron(np.eye(2), (1.0 - 2.0 * parity) / BINS).astype(np.float32)
    anywhere = pl.BlockSpec(memory_space=pltpu.HBM)
    vm = pltpu.VMEM
    dma = pltpu.SemaphoreType.DMA
    nxt, sig = pl.pallas_call(
        functools.partial(kernel, ends),
        out_shape=(
            vm((4, CX, CY, NZ), F32),
            vm((4, BINS), F32),
        ),
        in_specs=[anywhere] * 11,
        out_specs=(pl.BlockSpec(memory_space=pltpu.VMEM), pl.BlockSpec(memory_space=pltpu.VMEM)),
        scratch_shapes=[
            vm((5, CX, 2, 64, 128), F32),
            vm((5, CX, 2, 64, 128), F32),
            vm((3, CX, CY, NZ), F32),
            vm((5, 4, CY, NZ), F32),
            vm((2, 5, CY, NZ), F32),
            vm((7, FACES_DEV, 128), F32),
            vm((3, FACES_DEV, OBS), F32),
            vm((6, FACES_DEV, OBS), F32),
            vm((1, FACES_DEV), jnp.int32),
            vm((3, FACES_DEV), F32),
            vm((3, FACES_DEV), F32),
            vm((3, OBS), F32),
            vm((FACES_DEV, OBS), jnp.int32),
            vm((3 * NZ, NZ), BF16),
            vm((8, 128), F32),
            vm((128, 128), BF16),
            vm((16, 256), F32),
            vm((8, OBS), F32),
            vm((4, 8 * BINS, 128), F32),
            vm((2, 128, 128), F32),
            vm((2, N_YZ - 1, 16, 128), F32),
            vm((N_GX, 2, 128), F32),
            vm((N_GX - 1, 2, 128), F32),
            pltpu.SMEM((4, 128), F32),
            pltpu.SMEM((1, FACES_DEV), jnp.int32),
            dma((5, 2)), dma((10,)), dma((2, 3)), dma((2, 3)), dma((2,)), dma((2,)),
            dma((2,)), dma((2,)), dma(()), dma(()), pltpu.SemaphoreType.REGULAR((6,)),
        ],
        compiler_params=pltpu.CompilerParams(
            collective_id=0, has_side_effects=True, vmem_limit_bytes=57 * 2**20 + 2**19
        ),
    )(
        state, mean_flow, face_cell.reshape(1, FACES_DEV), face_normal, face_pos, observer_pos, time_bin,
        dz, jnp.asarray(table), jnp.asarray(table[:4]), jnp.asarray(had, BF16),
    )

    def write_out(nxt_ref, sig_ref, nxt_out, sig_out, sem):
        copies = [pltpu.make_async_copy(sig_ref, sig_out, sem.at[4])]
        copies += [pltpu.make_async_copy(nxt_ref.at[k], nxt_out.at[k], sem.at[k]) for k in range(4)]
        for c in copies:
            c.start()
        for c in copies:
            c.wait()

    return pl.pallas_call(
        write_out,
        out_shape=(
            jax.ShapeDtypeStruct((4, CX, CY, NZ), F32),
            jax.ShapeDtypeStruct((4, BINS), F32),
        ),
        in_specs=[pl.BlockSpec(memory_space=pltpu.VMEM)] * 2,
        out_specs=(anywhere, anywhere),
        scratch_shapes=[dma((5,))],
        compiler_params=pltpu.CompilerParams(vmem_limit_bytes=2**20),
    )(pltpu.with_memory_space_constraint(nxt, pltpu.VMEM), pltpu.with_memory_space_constraint(sig, pltpu.VMEM))


def solution(mesh):
    return jax.shard_map(
        per_device,
        mesh=mesh,
        in_specs=(
            P(None, "gx", "yz", None),
            P("gx", "yz", None),
            P(("gx", "yz")),
            P(None, ("gx", "yz")),
            P(None, ("gx", "yz")),
            P(),
            P(("gx", "yz"), None),
        ),
        out_specs=(P(None, "gx", "yz", None), P(("gx", "yz"), None)),
        check_vma=False,
    )
```

```python
import functools

import jax
import jax.numpy as jnp
import numpy as np
from jax import lax
from jax.experimental import pallas as pl
from jax.experimental.pallas import tpu as pltpu
from jax.sharding import PartitionSpec as P

CX, CY, NZ = 32, 48, 256
FACES_DEV, OBS, BINS = 192, 512, 64
N_GX, N_YZ = 16, 8
TIME_STEP = 0.25
INV_FOUR_PI = 1.0 / (4.0 * 3.141592653589793)
MESH = pl.DeviceIdType.MESH
F32, BF16 = jnp.float32, jnp.bfloat16

LAM = (-1.0 + np.sqrt(1.0 - 4.0 / 9.0)) / (2.0 / 3.0)
CC, DD = 25.0 / 12.0, -1.0 / 12.0
EDGE = DD / CC


def operator(n):
    a = np.eye(n)
    b = np.zeros((n, n))
    for i in range(n):
        if i == 0:
            a[0, 1] = 2.0
            b[0, :3] = (-2.5, 2.0, 0.5)
        elif i == n - 1:
            a[i, i - 1] = 2.0
            b[i, n - 3 :] = (-0.5, -2.0, 2.5)
        elif i in (1, n - 2):
            a[i, i - 1] = a[i, i + 1] = 0.25
            b[i, i + 1], b[i, i - 1] = 0.75, -0.75
        else:
            a[i, i - 1] = a[i, i + 1] = 1.0 / 3.0
            b[i, i + 1], b[i, i - 1] = 7.0 / 9.0, -7.0 / 9.0
            b[i, i + 2], b[i, i - 2] = 1.0 / 36.0, -1.0 / 36.0
    return np.linalg.solve(a, b)


def closure(n, total):
    lag = np.arange(n)[:, None] - np.arange(n)[None, :]
    inside = np.where(
        lag == 0, 0.0, np.sign(lag) * (CC * LAM ** np.abs(lag) + DD * (np.abs(lag) == 1))
    )
    rest = operator(total)[:n, :n] - inside
    factors = np.stack([CC * LAM ** (np.arange(n) + 1.0), DD * (np.arange(n) == 0)], 1)
    weights = np.linalg.lstsq(factors, rest, rcond=None)[0]
    scale = weights[:, 12] / LAM**12
    return np.concatenate([weights[:, :4] - scale[:, None] * LAM ** np.arange(4.0), scale[:, None]], 1)


def split2(x):
    hi = x.astype(BF16)
    return hi, (x - hi.astype(F32)).astype(BF16)


class Marks:
    def __init__(self):
        self.scope = None

    def __call__(self, name):
        if self.scope is not None:
            self.scope.__exit__(None, None, None)
        self.scope = None if name is None else jax.named_scope(name)
        if self.scope is not None:
            self.scope.__enter__()


def dot3(a, b):
    return (
        jnp.dot(a[0], b[0], preferred_element_type=F32)
        + jnp.dot(a[1], b[0], preferred_element_type=F32)
        + jnp.dot(a[0], b[1], preferred_element_type=F32)
    )


def kernel(
    ends, state, mean, face_cell, normal, pos, obs, tbin, dz, table, table_s_in, had,
    nxt, sig,
    fld, grd, zed, hal, tsum, stg, geo, sgn, face_v, normal_v, pos_v, obs_v, tbin_v, dz_v, table_v, had_v,
    rows_v, seen_v, binned, packed, recv_a, send_b, recv_b, table_s, cell_s,
    ld_sem, in_sem, xs_sem, xr_sem, ys_sem, yr_sem, as_sem, ar_sem, bs_sem, br_sem, near_sem,
):
    mark = Marks()
    gx = lax.axis_index("gx")
    yz = lax.axis_index("yz")

    mark("barrier")
    barrier = pltpu.get_barrier_semaphore()
    def tell(sem, along, step):
        here, count = (gx, N_GX) if along == "gx" else (yz, N_YZ)
        for sign in (1, -1):
            there = here + sign * step

            @pl.when(there < count if sign > 0 else there >= 0)
            def _():
                to = (there, yz) if along == "gx" else (gx, there)
                pl.semaphore_signal(sem, inc=1, device_id=to, device_id_type=MESH)

    def told(sem, *pairs):
        total = 0
        for along, step in pairs:
            here, count = (gx, N_GX) if along == "gx" else (yz, N_YZ)
            total = total + (here >= step).astype(jnp.int32) + (here < count - step).astype(jnp.int32)
        pl.semaphore_wait(sem, total)

    tell(barrier, "gx", 1)
    tell(barrier, "yz", 1)
    mark("start")
    order = (0, 4, 2, 3, 1)
    small = []
    for k, (s, d) in enumerate((
        (obs, obs_v), (tbin, tbin_v), (dz, dz_v), (table, table_v), (table_s_in, table_s),
        (face_cell, cell_s), (face_cell, face_v), (normal, normal_v), (pos, pos_v), (had, had_v),
    )):
        c = pltpu.make_async_copy(s, d, in_sem.at[k])
        c.start()
        small.append(c)

    loads = {}
    for f in order:
        src = mean if f == 4 else state.at[f]
        for t in range(2):
            c = pltpu.make_async_copy(
                src.at[:, :, pl.ds(128 * t, 128)], fld.at[f, :, t, pl.ds(8, CY), :], ld_sem.at[f, t]
            )
            c.start()
            loads[f, t] = c
    mark("barrier_wait")
    told(barrier, ("gx", 1), ("yz", 1))

    mark("issue")
    has_left, has_right = gx > 0, gx < N_GX - 1
    has_low, has_high = yz > 0, yz < N_YZ - 1
    right, left = (lax.rem(gx + 1, N_GX), yz), (lax.rem(gx + N_GX - 1, N_GX), yz)
    high, low = (gx, lax.rem(yz + 1, N_YZ)), (gx, lax.rem(yz + N_YZ - 1, N_YZ))

    def xcopy(src, dst, way, k):
        return pltpu.make_async_remote_copy(
            src_ref=src, dst_ref=dst, send_sem=xs_sem.at[way, k], recv_sem=xr_sem.at[way, k],
            device_id=(right, left)[way], device_id_type=MESH,
        )

    planes, sums = ([], []), ([], [])
    for way, plane in ((0, CX - 1), (1, 0)):
        planes[way].append(xcopy(state.at[:, plane], hal.at[pl.ds(0, 4), 2 + way], way, 0))
        planes[way].append(xcopy(mean.at[plane], hal.at[4, 2 + way], way, 0))
        for f in range(5):
            sums[way].append(xcopy(tsum.at[way, f], hal.at[f, way], way, 1 + f // 4))
    all_planes = [xcopy(tsum.at[way], hal.at[:, 2 + way], way, 0) for way in range(2)]
    all_sums = [
        (xcopy(tsum.at[way, pl.ds(0, 4)], hal.at[pl.ds(0, 4), way], way, 1), sums[way][4]) for way in range(2)
    ]
    tell(near_sem.at[0], "gx", 1)
    tell(near_sem.at[0], "yz", 1)
    sends = (has_right, has_left)
    gets = (has_left, has_right)
    for way in range(2):
        @pl.when(sends[way])
        def _():
            planes[way][0].start()
            planes[way][1].start()


    yc = ([], [])
    for k, f in enumerate((0, 2, 4)):
        for way, (first, there) in enumerate(((8 + CY - 3, 5), (8, 8 + CY))):
            yc[way].append(pltpu.make_async_remote_copy(
                src_ref=fld.at[f, :, :, pl.ds(first, 3), :], dst_ref=fld.at[f, :, :, pl.ds(there, 3), :],
                send_sem=ys_sem.at[way], recv_sem=yr_sem.at[way],
                device_id=(high, low)[way], device_id_type=MESH,
            ))
    yall = [
        pltpu.make_async_remote_copy(
            src_ref=fld.at[pl.ds(0, 3), :, :, pl.ds(row, 3), :], dst_ref=fld.at[pl.ds(0, 3), :, :, pl.ds(row, 3), :],
            send_sem=ys_sem.at[way], recv_sem=yr_sem.at[way], device_id=(high, low)[way], device_id_type=MESH,
        )
        for way, row in ((0, 5), (1, 8 + CY))
    ]
    ysends = (has_high, has_low)
    ygets = (has_low, has_high)

    def send_y(f):
        loads[f, 0].wait()
        loads[f, 1].wait()
        for way in range(2):
            @pl.when(ysends[way])
            def _():
                yc[way][f // 2].start()

    mark("observers")
    to = lax.broadcasted_iota(jnp.int32, (OBS, OBS), 1)
    source = (
        32 * (to & 15) + 4 * (lax.shift_right_logical(to, 4) & 7)
        + 2 * lax.shift_right_logical(to, 8) + (lax.shift_right_logical(to, 7) & 1)
    )
    perm = jnp.where(lax.broadcasted_iota(jnp.int32, (OBS, OBS), 0) == source, 1.0, 0.0).astype(BF16)
    small[0].wait()
    small[1].wait()
    which = jnp.dot(tbin_v[...].astype(F32).astype(BF16), perm, preferred_element_type=F32).astype(jnp.int32)
    for k in range(6):
        sgn[k] = jnp.where((which & (1 << k)) == 0, 1.0, -1.0)
    whole = obs_v[...]
    o_hi = whole.astype(BF16)
    rest = whole - o_hi.astype(F32)
    o_mid = rest.astype(BF16)
    o_lo = (rest - o_mid.astype(F32)).astype(BF16)
    seen_v[pl.ds(0, 3), :] = (
        jnp.dot(o_hi, perm, preferred_element_type=F32)
        + jnp.dot(o_mid, perm, preferred_element_type=F32)
        + jnp.dot(o_lo, perm, preferred_element_type=F32)
    )
    send_y(0)
    mark("columns")
    for c in small[3:]:
        c.wait()
    cell = face_v[...]
    line = lax.shift_right_logical(cell, 8)
    fx = lax.shift_right_logical(lax.shift_right_logical(line, 7) * 21846, 16)
    fy = line - CY * lax.shift_right_logical(lax.shift_right_logical(line, 4) * 21846, 16)
    fx = fx & (CX - 1)
    fz = cell & 255
    rows_v[...] = jnp.zeros((16, 256), F32)
    rows_v[pl.ds(0, 3), pl.ds(0, FACES_DEV)] = pos_v[...]
    rows_v[pl.ds(3, 3), pl.ds(0, FACES_DEV)] = normal_v[...]
    rows_v[pl.ds(6, 1), pl.ds(0, FACES_DEV)] = fx.astype(F32)
    rows_v[pl.ds(7, 1), pl.ds(0, FACES_DEV)] = fy.astype(F32)
    rows_v[pl.ds(8, 1), pl.ds(0, FACES_DEV)] = fz.astype(F32)
    cols = rows_v[...].T
    col = lambda k: cols[:FACES_DEV, k : k + 1]
    xcol, ycol, zcol = col(6), col(7), col(8)
    lane = lax.broadcasted_iota(jnp.int32, (FACES_DEV, 128), 1).astype(F32)
    zlane = zcol - jnp.where(zcol >= 128.0, 128.0, 0.0)
    zmask = zlane == lane
    pick = lambda a: jnp.sum(jnp.where(zmask, a, 0.0), axis=1, keepdims=True)
    xmask = xcol == lane
    coef = [
        jnp.sum(jnp.where(xmask, table_v[pl.ds(k, 1), :], 0.0), axis=1, keepdims=True) for k in range(4)
    ]
    upper = lane >= CY
    hit = jnp.where(upper, lane - CY, lane) == ycol
    weights = [
        jnp.where(hit, jnp.where(upper, coef[2 * k + 1], coef[2 * k]), 0.0) for k in range(2)
    ]
    send_y(4)
    mark("geometry")
    for t in range(4):
        lanes = slice(128 * t, 128 * t + 128)
        dx = seen_v[0:1, lanes] - col(0)
        dy_ = seen_v[1:2, lanes] - col(1)
        dz_ = seen_v[2:3, lanes] - col(2)
        inv = lax.rsqrt(dx * dx + dy_ * dy_ + dz_ * dz_)
        nr = (col(3) * dx + col(4) * dy_ + col(5) * dz_) * inv
        q1 = INV_FOUR_PI * inv
        geo[0, :, lanes] = q1
        geo[1, :, lanes] = q1 * nr
        geo[2, :, lanes] = q1 * nr * inv

    send_y(2)
    mark("sweeps")
    small[2].wait()

    def along_z(j):
        q = j // 2
        x0 = 16 * (j - 2 * q)
        f = jnp.where(q == 0, 0, q + 2)
        v = fld[f, pl.ds(x0, 16), :, pl.ds(8, CY), :]
        v = jnp.concatenate([v[:, 0], v[:, 1]], axis=-1).reshape(16 * CY, NZ)
        hi, lo = split2(v)
        out = jnp.dot(jnp.concatenate([hi, lo, hi], axis=1), dz_v[...], preferred_element_type=F32)
        zed[q, pl.ds(x0, 16)] = out.reshape(16, CY, NZ)

    jobs = 0
    for f, per_half in zip((0, 3, 2, 1, 4), (1, 1, 1, 0, 0)):
        if f not in (0, 2, 4):
            loads[f, 0].wait()
            loads[f, 1].wait()

        def sweep(t, _, f=f, per_half=per_half, jobs=jobs):
            zero = jnp.zeros((CY, 128), F32)
            at = lambda i: fld[f, i, t, pl.ds(8, CY), :] if 0 <= i < CX else zero
            up, down, v_old, w_old = zero, zero, zero, zero
            v, w = at(0), at(CX - 1)
            for i in range(CX):
                if i * per_half // CX != (i - 1) * per_half // CX:
                    along_z(jobs + per_half * t + i * per_half // CX)
                k = CX - 1 - i
                v_new, w_new = at(i + 1), at(k - 1)
                if i < CX // 2:
                    grd[f, i, t, pl.ds(0, CY), :] = up
                    grd[f, k, t, pl.ds(0, CY), :] = down
                else:
                    grd[f, i, t, pl.ds(0, CY), :] = (up - grd[f, i, t, pl.ds(0, CY), :]) + EDGE * (v_old - v_new)
                    grd[f, k, t, pl.ds(0, CY), :] = (grd[f, k, t, pl.ds(0, CY), :] - down) + EDGE * (w_new - w_old)
                up_sum, down_sum = up + v, down + w
                up, down = LAM * up_sum, LAM * down_sum
                v_old, v, w_old, w = v, v_new, w, w_new
            lanes = pl.ds(pl.multiple_of(128 * t, 128), 128)
            tsum[0, f, :, lanes] = up_sum
            tsum[1, f, :, lanes] = down_sum
            return 0

        lax.fori_loop(0, 2, sweep, 0)
        if f == 0:
            told(near_sem.at[0], ("gx", 1), ("yz", 1))
            tell(near_sem.at[1], "yz", 2)
            tell(near_sem.at[2], "gx", 2)
        jobs += 2 * per_half
        even = lax.rem(yz, 2) == 0
        for way in range(2):
            if f in (2, 1, 4):
                @pl.when(sends[way])
                def _():
                    sums[way][f].start()
            else:
                @pl.when(jnp.logical_and(sends[way], even))
                def _():
                    sums[way][f].start()
            if f == 2:
                @pl.when(jnp.logical_and(sends[way], jnp.logical_not(even)))
                def _():
                    for k in (0, 3):
                        sums[way][k].start()

    mark("ends")
    for way, there in ((0, jnp.logical_not(has_left)), (1, jnp.logical_not(has_right))):
        @pl.when(there)
        def _():
            def close(n, _):
                f, t = n // 2, n % 2
                lanes = pl.ds(pl.multiple_of(128 * t, 128), 128)
                far = tsum[1 - way, f, :, lanes]
                one, two = float(ends[0, 4]) * far, float(ends[1, 4]) * far
                for i in range(4):
                    v = fld[f, i if way == 0 else CX - 1 - i, t, pl.ds(8, CY), :]
                    one = one + float(ends[0, i]) * v
                    two = two + float(ends[1, i]) * v
                hal[f, way, :, lanes] = one
                hal[f, 2 + way, :, lanes] = two
                return 0

            lax.fori_loop(0, 10, close, 0)
    for way, there, row in ((0, jnp.logical_not(has_low), 5), (1, jnp.logical_not(has_high), 8 + CY)):
        @pl.when(there)
        def _():
            for f in (0, 2, 4):
                fld[f, :, :, pl.ds(row, 3), :] = jnp.zeros((CX, 2, 3, 128), F32)

    mark("wait_y")
    for way in range(2):
        @pl.when(ygets[way])
        def _():
            yall[way].wait_recv()

    mark("local")
    def local(n, _):
        for j in range(2):
            for t in range(2):
                x = 2 * n + j
                at = lambda f, s=0: fld[f, x, t, pl.ds(8 + s, CY), :]
                pz, wz, mz = (zed[q, x, :, 128 * t : 128 * t + 128] for q in range(3))

                def dy(f):
                    return (
                        0.75 * (at(f, 1) - at(f, -1)) - 0.15 * (at(f, 2) - at(f, -2))
                        + (1.0 / 60.0) * (at(f, 3) - at(f, -3))
                    )

                px, ux, vx, wx, mx = (grd[f, x, t, pl.ds(0, CY), :] for f in range(5))
                m, u, v, w = at(4), at(1), at(2), at(3)
                cm = CC * m
                grd[0, x, t, pl.ds(0, CY), :] = cm * px + CC * ux + dy(2) + wz
                grd[1, x, t, pl.ds(0, CY), :] = cm * ux + CC * (u * mx + px) + v * dy(4) + w * mz
                grd[2, x, t, pl.ds(0, CY), :] = cm * vx + dy(0)
                grd[3, x, t, pl.ds(0, CY), :] = cm * wx + pz
        return 0

    lax.fori_loop(0, CX // 2, local, 0)

    mark("gather")
    corner = gx * (CX * CY * N_YZ) + yz * CY
    grd_rows = grd.reshape(5, CX * 2 * 64, 128)
    fld_rows = fld.reshape(5, CX * 2 * 64, 128)

    def gather(n, _):
        for k in range(16):
            j = n * 16 + k
            cell = cell_s[0, j]
            line = jnp.maximum(lax.shift_right_logical(cell, 8) - corner, 0)
            x = lax.shift_right_logical(lax.shift_right_logical(line, 7) * 86, 8)
            row = line - 256 * x + (lax.shift_right_logical(cell, 1) & 64)
            for q in range(4):
                stg[q, pl.ds(j, 1), :] = grd_rows[q, pl.ds(row, 1), :]
            for q, f in ((4, 0), (5, 1), (6, 4)):
                stg[q, pl.ds(j, 1), :] = fld_rows[f, pl.ds(row + 8, 1), :]
        return 0

    lax.fori_loop(0, FACES_DEV // 16, gather, 0)

    told(near_sem.at[1], ("yz", 2))
    tell(near_sem.at[3], "yz", 4)
    told(near_sem.at[2], ("gx", 2))
    tell(near_sem.at[4], "gx", 4)
    mark("picks")
    face0 = [pick(stg[q]) for q in range(7)]
    fp, fu, fm = face0[4], face0[5], face0[6]
    fn = [col(3 + k) for k in range(3)]
    to0 = (fm, jnp.ones_like(fm))
    toa = (fn[0], fn[0] * fm, fn[1] * fm, fn[2] * fm, fn[0] * fu)

    def left_of(k, scales):
        out = []
        for scale in scales:
            hi, lo = split2(weights[k] * scale)
            out += [hi, lo, hi]
        return jnp.concatenate(out, axis=1)

    lefts = [(left_of(k, to0), left_of(k, toa[:4]), left_of(k, toa[4:])) for k in range(2)]

    mark("wait_x")
    for way in range(2):
        @pl.when(gets[way])
        def _():
            all_planes[way].wait_recv()

    zwide = lax.broadcasted_iota(jnp.int32, (FACES_DEV, NZ), 1).astype(F32) == zcol
    pad = jnp.zeros((128 - 2 * CY, NZ), BF16)

    def rights(k, fields):
        out = []
        for f in fields:
            hi, lo = split2(hal[f, pl.ds(2 * k, 2)].reshape(2 * CY, NZ))
            out += [hi, pad, hi, pad, lo, pad]
        return out

    def times(a, right):
        return jnp.dot(a, jnp.concatenate(right, axis=0), preferred_element_type=F32)

    def most_at_faces(k):
        right = rights(k, range(4))
        return times(lefts[k][0], right[:12]), times(lefts[k][1], right)

    add0, adda = most_at_faces(1)
    adda = adda + times(lefts[1][2], rights(1, (4,)))
    mark("wait_t")
    for way in range(2):
        @pl.when(gets[way])
        def _():
            all_sums[way][0].wait_recv()
    more0, morea = most_at_faces(0)
    add0, adda = add0 + more0, adda + morea
    mark("wait_u")
    for way in range(2):
        @pl.when(gets[way])
        def _():
            all_sums[way][1].wait_recv()
    mark("near")
    adda = adda + times(lefts[0][2], rights(0, (4,)))
    pickw = lambda a: jnp.sum(jnp.where(zwide, a, 0.0), axis=1, keepdims=True)
    rate0 = -(face0[0] + pickw(add0))
    ratea = -(col(3) * face0[1] + col(4) * face0[2] + col(5) * face0[3] + pickw(adda))
    pnext = fp + TIME_STEP * rate0
    for t in range(4):
        lanes = slice(128 * t, 128 * t + 128)
        geo[0, :, lanes] = ratea * geo[0, :, lanes] + rate0 * geo[1, :, lanes] + pnext * geo[2, :, lanes]

    def patterns(n, _):
        t = n // 8
        block = n - 8 * t
        lanes = pl.ds(pl.multiple_of(128 * t, 128), 128)
        after = block + 1
        bit = jnp.where(after % 2 == 1, 3, jnp.where(after % 4 == 2, 4, 5))
        acc = [jnp.zeros((8, 128), F32)] * 8
        for g in range(FACES_DEV // 8):
            rows = pl.ds(8 * g, 8)
            what = geo[0, rows, lanes]
            geo[0, rows, lanes] = what * sgn[bit, rows, lanes]
            parts = [what]
            for k in range(3):
                sign = sgn[k, rows, lanes]
                parts += [part * sign for part in parts]
            acc = [a + part for a, part in zip(acc, parts)]
        for k in range(8):
            binned[t, pl.ds(pl.multiple_of(64 * block, 8) + 8 * k, 8), :] = acc[k]
        return 0

    def folded(t):
        out = binned[t, pl.ds(0, BINS, stride=8), :]
        for k in range(1, 8):
            out = out + binned[t, pl.ds(k, BINS, stride=8), :]
        return out

    def acopy(half, k):
        peer = lax.rem(yz + k, N_YZ)
        return pltpu.make_async_remote_copy(
            src_ref=packed.at[half, pl.ds(pl.multiple_of(16 * peer, 16), 16), :], dst_ref=recv_a.at[half, k - 1],
            send_sem=as_sem.at[half], recv_sem=ar_sem.at[half], device_id=(gx, peer), device_id_type=MESH,
        )

    def bcopy(k):
        peer = lax.rem(gx + k, N_GX)
        return pltpu.make_async_remote_copy(
            src_ref=send_b.at[peer], dst_ref=recv_b.at[k - 1],
            send_sem=bs_sem, recv_sem=br_sem, device_id=(peer, yz), device_id_type=MESH,
        )

    def whole(ref, send_sem, recv_sem, to):
        return pltpu.make_async_remote_copy(
            src_ref=ref, dst_ref=ref, send_sem=send_sem, recv_sem=recv_sem, device_id=to, device_id_type=MESH,
        )

    awhole = [whole(recv_a.at[half], as_sem.at[half], ar_sem.at[half], high) for half in range(2)]
    bwhole = whole(recv_b, bs_sem, br_sem, right)

    told(near_sem.at[3], ("yz", 4))
    for half in range(2):
        mark(f"bins{half}")
        lax.fori_loop(16 * half, 16 * half + 16, patterns, 0, unroll=4)
        mark(f"pack{half}")
        had = had_v[...]
        both = jnp.concatenate([folded(2 * half), folded(2 * half + 1)], axis=0).T
        hi = both.astype(BF16)
        rest = both - hi.astype(F32)
        mid = rest.astype(BF16)
        lo = (rest - mid.astype(F32)).astype(BF16)
        packed[half] = (
            jnp.dot(hi, had, preferred_element_type=F32)
            + jnp.dot(mid, had, preferred_element_type=F32)
            + jnp.dot(lo, had, preferred_element_type=F32)
        )
        for k in (4, 3, 5, 2, 6, 1, 7):
            acopy(half, k).start()
        if half == 0:
            told(near_sem.at[4], ("gx", 4))
            tell(near_sem.at[5], "gx", 8)

    mark("finish_a")
    def finish(x, _):
        ca, cb = table_s[0, x], table_s[1, x]
        for t in range(2):
            for h in range(2):
                lanes = pl.ds(128 * t, 128)
                ys = pl.ds(24 * h, 24)
                px, ux, vx, wx, mx = (ca * hal[f, 0, ys, lanes] + cb * hal[f, 1, ys, lanes] for f in range(5))
                p, u, v, w, m = (fld[f, x, t, pl.ds(8 + 24 * h, 24), :] for f in range(5))
                n0, n1, n2, n3 = (grd[q, x, t, ys, :] for q in range(4))
                nxt[0, x, ys, lanes] = p - TIME_STEP * (n0 + m * px + ux)
                nxt[1, x, ys, lanes] = u - TIME_STEP * (n1 + m * ux + u * mx + px)
                nxt[2, x, ys, lanes] = v - TIME_STEP * (n2 + m * vx)
                nxt[3, x, ys, lanes] = w - TIME_STEP * (n3 + m * wx)
        return 0

    def edges():
        for x, k, sign in ((0, 2, DD), (CX - 1, 3, -DD)):
            for t in range(2):
                lanes = pl.ds(128 * t, 128)
                px, ux, vx, wx, mx = ((-TIME_STEP * sign) * hal[f, k, :, lanes] for f in range(5))
                u, m = fld[1, x, t, pl.ds(8, CY), :], fld[4, x, t, pl.ds(8, CY), :]
                nxt[0, x, :, lanes] += m * px + ux
                nxt[1, x, :, lanes] += m * ux + u * mx + px
                nxt[2, x, :, lanes] += m * vx
                nxt[3, x, :, lanes] += m * wx

    lax.fori_loop(0, CX // 2, finish, 0)

    mark("wait_a")
    for half in range(2):
        awhole[half].wait_recv()
        total = packed[half, pl.ds(pl.multiple_of(16 * yz, 16), 16), :]
        for k in range(N_YZ - 1):
            total = total + recv_a[half, k]
        for g in range(N_GX):
            send_b[g, pl.ds(half, 1), :] = total[g : g + 1]
    mark("far_wait")
    told(near_sem.at[5], ("gx", 8))
    hops = lambda k: min(k // 4, 4 - k // 4) + min(k % 4, 4 - k % 4)
    for k in sorted(range(1, N_GX), key=hops, reverse=True):
        bcopy(k).start()

    mark("finish_b")
    lax.fori_loop(CX // 2, CX, finish, 0)
    edges()

    mark("wait_b")
    bwhole.wait_recv()
    total = send_b[gx]
    for k in range(N_GX - 1):
        total = total + recv_b[k]
    for h in range(2):
        for h2 in range(2):
            sig[pl.ds(2 * h + h2, 1), :] = total[h : h + 1, BINS * h2 : BINS * h2 + BINS]

    mark("drain")
    for way in range(2):
        @pl.when(sends[way])
        def _():
            for c in (all_planes[way], *all_sums[way]):
                c.wait_send()

        @pl.when(ysends[way])
        def _():
            yall[way].wait_send()
    for c in (*awhole, bwhole):
        c.wait_send()
    mark(None)


def per_device(state, mean_flow, face_cell, face_normal, face_pos, observer_pos, time_bin):
    n = np.arange(CX)
    table = np.zeros((8, 128), np.float32)
    table[0, :CX] = CC * LAM ** (n + 1.0)
    table[1, :CX] = -CC * LAM ** (CX - n * 1.0)
    table[2, 0] = DD
    table[3, CX - 1] = -DD
    dz = operator(NZ).T.astype(np.float32)
    dz_hi, dz_lo = split2(jnp.asarray(dz))
    dz = jnp.concatenate([dz_hi, dz_hi, dz_lo], axis=0)
    ends = closure(CX, CX * N_GX)
    gray = np.arange(BINS) // 8 * 8
    gray = (gray ^ (gray >> 1) & 56) + np.arange(BINS) % 8
    common = gray[:, None] & np.arange(BINS)[None, :]
    parity = sum((common >> k) & 1 for k in range(6)) % 2
    had = np.kron(np.eye(2), (1.0 - 2.0 * parity) / BINS).astype(np.float32)
    anywhere = pl.BlockSpec(memory_space=pltpu.HBM)
    vm = pltpu.VMEM
    dma = pltpu.SemaphoreType.DMA
    nxt, sig = pl.pallas_call(
        functools.partial(kernel, ends),
        out_shape=(
            vm((4, CX, CY, NZ), F32),
            vm((4, BINS), F32),
        ),
        in_specs=[anywhere] * 11,
        out_specs=(pl.BlockSpec(memory_space=pltpu.VMEM), pl.BlockSpec(memory_space=pltpu.VMEM)),
        scratch_shapes=[
            vm((5, CX, 2, 64, 128), F32),
            vm((5, CX, 2, 64, 128), F32),
            vm((3, CX, CY, NZ), F32),
            vm((5, 4, CY, NZ), F32),
            vm((2, 5, CY, NZ), F32),
            vm((7, FACES_DEV, 128), F32),
            vm((3, FACES_DEV, OBS), F32),
            vm((6, FACES_DEV, OBS), F32),
            vm((1, FACES_DEV), jnp.int32),
            vm((3, FACES_DEV), F32),
            vm((3, FACES_DEV), F32),
            vm((3, OBS), F32),
            vm((FACES_DEV, OBS), jnp.int32),
            vm((3 * NZ, NZ), BF16),
            vm((8, 128), F32),
            vm((128, 128), BF16),
            vm((16, 256), F32),
            vm((8, OBS), F32),
            vm((4, 8 * BINS, 128), F32),
            vm((2, 128, 128), F32),
            vm((2, N_YZ - 1, 16, 128), F32),
            vm((N_GX, 2, 128), F32),
            vm((N_GX - 1, 2, 128), F32),
            pltpu.SMEM((4, 128), F32),
            pltpu.SMEM((1, FACES_DEV), jnp.int32),
            dma((5, 2)), dma((10,)), dma((2, 3)), dma((2, 3)), dma((2,)), dma((2,)),
            dma((2,)), dma((2,)), dma(()), dma(()), pltpu.SemaphoreType.REGULAR((6,)),
        ],
        compiler_params=pltpu.CompilerParams(
            collective_id=0, has_side_effects=True, vmem_limit_bytes=57 * 2**20 + 2**19
        ),
    )(
        state, mean_flow, face_cell.reshape(1, FACES_DEV), face_normal, face_pos, observer_pos, time_bin,
        dz, jnp.asarray(table), jnp.asarray(table[:4]), jnp.asarray(had, BF16),
    )

    def write_out(nxt_ref, sig_ref, nxt_out, sig_out, sem):
        copies = [pltpu.make_async_copy(sig_ref, sig_out, sem.at[4])]
        copies += [pltpu.make_async_copy(nxt_ref.at[k], nxt_out.at[k], sem.at[k]) for k in range(4)]
        for c in copies:
            c.start()
        for c in copies:
            c.wait()

    return pl.pallas_call(
        write_out,
        out_shape=(
            jax.ShapeDtypeStruct((4, CX, CY, NZ), F32),
            jax.ShapeDtypeStruct((4, BINS), F32),
        ),
        in_specs=[pl.BlockSpec(memory_space=pltpu.VMEM)] * 2,
        out_specs=(anywhere, anywhere),
        scratch_shapes=[dma((5,))],
        compiler_params=pltpu.CompilerParams(vmem_limit_bytes=2**20),
    )(pltpu.with_memory_space_constraint(nxt, pltpu.VMEM), pltpu.with_memory_space_constraint(sig, pltpu.VMEM))


def solution(mesh):
    return jax.shard_map(
        per_device,
        mesh=mesh,
        in_specs=(
            P(None, "gx", "yz", None),
            P("gx", "yz", None),
            P(("gx", "yz")),
            P(None, ("gx", "yz")),
            P(None, ("gx", "yz")),
            P(),
            P(("gx", "yz"), None),
        ),
        out_specs=(P(None, "gx", "yz", None), P(("gx", "yz"), None)),
        check_vma=False,
    )
```

```python
import functools

import jax
import jax.numpy as jnp
import numpy as np
from jax import lax
from jax.experimental import pallas as pl
from jax.experimental.pallas import tpu as pltpu
from jax.sharding import PartitionSpec as P

CX, CY, NZ = 32, 48, 256
FACES_DEV, OBS, BINS = 192, 512, 64
N_GX, N_YZ = 16, 8
TIME_STEP = 0.25
INV_FOUR_PI = 1.0 / (4.0 * 3.141592653589793)
MESH = pl.DeviceIdType.MESH
F32, BF16 = jnp.float32, jnp.bfloat16

LAM = (-1.0 + np.sqrt(1.0 - 4.0 / 9.0)) / (2.0 / 3.0)
CC, DD = 25.0 / 12.0, -1.0 / 12.0
EDGE = DD / CC


def operator(n):
    a = np.eye(n)
    b = np.zeros((n, n))
    for i in range(n):
        if i == 0:
            a[0, 1] = 2.0
            b[0, :3] = (-2.5, 2.0, 0.5)
        elif i == n - 1:
            a[i, i - 1] = 2.0
            b[i, n - 3 :] = (-0.5, -2.0, 2.5)
        elif i in (1, n - 2):
            a[i, i - 1] = a[i, i + 1] = 0.25
            b[i, i + 1], b[i, i - 1] = 0.75, -0.75
        else:
            a[i, i - 1] = a[i, i + 1] = 1.0 / 3.0
            b[i, i + 1], b[i, i - 1] = 7.0 / 9.0, -7.0 / 9.0
            b[i, i + 2], b[i, i - 2] = 1.0 / 36.0, -1.0 / 36.0
    return np.linalg.solve(a, b)


def closure(n, total):
    lag = np.arange(n)[:, None] - np.arange(n)[None, :]
    inside = np.where(
        lag == 0, 0.0, np.sign(lag) * (CC * LAM ** np.abs(lag) + DD * (np.abs(lag) == 1))
    )
    rest = operator(total)[:n, :n] - inside
    factors = np.stack([CC * LAM ** (np.arange(n) + 1.0), DD * (np.arange(n) == 0)], 1)
    weights = np.linalg.lstsq(factors, rest, rcond=None)[0]
    scale = weights[:, 12] / LAM**12
    return np.concatenate([weights[:, :4] - scale[:, None] * LAM ** np.arange(4.0), scale[:, None]], 1)


def split2(x):
    hi = x.astype(BF16)
    return hi, (x - hi.astype(F32)).astype(BF16)


class Marks:
    def __init__(self):
        self.scope = None

    def __call__(self, name):
        if self.scope is not None:
            self.scope.__exit__(None, None, None)
        self.scope = None if name is None else jax.named_scope(name)
        if self.scope is not None:
            self.scope.__enter__()


def dot3(a, b):
    return (
        jnp.dot(a[0], b[0], preferred_element_type=F32)
        + jnp.dot(a[1], b[0], preferred_element_type=F32)
        + jnp.dot(a[0], b[1], preferred_element_type=F32)
    )


def kernel(
    ends, state, mean, face_cell, normal, pos, obs, tbin, dz, table, table_s_in, had,
    nxt, sig,
    fld, grd, zed, hal, tsum, stg, geo, sgn, face_v, normal_v, pos_v, obs_v, tbin_v, dz_v, table_v, had_v,
    rows_v, seen_v, binned, packed, recv_a, send_b, recv_b, table_s, cell_s,
    ld_sem, in_sem, xs_sem, xr_sem, ys_sem, yr_sem, as_sem, ar_sem, bs_sem, br_sem, near_sem,
):
    mark = Marks()
    gx = lax.axis_index("gx")
    yz = lax.axis_index("yz")

    mark("barrier")
    barrier = pltpu.get_barrier_semaphore()
    def tell(sem, along, step):
        here, count = (gx, N_GX) if along == "gx" else (yz, N_YZ)
        for sign in (1, -1):
            there = here + sign * step

            @pl.when(there < count if sign > 0 else there >= 0)
            def _():
                to = (there, yz) if along == "gx" else (gx, there)
                pl.semaphore_signal(sem, inc=1, device_id=to, device_id_type=MESH)

    def told(sem, *pairs):
        total = 0
        for along, step in pairs:
            here, count = (gx, N_GX) if along == "gx" else (yz, N_YZ)
            total = total + (here >= step).astype(jnp.int32) + (here < count - step).astype(jnp.int32)
        pl.semaphore_wait(sem, total)

    tell(barrier, "gx", 1)
    tell(barrier, "yz", 1)
    mark("start")
    order = (0, 4, 2, 3, 1)
    small = []
    for k, (s, d) in enumerate((
        (obs, obs_v), (tbin, tbin_v), (dz, dz_v), (table, table_v), (table_s_in, table_s),
        (face_cell, cell_s), (face_cell, face_v), (normal, normal_v), (pos, pos_v), (had, had_v),
    )):
        c = pltpu.make_async_copy(s, d, in_sem.at[k])
        c.start()
        small.append(c)

    loads = {}
    for f in order:
        src = mean if f == 4 else state.at[f]
        for t in range(2):
            c = pltpu.make_async_copy(
                src.at[:, :, pl.ds(128 * t, 128)], fld.at[f, :, t, pl.ds(8, CY), :], ld_sem.at[f, t]
            )
            c.start()
            loads[f, t] = c
    mark("barrier_wait")
    told(barrier, ("gx", 1), ("yz", 1))

    mark("issue")
    has_left, has_right = gx > 0, gx < N_GX - 1
    has_low, has_high = yz > 0, yz < N_YZ - 1
    right, left = (lax.rem(gx + 1, N_GX), yz), (lax.rem(gx + N_GX - 1, N_GX), yz)
    high, low = (gx, lax.rem(yz + 1, N_YZ)), (gx, lax.rem(yz + N_YZ - 1, N_YZ))

    def xcopy(src, dst, way, k):
        return pltpu.make_async_remote_copy(
            src_ref=src, dst_ref=dst, send_sem=xs_sem.at[way, k], recv_sem=xr_sem.at[way, k],
            device_id=(right, left)[way], device_id_type=MESH,
        )

    planes, sums = ([], []), ([], [])
    for way, plane in ((0, CX - 1), (1, 0)):
        planes[way].append(xcopy(state.at[:, plane], hal.at[pl.ds(0, 4), 2 + way], way, 0))
        planes[way].append(xcopy(mean.at[plane], hal.at[4, 2 + way], way, 0))
        for f in range(5):
            sums[way].append(xcopy(tsum.at[way, f], hal.at[f, way], way, 1 + f // 4))
    all_planes = [xcopy(tsum.at[way], hal.at[:, 2 + way], way, 0) for way in range(2)]
    all_sums = [
        (xcopy(tsum.at[way, pl.ds(0, 4)], hal.at[pl.ds(0, 4), way], way, 1), sums[way][4]) for way in range(2)
    ]
    tell(near_sem.at[0], "gx", 1)
    tell(near_sem.at[0], "yz", 1)
    sends = (has_right, has_left)
    gets = (has_left, has_right)
    for way in range(2):
        @pl.when(sends[way])
        def _():
            planes[way][0].start()
            planes[way][1].start()


    yc = ([], [])
    for k, f in enumerate((0, 2, 4)):
        for way, (first, there) in enumerate(((8 + CY - 3, 5), (8, 8 + CY))):
            yc[way].append(pltpu.make_async_remote_copy(
                src_ref=fld.at[f, :, :, pl.ds(first, 3), :], dst_ref=fld.at[f, :, :, pl.ds(there, 3), :],
                send_sem=ys_sem.at[way], recv_sem=yr_sem.at[way],
                device_id=(high, low)[way], device_id_type=MESH,
            ))
    yall = [
        pltpu.make_async_remote_copy(
            src_ref=fld.at[pl.ds(0, 3), :, :, pl.ds(row, 3), :], dst_ref=fld.at[pl.ds(0, 3), :, :, pl.ds(row, 3), :],
            send_sem=ys_sem.at[way], recv_sem=yr_sem.at[way], device_id=(high, low)[way], device_id_type=MESH,
        )
        for way, row in ((0, 5), (1, 8 + CY))
    ]
    ysends = (has_high, has_low)
    ygets = (has_low, has_high)

    def send_y(f):
        loads[f, 0].wait()
        loads[f, 1].wait()
        for way in range(2):
            @pl.when(ysends[way])
            def _():
                yc[way][f // 2].start()

    mark("observers")
    to = lax.broadcasted_iota(jnp.int32, (OBS, OBS), 1)
    source = (
        32 * (to & 15) + 4 * (lax.shift_right_logical(to, 4) & 7)
        + 2 * lax.shift_right_logical(to, 8) + (lax.shift_right_logical(to, 7) & 1)
    )
    perm = jnp.where(lax.broadcasted_iota(jnp.int32, (OBS, OBS), 0) == source, 1.0, 0.0).astype(BF16)
    small[0].wait()
    small[1].wait()
    which = jnp.dot(tbin_v[...].astype(F32).astype(BF16), perm, preferred_element_type=F32).astype(jnp.int32)
    for k in range(6):
        sgn[k] = jnp.where((which & (1 << k)) == 0, 1.0, -1.0)
    whole = obs_v[...]
    o_hi = whole.astype(BF16)
    rest = whole - o_hi.astype(F32)
    o_mid = rest.astype(BF16)
    o_lo = (rest - o_mid.astype(F32)).astype(BF16)
    seen_v[pl.ds(0, 3), :] = (
        jnp.dot(o_hi, perm, preferred_element_type=F32)
        + jnp.dot(o_mid, perm, preferred_element_type=F32)
        + jnp.dot(o_lo, perm, preferred_element_type=F32)
    )
    send_y(0)
    mark("columns")
    for c in small[3:]:
        c.wait()
    cell = face_v[...]
    line = lax.shift_right_logical(cell, 8)
    fx = lax.shift_right_logical(lax.shift_right_logical(line, 7) * 21846, 16)
    fy = line - CY * lax.shift_right_logical(lax.shift_right_logical(line, 4) * 21846, 16)
    fx = fx & (CX - 1)
    fz = cell & 255
    rows_v[...] = jnp.zeros((16, 256), F32)
    rows_v[pl.ds(0, 3), pl.ds(0, FACES_DEV)] = pos_v[...]
    rows_v[pl.ds(3, 3), pl.ds(0, FACES_DEV)] = normal_v[...]
    rows_v[pl.ds(6, 1), pl.ds(0, FACES_DEV)] = fx.astype(F32)
    rows_v[pl.ds(7, 1), pl.ds(0, FACES_DEV)] = fy.astype(F32)
    rows_v[pl.ds(8, 1), pl.ds(0, FACES_DEV)] = fz.astype(F32)
    cols = rows_v[...].T
    col = lambda k: cols[:FACES_DEV, k : k + 1]
    xcol, ycol, zcol = col(6), col(7), col(8)
    lane = lax.broadcasted_iota(jnp.int32, (FACES_DEV, 128), 1).astype(F32)
    zlane = zcol - jnp.where(zcol >= 128.0, 128.0, 0.0)
    zmask = zlane == lane
    pick = lambda a: jnp.sum(jnp.where(zmask, a, 0.0), axis=1, keepdims=True)
    xmask = xcol == lane
    coef = [
        jnp.sum(jnp.where(xmask, table_v[pl.ds(k, 1), :], 0.0), axis=1, keepdims=True) for k in range(4)
    ]
    upper = lane >= CY
    hit = jnp.where(upper, lane - CY, lane) == ycol
    weights = [
        jnp.where(hit, jnp.where(upper, coef[2 * k + 1], coef[2 * k]), 0.0) for k in range(2)
    ]
    send_y(4)
    mark("geometry")
    for t in range(4):
        lanes = slice(128 * t, 128 * t + 128)
        dx = seen_v[0:1, lanes] - col(0)
        dy_ = seen_v[1:2, lanes] - col(1)
        dz_ = seen_v[2:3, lanes] - col(2)
        inv = lax.rsqrt(dx * dx + dy_ * dy_ + dz_ * dz_)
        nr = (col(3) * dx + col(4) * dy_ + col(5) * dz_) * inv
        q1 = INV_FOUR_PI * inv
        geo[0, :, lanes] = q1
        geo[1, :, lanes] = q1 * nr
        geo[2, :, lanes] = q1 * nr * inv

    send_y(2)
    mark("sweeps")
    small[2].wait()

    def along_z(j):
        q = j // 2
        x0 = 16 * (j - 2 * q)
        f = jnp.where(q == 0, 0, q + 2)
        v = fld[f, pl.ds(x0, 16), :, pl.ds(8, CY), :]
        v = jnp.concatenate([v[:, 0], v[:, 1]], axis=-1).reshape(16 * CY, NZ)
        hi, lo = split2(v)
        out = jnp.dot(jnp.concatenate([hi, lo, hi], axis=1), dz_v[...], preferred_element_type=F32)
        zed[q, pl.ds(x0, 16)] = out.reshape(16, CY, NZ)

    jobs = 0
    for f, per_half in zip((0, 3, 2, 1, 4), (1, 1, 1, 0, 0)):
        if f not in (0, 2, 4):
            loads[f, 0].wait()
            loads[f, 1].wait()

        def sweep(t, _, f=f, per_half=per_half, jobs=jobs):
            zero = jnp.zeros((CY, 128), F32)
            at = lambda i: fld[f, i, t, pl.ds(8, CY), :] if 0 <= i < CX else zero
            up, down, v_old, w_old = zero, zero, zero, zero
            v, w = at(0), at(CX - 1)
            for i in range(CX):
                if i * per_half // CX != (i - 1) * per_half // CX:
                    along_z(jobs + per_half * t + i * per_half // CX)
                k = CX - 1 - i
                v_new, w_new = at(i + 1), at(k - 1)
                if i < CX // 2:
                    grd[f, i, t, pl.ds(0, CY), :] = up
                    grd[f, k, t, pl.ds(0, CY), :] = down
                else:
                    grd[f, i, t, pl.ds(0, CY), :] = (up - grd[f, i, t, pl.ds(0, CY), :]) + EDGE * (v_old - v_new)
                    grd[f, k, t, pl.ds(0, CY), :] = (grd[f, k, t, pl.ds(0, CY), :] - down) + EDGE * (w_new - w_old)
                up_sum, down_sum = up + v, down + w
                up, down = LAM * up_sum, LAM * down_sum
                v_old, v, w_old, w = v, v_new, w, w_new
            lanes = pl.ds(pl.multiple_of(128 * t, 128), 128)
            tsum[0, f, :, lanes] = up_sum
            tsum[1, f, :, lanes] = down_sum
            return 0

        lax.fori_loop(0, 2, sweep, 0)
        if f == 0:
            told(near_sem.at[0], ("gx", 1), ("yz", 1))
            tell(near_sem.at[1], "yz", 2)
            tell(near_sem.at[2], "gx", 2)
        jobs += 2 * per_half
        even = lax.rem(yz, 2) == 0
        for way in range(2):
            if f in (2, 1, 4):
                @pl.when(sends[way])
                def _():
                    sums[way][f].start()
            else:
                @pl.when(jnp.logical_and(sends[way], even))
                def _():
                    sums[way][f].start()
            if f == 2:
                @pl.when(jnp.logical_and(sends[way], jnp.logical_not(even)))
                def _():
                    for k in (0, 3):
                        sums[way][k].start()

    told(near_sem.at[1], ("yz", 2))
    tell(near_sem.at[3], "yz", 4)
    mark("ends")
    for way, there in ((0, jnp.logical_not(has_left)), (1, jnp.logical_not(has_right))):
        @pl.when(there)
        def _():
            def close(n, _):
                f, t = n // 2, n % 2
                lanes = pl.ds(pl.multiple_of(128 * t, 128), 128)
                far = tsum[1 - way, f, :, lanes]
                one, two = float(ends[0, 4]) * far, float(ends[1, 4]) * far
                for i in range(4):
                    v = fld[f, i if way == 0 else CX - 1 - i, t, pl.ds(8, CY), :]
                    one = one + float(ends[0, i]) * v
                    two = two + float(ends[1, i]) * v
                hal[f, way, :, lanes] = one
                hal[f, 2 + way, :, lanes] = two
                return 0

            lax.fori_loop(0, 10, close, 0)
    for way, there, row in ((0, jnp.logical_not(has_low), 5), (1, jnp.logical_not(has_high), 8 + CY)):
        @pl.when(there)
        def _():
            for f in (0, 2, 4):
                fld[f, :, :, pl.ds(row, 3), :] = jnp.zeros((CX, 2, 3, 128), F32)

    mark("wait_y")
    for way in range(2):
        @pl.when(ygets[way])
        def _():
            yall[way].wait_recv()

    mark("local")
    def local(n, _):
        for j in range(2):
            for t in range(2):
                x = 2 * n + j
                at = lambda f, s=0: fld[f, x, t, pl.ds(8 + s, CY), :]
                pz, wz, mz = (zed[q, x, :, 128 * t : 128 * t + 128] for q in range(3))

                def dy(f):
                    return (
                        0.75 * (at(f, 1) - at(f, -1)) - 0.15 * (at(f, 2) - at(f, -2))
                        + (1.0 / 60.0) * (at(f, 3) - at(f, -3))
                    )

                px, ux, vx, wx, mx = (grd[f, x, t, pl.ds(0, CY), :] for f in range(5))
                m, u, v, w = at(4), at(1), at(2), at(3)
                cm = CC * m
                grd[0, x, t, pl.ds(0, CY), :] = cm * px + CC * ux + dy(2) + wz
                grd[1, x, t, pl.ds(0, CY), :] = cm * ux + CC * (u * mx + px) + v * dy(4) + w * mz
                grd[2, x, t, pl.ds(0, CY), :] = cm * vx + dy(0)
                grd[3, x, t, pl.ds(0, CY), :] = cm * wx + pz
        return 0

    lax.fori_loop(0, CX // 2, local, 0)

    mark("gather")
    corner = gx * (CX * CY * N_YZ) + yz * CY
    grd_rows = grd.reshape(5, CX * 2 * 64, 128)
    fld_rows = fld.reshape(5, CX * 2 * 64, 128)

    def gather(n, _):
        for k in range(16):
            j = n * 16 + k
            cell = cell_s[0, j]
            line = jnp.maximum(lax.shift_right_logical(cell, 8) - corner, 0)
            x = lax.shift_right_logical(lax.shift_right_logical(line, 7) * 86, 8)
            row = line - 256 * x + (lax.shift_right_logical(cell, 1) & 64)
            for q in range(4):
                stg[q, pl.ds(j, 1), :] = grd_rows[q, pl.ds(row, 1), :]
            for q, f in ((4, 0), (5, 1), (6, 4)):
                stg[q, pl.ds(j, 1), :] = fld_rows[f, pl.ds(row + 8, 1), :]
        return 0

    lax.fori_loop(0, FACES_DEV // 16, gather, 0)

    told(near_sem.at[2], ("gx", 2))
    tell(near_sem.at[4], "gx", 4)
    mark("picks")
    face0 = [pick(stg[q]) for q in range(7)]
    fp, fu, fm = face0[4], face0[5], face0[6]
    fn = [col(3 + k) for k in range(3)]
    to0 = (fm, jnp.ones_like(fm))
    toa = (fn[0], fn[0] * fm, fn[1] * fm, fn[2] * fm, fn[0] * fu)

    def left_of(k, scales):
        out = []
        for scale in scales:
            hi, lo = split2(weights[k] * scale)
            out += [hi, lo, hi]
        return jnp.concatenate(out, axis=1)

    lefts = [(left_of(k, to0), left_of(k, toa[:4]), left_of(k, toa[4:])) for k in range(2)]

    mark("wait_x")
    for way in range(2):
        @pl.when(gets[way])
        def _():
            all_planes[way].wait_recv()

    zwide = lax.broadcasted_iota(jnp.int32, (FACES_DEV, NZ), 1).astype(F32) == zcol
    pad = jnp.zeros((128 - 2 * CY, NZ), BF16)

    def rights(k, fields):
        out = []
        for f in fields:
            hi, lo = split2(hal[f, pl.ds(2 * k, 2)].reshape(2 * CY, NZ))
            out += [hi, pad, hi, pad, lo, pad]
        return out

    def times(a, right):
        return jnp.dot(a, jnp.concatenate(right, axis=0), preferred_element_type=F32)

    def most_at_faces(k):
        right = rights(k, range(4))
        return times(lefts[k][0], right[:12]), times(lefts[k][1], right)

    add0, adda = most_at_faces(1)
    adda = adda + times(lefts[1][2], rights(1, (4,)))
    mark("wait_t")
    for way in range(2):
        @pl.when(gets[way])
        def _():
            all_sums[way][0].wait_recv()
    more0, morea = most_at_faces(0)
    add0, adda = add0 + more0, adda + morea
    mark("wait_u")
    for way in range(2):
        @pl.when(gets[way])
        def _():
            all_sums[way][1].wait_recv()
    mark("near")
    adda = adda + times(lefts[0][2], rights(0, (4,)))
    pickw = lambda a: jnp.sum(jnp.where(zwide, a, 0.0), axis=1, keepdims=True)
    rate0 = -(face0[0] + pickw(add0))
    ratea = -(col(3) * face0[1] + col(4) * face0[2] + col(5) * face0[3] + pickw(adda))
    pnext = fp + TIME_STEP * rate0
    for t in range(4):
        lanes = slice(128 * t, 128 * t + 128)
        geo[0, :, lanes] = ratea * geo[0, :, lanes] + rate0 * geo[1, :, lanes] + pnext * geo[2, :, lanes]

    def patterns(n, _):
        t = n // 8
        block = n - 8 * t
        after = block + 1
        if isinstance(n, int):
            lanes, store = pl.ds(128 * t, 128), 64 * block
            bit = 3 if after % 2 == 1 else (4 if after % 4 == 2 else 5)
        else:
            lanes, store = pl.ds(pl.multiple_of(128 * t, 128), 128), pl.multiple_of(64 * block, 8)
            bit = jnp.where(after % 2 == 1, 3, jnp.where(after % 4 == 2, 4, 5))
        acc = [jnp.zeros((8, 128), F32)] * 8
        for g in range(FACES_DEV // 8):
            rows = pl.ds(8 * g, 8)
            what = geo[0, rows, lanes]
            geo[0, rows, lanes] = what * sgn[bit, rows, lanes]
            parts = [what]
            for k in range(3):
                sign = sgn[k, rows, lanes]
                parts += [part * sign for part in parts]
            acc = [a + part for a, part in zip(acc, parts)]
        for k in range(8):
            binned[t, pl.ds(store + 8 * k, 8), :] = acc[k]
        return 0

    def folded(t):
        out = binned[t, pl.ds(0, BINS, stride=8), :]
        for k in range(1, 8):
            out = out + binned[t, pl.ds(k, BINS, stride=8), :]
        return out

    def acopy(half, k):
        peer = lax.rem(yz + k, N_YZ)
        return pltpu.make_async_remote_copy(
            src_ref=packed.at[half, pl.ds(pl.multiple_of(16 * peer, 16), 16), :], dst_ref=recv_a.at[half, k - 1],
            send_sem=as_sem.at[half], recv_sem=ar_sem.at[half], device_id=(gx, peer), device_id_type=MESH,
        )

    def bcopy(k):
        peer = lax.rem(gx + k, N_GX)
        return pltpu.make_async_remote_copy(
            src_ref=send_b.at[peer], dst_ref=recv_b.at[k - 1],
            send_sem=bs_sem, recv_sem=br_sem, device_id=(peer, yz), device_id_type=MESH,
        )

    def whole(ref, send_sem, recv_sem, to):
        return pltpu.make_async_remote_copy(
            src_ref=ref, dst_ref=ref, send_sem=send_sem, recv_sem=recv_sem, device_id=to, device_id_type=MESH,
        )

    awhole = [whole(recv_a.at[half], as_sem.at[half], ar_sem.at[half], high) for half in range(2)]
    bwhole = whole(recv_b, bs_sem, br_sem, right)

    def pack(half):
        had = had_v[...]
        both = jnp.concatenate([folded(2 * half), folded(2 * half + 1)], axis=0).T
        hi = both.astype(BF16)
        rest = both - hi.astype(F32)
        mid = rest.astype(BF16)
        lo = (rest - mid.astype(F32)).astype(BF16)
        packed[half] = (
            jnp.dot(hi, had, preferred_element_type=F32)
            + jnp.dot(mid, had, preferred_element_type=F32)
            + jnp.dot(lo, had, preferred_element_type=F32)
        )

    def send_half(half):
        for k in (4, 3, 5, 2, 6, 1, 7):
            acopy(half, k).start()

    mark("bins0")
    lax.fori_loop(0, 16, patterns, 0, unroll=4)
    mark("pack0")
    pack(0)
    for n in range(16, 20):
        patterns(n, 0)
    told(near_sem.at[3], ("yz", 4))
    send_half(0)
    told(near_sem.at[4], ("gx", 4))
    tell(near_sem.at[5], "gx", 8)
    mark("bins1")
    lax.fori_loop(20, 32, patterns, 0, unroll=4)
    mark("pack1")
    pack(1)
    send_half(1)

    mark("finish_a")
    def finish(x, _):
        ca, cb = table_s[0, x], table_s[1, x]
        for t in range(2):
            for h in range(2):
                lanes = pl.ds(128 * t, 128)
                ys = pl.ds(24 * h, 24)
                px, ux, vx, wx, mx = (ca * hal[f, 0, ys, lanes] + cb * hal[f, 1, ys, lanes] for f in range(5))
                p, u, v, w, m = (fld[f, x, t, pl.ds(8 + 24 * h, 24), :] for f in range(5))
                n0, n1, n2, n3 = (grd[q, x, t, ys, :] for q in range(4))
                nxt[0, x, ys, lanes] = p - TIME_STEP * (n0 + m * px + ux)
                nxt[1, x, ys, lanes] = u - TIME_STEP * (n1 + m * ux + u * mx + px)
                nxt[2, x, ys, lanes] = v - TIME_STEP * (n2 + m * vx)
                nxt[3, x, ys, lanes] = w - TIME_STEP * (n3 + m * wx)
        return 0

    def edges():
        for x, k, sign in ((0, 2, DD), (CX - 1, 3, -DD)):
            for t in range(2):
                lanes = pl.ds(128 * t, 128)
                px, ux, vx, wx, mx = ((-TIME_STEP * sign) * hal[f, k, :, lanes] for f in range(5))
                u, m = fld[1, x, t, pl.ds(8, CY), :], fld[4, x, t, pl.ds(8, CY), :]
                nxt[0, x, :, lanes] += m * px + ux
                nxt[1, x, :, lanes] += m * ux + u * mx + px
                nxt[2, x, :, lanes] += m * vx
                nxt[3, x, :, lanes] += m * wx

    lax.fori_loop(0, CX // 2, finish, 0)

    mark("wait_a")
    for half in range(2):
        awhole[half].wait_recv()
        total = packed[half, pl.ds(pl.multiple_of(16 * yz, 16), 16), :]
        for k in range(N_YZ - 1):
            total = total + recv_a[half, k]
        for g in range(N_GX):
            send_b[g, pl.ds(half, 1), :] = total[g : g + 1]
    mark("far_wait")
    told(near_sem.at[5], ("gx", 8))
    hops = lambda k: min(k // 4, 4 - k // 4) + min(k % 4, 4 - k % 4)
    for k in sorted(range(1, N_GX), key=hops, reverse=True):
        bcopy(k).start()

    mark("finish_b")
    lax.fori_loop(CX // 2, CX, finish, 0)
    edges()

    mark("wait_b")
    bwhole.wait_recv()
    total = send_b[gx]
    for k in range(N_GX - 1):
        total = total + recv_b[k]
    for h in range(2):
        for h2 in range(2):
            sig[pl.ds(2 * h + h2, 1), :] = total[h : h + 1, BINS * h2 : BINS * h2 + BINS]

    mark("drain")
    for way in range(2):
        @pl.when(sends[way])
        def _():
            for c in (all_planes[way], *all_sums[way]):
                c.wait_send()

        @pl.when(ysends[way])
        def _():
            yall[way].wait_send()
    for c in (*awhole, bwhole):
        c.wait_send()
    mark(None)


def per_device(state, mean_flow, face_cell, face_normal, face_pos, observer_pos, time_bin):
    n = np.arange(CX)
    table = np.zeros((8, 128), np.float32)
    table[0, :CX] = CC * LAM ** (n + 1.0)
    table[1, :CX] = -CC * LAM ** (CX - n * 1.0)
    table[2, 0] = DD
    table[3, CX - 1] = -DD
    dz = operator(NZ).T.astype(np.float32)
    dz_hi, dz_lo = split2(jnp.asarray(dz))
    dz = jnp.concatenate([dz_hi, dz_hi, dz_lo], axis=0)
    ends = closure(CX, CX * N_GX)
    gray = np.arange(BINS) // 8 * 8
    gray = (gray ^ (gray >> 1) & 56) + np.arange(BINS) % 8
    common = gray[:, None] & np.arange(BINS)[None, :]
    parity = sum((common >> k) & 1 for k in range(6)) % 2
    had = np.kron(np.eye(2), (1.0 - 2.0 * parity) / BINS).astype(np.float32)
    anywhere = pl.BlockSpec(memory_space=pltpu.HBM)
    vm = pltpu.VMEM
    dma = pltpu.SemaphoreType.DMA
    nxt, sig = pl.pallas_call(
        functools.partial(kernel, ends),
        out_shape=(
            vm((4, CX, CY, NZ), F32),
            vm((4, BINS), F32),
        ),
        in_specs=[anywhere] * 11,
        out_specs=(pl.BlockSpec(memory_space=pltpu.VMEM), pl.BlockSpec(memory_space=pltpu.VMEM)),
        scratch_shapes=[
            vm((5, CX, 2, 64, 128), F32),
            vm((5, CX, 2, 64, 128), F32),
            vm((3, CX, CY, NZ), F32),
            vm((5, 4, CY, NZ), F32),
            vm((2, 5, CY, NZ), F32),
            vm((7, FACES_DEV, 128), F32),
            vm((3, FACES_DEV, OBS), F32),
            vm((6, FACES_DEV, OBS), F32),
            vm((1, FACES_DEV), jnp.int32),
            vm((3, FACES_DEV), F32),
            vm((3, FACES_DEV), F32),
            vm((3, OBS), F32),
            vm((FACES_DEV, OBS), jnp.int32),
            vm((3 * NZ, NZ), BF16),
            vm((8, 128), F32),
            vm((128, 128), BF16),
            vm((16, 256), F32),
            vm((8, OBS), F32),
            vm((4, 8 * BINS, 128), F32),
            vm((2, 128, 128), F32),
            vm((2, N_YZ - 1, 16, 128), F32),
            vm((N_GX, 2, 128), F32),
            vm((N_GX - 1, 2, 128), F32),
            pltpu.SMEM((4, 128), F32),
            pltpu.SMEM((1, FACES_DEV), jnp.int32),
            dma((5, 2)), dma((10,)), dma((2, 3)), dma((2, 3)), dma((2,)), dma((2,)),
            dma((2,)), dma((2,)), dma(()), dma(()), pltpu.SemaphoreType.REGULAR((6,)),
        ],
        compiler_params=pltpu.CompilerParams(
            collective_id=0, has_side_effects=True, vmem_limit_bytes=57 * 2**20 + 2**19
        ),
    )(
        state, mean_flow, face_cell.reshape(1, FACES_DEV), face_normal, face_pos, observer_pos, time_bin,
        dz, jnp.asarray(table), jnp.asarray(table[:4]), jnp.asarray(had, BF16),
    )

    def write_out(nxt_ref, sig_ref, nxt_out, sig_out, sem):
        copies = [pltpu.make_async_copy(sig_ref, sig_out, sem.at[4])]
        copies += [pltpu.make_async_copy(nxt_ref.at[k], nxt_out.at[k], sem.at[k]) for k in range(4)]
        for c in copies:
            c.start()
        for c in copies:
            c.wait()

    return pl.pallas_call(
        write_out,
        out_shape=(
            jax.ShapeDtypeStruct((4, CX, CY, NZ), F32),
            jax.ShapeDtypeStruct((4, BINS), F32),
        ),
        in_specs=[pl.BlockSpec(memory_space=pltpu.VMEM)] * 2,
        out_specs=(anywhere, anywhere),
        scratch_shapes=[dma((5,))],
        compiler_params=pltpu.CompilerParams(vmem_limit_bytes=2**20),
    )(pltpu.with_memory_space_constraint(nxt, pltpu.VMEM), pltpu.with_memory_space_constraint(sig, pltpu.VMEM))


def solution(mesh):
    return jax.shard_map(
        per_device,
        mesh=mesh,
        in_specs=(
            P(None, "gx", "yz", None),
            P("gx", "yz", None),
            P(("gx", "yz")),
            P(None, ("gx", "yz")),
            P(None, ("gx", "yz")),
            P(),
            P(("gx", "yz"), None),
        ),
        out_specs=(P(None, "gx", "yz", None), P(("gx", "yz"), None)),
        check_vma=False,
    )
```

```python
import functools

import jax
import jax.numpy as jnp
import numpy as np
from jax import lax
from jax.experimental import pallas as pl
from jax.experimental.pallas import tpu as pltpu
from jax.sharding import PartitionSpec as P

CX, CY, NZ = 32, 48, 256
FACES_DEV, OBS, BINS = 192, 512, 64
N_GX, N_YZ = 16, 8
TIME_STEP = 0.25
INV_FOUR_PI = 1.0 / (4.0 * 3.141592653589793)
MESH = pl.DeviceIdType.MESH
F32, BF16 = jnp.float32, jnp.bfloat16

LAM = (-1.0 + np.sqrt(1.0 - 4.0 / 9.0)) / (2.0 / 3.0)
CC, DD = 25.0 / 12.0, -1.0 / 12.0
EDGE = DD / CC


def operator(n):
    a = np.eye(n)
    b = np.zeros((n, n))
    for i in range(n):
        if i == 0:
            a[0, 1] = 2.0
            b[0, :3] = (-2.5, 2.0, 0.5)
        elif i == n - 1:
            a[i, i - 1] = 2.0
            b[i, n - 3 :] = (-0.5, -2.0, 2.5)
        elif i in (1, n - 2):
            a[i, i - 1] = a[i, i + 1] = 0.25
            b[i, i + 1], b[i, i - 1] = 0.75, -0.75
        else:
            a[i, i - 1] = a[i, i + 1] = 1.0 / 3.0
            b[i, i + 1], b[i, i - 1] = 7.0 / 9.0, -7.0 / 9.0
            b[i, i + 2], b[i, i - 2] = 1.0 / 36.0, -1.0 / 36.0
    return np.linalg.solve(a, b)


def closure(n, total):
    lag = np.arange(n)[:, None] - np.arange(n)[None, :]
    inside = np.where(
        lag == 0, 0.0, np.sign(lag) * (CC * LAM ** np.abs(lag) + DD * (np.abs(lag) == 1))
    )
    rest = operator(total)[:n, :n] - inside
    factors = np.stack([CC * LAM ** (np.arange(n) + 1.0), DD * (np.arange(n) == 0)], 1)
    weights = np.linalg.lstsq(factors, rest, rcond=None)[0]
    scale = weights[:, 12] / LAM**12
    return np.concatenate([weights[:, :4] - scale[:, None] * LAM ** np.arange(4.0), scale[:, None]], 1)


def split2(x):
    hi = x.astype(BF16)
    return hi, (x - hi.astype(F32)).astype(BF16)


class Marks:
    def __init__(self):
        self.scope = None

    def __call__(self, name):
        if self.scope is not None:
            self.scope.__exit__(None, None, None)
        self.scope = None if name is None else jax.named_scope(name)
        if self.scope is not None:
            self.scope.__enter__()


def dot3(a, b):
    return (
        jnp.dot(a[0], b[0], preferred_element_type=F32)
        + jnp.dot(a[1], b[0], preferred_element_type=F32)
        + jnp.dot(a[0], b[1], preferred_element_type=F32)
    )


def kernel(
    ends, state, mean, face_cell, normal, pos, obs, tbin, dz, table, table_s_in, had,
    nxt, sig,
    fld, grd, zed, hal, tsum, stg, geo, sgn, face_v, normal_v, pos_v, obs_v, tbin_v, dz_v, table_v, had_v,
    rows_v, seen_v, binned, packed, recv_a, send_b, recv_b, table_s, cell_s,
    ld_sem, in_sem, xs_sem, xr_sem, ys_sem, yr_sem, as_sem, ar_sem, bs_sem, br_sem, near_sem,
):
    mark = Marks()
    gx = lax.axis_index("gx")
    yz = lax.axis_index("yz")

    mark("barrier")
    barrier = pltpu.get_barrier_semaphore()
    def tell(sem, along, step):
        here, count = (gx, N_GX) if along == "gx" else (yz, N_YZ)
        for sign in (1, -1):
            there = here + sign * step

            @pl.when(there < count if sign > 0 else there >= 0)
            def _():
                to = (there, yz) if along == "gx" else (gx, there)
                pl.semaphore_signal(sem, inc=1, device_id=to, device_id_type=MESH)

    def told(sem, *pairs):
        total = 0
        for along, step in pairs:
            here, count = (gx, N_GX) if along == "gx" else (yz, N_YZ)
            total = total + (here >= step).astype(jnp.int32) + (here < count - step).astype(jnp.int32)
        pl.semaphore_wait(sem, total)

    tell(barrier, "gx", 1)
    tell(barrier, "yz", 1)
    mark("start")
    order = (0, 4, 2, 3, 1)
    small = []
    for k, (s, d) in enumerate((
        (obs, obs_v), (tbin, tbin_v), (dz, dz_v), (table, table_v), (table_s_in, table_s),
        (face_cell, cell_s), (face_cell, face_v), (normal, normal_v), (pos, pos_v), (had, had_v),
    )):
        c = pltpu.make_async_copy(s, d, in_sem.at[k])
        c.start()
        small.append(c)

    loads = {}
    for f in order:
        src = mean if f == 4 else state.at[f]
        for t in range(2):
            c = pltpu.make_async_copy(
                src.at[:, :, pl.ds(128 * t, 128)], fld.at[f, :, t, pl.ds(8, CY), :], ld_sem.at[f]
            )
            c.start()
        loads[f] = pltpu.make_async_copy(src, zed.at[0], ld_sem.at[f])
    mark("barrier_wait")
    told(barrier, ("gx", 1), ("yz", 1))

    mark("issue")
    has_left, has_right = gx > 0, gx < N_GX - 1
    has_low, has_high = yz > 0, yz < N_YZ - 1
    right, left = (lax.rem(gx + 1, N_GX), yz), (lax.rem(gx + N_GX - 1, N_GX), yz)
    high, low = (gx, lax.rem(yz + 1, N_YZ)), (gx, lax.rem(yz + N_YZ - 1, N_YZ))

    def xcopy(src, dst, way, k):
        return pltpu.make_async_remote_copy(
            src_ref=src, dst_ref=dst, send_sem=xs_sem.at[way, k], recv_sem=xr_sem.at[way, k],
            device_id=(right, left)[way], device_id_type=MESH,
        )

    planes, sums = ([], []), ([], [])
    for way, plane in ((0, CX - 1), (1, 0)):
        planes[way].append(xcopy(state.at[:, plane], hal.at[pl.ds(0, 4), 2 + way], way, 0))
        planes[way].append(xcopy(mean.at[plane], hal.at[4, 2 + way], way, 0))
        for f in range(5):
            sums[way].append(xcopy(tsum.at[way, f], hal.at[f, way], way, 1 + f // 4))
    all_planes = [xcopy(tsum.at[way], hal.at[:, 2 + way], way, 0) for way in range(2)]
    all_sums = [
        (xcopy(tsum.at[way, pl.ds(0, 4)], hal.at[pl.ds(0, 4), way], way, 1), sums[way][4]) for way in range(2)
    ]
    tell(near_sem.at[0], "gx", 1)
    tell(near_sem.at[0], "yz", 1)
    sends = (has_right, has_left)
    gets = (has_left, has_right)
    for way in range(2):
        @pl.when(sends[way])
        def _():
            planes[way][0].start()
            planes[way][1].start()


    yc = ([], [])
    for k, f in enumerate((0, 2, 4)):
        for way, (first, there) in enumerate(((8 + CY - 3, 5), (8, 8 + CY))):
            yc[way].append(pltpu.make_async_remote_copy(
                src_ref=fld.at[f, :, :, pl.ds(first, 3), :], dst_ref=fld.at[f, :, :, pl.ds(there, 3), :],
                send_sem=ys_sem.at[way], recv_sem=yr_sem.at[way],
                device_id=(high, low)[way], device_id_type=MESH,
            ))
    yall = [
        pltpu.make_async_remote_copy(
            src_ref=fld.at[pl.ds(0, 3), :, :, pl.ds(row, 3), :], dst_ref=fld.at[pl.ds(0, 3), :, :, pl.ds(row, 3), :],
            send_sem=ys_sem.at[way], recv_sem=yr_sem.at[way], device_id=(high, low)[way], device_id_type=MESH,
        )
        for way, row in ((0, 5), (1, 8 + CY))
    ]
    ysends = (has_high, has_low)
    ygets = (has_low, has_high)

    def send_y(f):
        loads[f].wait()
        for way in range(2):
            @pl.when(ysends[way])
            def _():
                yc[way][f // 2].start()

    mark("observers")
    to = lax.broadcasted_iota(jnp.int32, (OBS, OBS), 1)
    source = (
        32 * (to & 15) + 4 * (lax.shift_right_logical(to, 4) & 7)
        + 2 * lax.shift_right_logical(to, 8) + (lax.shift_right_logical(to, 7) & 1)
    )
    perm = jnp.where(lax.broadcasted_iota(jnp.int32, (OBS, OBS), 0) == source, 1.0, 0.0).astype(BF16)
    small[0].wait()
    small[1].wait()
    which = jnp.dot(tbin_v[...].astype(F32).astype(BF16), perm, preferred_element_type=F32).astype(jnp.int32)
    for k in range(6):
        sgn[k] = jnp.where((which & (1 << k)) == 0, 1.0, -1.0)
    whole = obs_v[...]
    o_hi = whole.astype(BF16)
    rest = whole - o_hi.astype(F32)
    o_mid = rest.astype(BF16)
    o_lo = (rest - o_mid.astype(F32)).astype(BF16)
    seen_v[pl.ds(0, 3), :] = (
        jnp.dot(o_hi, perm, preferred_element_type=F32)
        + jnp.dot(o_mid, perm, preferred_element_type=F32)
        + jnp.dot(o_lo, perm, preferred_element_type=F32)
    )
    send_y(0)
    mark("columns")
    for c in small[3:]:
        c.wait()
    cell = face_v[...]
    line = lax.shift_right_logical(cell, 8)
    fx = lax.shift_right_logical(lax.shift_right_logical(line, 7) * 21846, 16)
    fy = line - CY * lax.shift_right_logical(lax.shift_right_logical(line, 4) * 21846, 16)
    fx = fx & (CX - 1)
    fz = cell & 255
    rows_v[...] = jnp.zeros((16, 256), F32)
    rows_v[pl.ds(0, 3), pl.ds(0, FACES_DEV)] = pos_v[...]
    rows_v[pl.ds(3, 3), pl.ds(0, FACES_DEV)] = normal_v[...]
    rows_v[pl.ds(6, 1), pl.ds(0, FACES_DEV)] = fx.astype(F32)
    rows_v[pl.ds(7, 1), pl.ds(0, FACES_DEV)] = fy.astype(F32)
    rows_v[pl.ds(8, 1), pl.ds(0, FACES_DEV)] = fz.astype(F32)
    cols = rows_v[...].T
    col = lambda k: cols[:FACES_DEV, k : k + 1]
    xcol, ycol, zcol = col(6), col(7), col(8)
    lane = lax.broadcasted_iota(jnp.int32, (FACES_DEV, 128), 1).astype(F32)
    zlane = zcol - jnp.where(zcol >= 128.0, 128.0, 0.0)
    zmask = zlane == lane
    pick = lambda a: jnp.sum(jnp.where(zmask, a, 0.0), axis=1, keepdims=True)
    xmask = xcol == lane
    coef = [
        jnp.sum(jnp.where(xmask, table_v[pl.ds(k, 1), :], 0.0), axis=1, keepdims=True) for k in range(4)
    ]
    upper = lane >= CY
    hit = jnp.where(upper, lane - CY, lane) == ycol
    weights = [
        jnp.where(hit, jnp.where(upper, coef[2 * k + 1], coef[2 * k]), 0.0) for k in range(2)
    ]
    send_y(4)
    mark("geometry")
    for t in range(4):
        lanes = slice(128 * t, 128 * t + 128)
        dx = seen_v[0:1, lanes] - col(0)
        dy_ = seen_v[1:2, lanes] - col(1)
        dz_ = seen_v[2:3, lanes] - col(2)
        inv = lax.rsqrt(dx * dx + dy_ * dy_ + dz_ * dz_)
        nr = (col(3) * dx + col(4) * dy_ + col(5) * dz_) * inv
        q1 = INV_FOUR_PI * inv
        geo[0, :, lanes] = q1
        geo[1, :, lanes] = q1 * nr
        geo[2, :, lanes] = q1 * nr * inv

    send_y(2)
    mark("sweeps")
    small[2].wait()

    def along_z(j):
        q = j // 2
        x0 = 16 * (j - 2 * q)
        f = jnp.where(q == 0, 0, q + 2)
        v = fld[f, pl.ds(x0, 16), :, pl.ds(8, CY), :]
        v = jnp.concatenate([v[:, 0], v[:, 1]], axis=-1).reshape(16 * CY, NZ)
        hi, lo = split2(v)
        out = jnp.dot(jnp.concatenate([hi, lo, hi], axis=1), dz_v[...], preferred_element_type=F32)
        zed[q, pl.ds(x0, 16)] = out.reshape(16, CY, NZ)

    jobs = 0
    for f, per_half in zip((0, 3, 2, 1, 4), (1, 1, 1, 0, 0)):
        if f not in (0, 2, 4):
            loads[f].wait()

        def sweep(t, _, f=f, per_half=per_half, jobs=jobs):
            zero = jnp.zeros((CY, 128), F32)
            at = lambda i: fld[f, i, t, pl.ds(8, CY), :] if 0 <= i < CX else zero
            up, down, v_old, w_old = zero, zero, zero, zero
            v, w = at(0), at(CX - 1)
            for i in range(CX):
                if i * per_half // CX != (i - 1) * per_half // CX:
                    along_z(jobs + per_half * t + i * per_half // CX)
                k = CX - 1 - i
                v_new, w_new = at(i + 1), at(k - 1)
                if i < CX // 2:
                    grd[f, i, t, pl.ds(0, CY), :] = up
                    grd[f, k, t, pl.ds(0, CY), :] = down
                else:
                    grd[f, i, t, pl.ds(0, CY), :] = (up - grd[f, i, t, pl.ds(0, CY), :]) + EDGE * (v_old - v_new)
                    grd[f, k, t, pl.ds(0, CY), :] = (grd[f, k, t, pl.ds(0, CY), :] - down) + EDGE * (w_new - w_old)
                up_sum, down_sum = up + v, down + w
                up, down = LAM * up_sum, LAM * down_sum
                v_old, v, w_old, w = v, v_new, w, w_new
            lanes = pl.ds(pl.multiple_of(128 * t, 128), 128)
            tsum[0, f, :, lanes] = up_sum
            tsum[1, f, :, lanes] = down_sum
            return 0

        lax.fori_loop(0, 2, sweep, 0)
        if f == 0:
            told(near_sem.at[0], ("gx", 1), ("yz", 1))
            tell(near_sem.at[1], "yz", 2)
            tell(near_sem.at[2], "gx", 2)
        jobs += 2 * per_half
        even = lax.rem(yz, 2) == 0
        for way in range(2):
            if f in (2, 1, 4):
                @pl.when(sends[way])
                def _():
                    sums[way][f].start()
            else:
                @pl.when(jnp.logical_and(sends[way], even))
                def _():
                    sums[way][f].start()
            if f == 2:
                @pl.when(jnp.logical_and(sends[way], jnp.logical_not(even)))
                def _():
                    for k in (0, 3):
                        sums[way][k].start()

    told(near_sem.at[1], ("yz", 2))
    tell(near_sem.at[3], "yz", 4)
    mark("ends")
    for way, there in ((0, jnp.logical_not(has_left)), (1, jnp.logical_not(has_right))):
        @pl.when(there)
        def _():
            def close(n, _):
                f, t = n // 2, n % 2
                lanes = pl.ds(pl.multiple_of(128 * t, 128), 128)
                far = tsum[1 - way, f, :, lanes]
                one, two = float(ends[0, 4]) * far, float(ends[1, 4]) * far
                for i in range(4):
                    v = fld[f, i if way == 0 else CX - 1 - i, t, pl.ds(8, CY), :]
                    one = one + float(ends[0, i]) * v
                    two = two + float(ends[1, i]) * v
                hal[f, way, :, lanes] = one
                hal[f, 2 + way, :, lanes] = two
                return 0

            lax.fori_loop(0, 10, close, 0)
    for way, there, row in ((0, jnp.logical_not(has_low), 5), (1, jnp.logical_not(has_high), 8 + CY)):
        @pl.when(there)
        def _():
            for f in (0, 2, 4):
                fld[f, :, :, pl.ds(row, 3), :] = jnp.zeros((CX, 2, 3, 128), F32)

    mark("wait_y")
    for way in range(2):
        @pl.when(ygets[way])
        def _():
            yall[way].wait_recv()

    mark("local")
    def local(n, _):
        for j in range(2):
            for t in range(2):
                x = 2 * n + j
                at = lambda f, s=0: fld[f, x, t, pl.ds(8 + s, CY), :]
                pz, wz, mz = (zed[q, x, :, 128 * t : 128 * t + 128] for q in range(3))

                def dy(f):
                    return (
                        0.75 * (at(f, 1) - at(f, -1)) - 0.15 * (at(f, 2) - at(f, -2))
                        + (1.0 / 60.0) * (at(f, 3) - at(f, -3))
                    )

                px, ux, vx, wx, mx = (grd[f, x, t, pl.ds(0, CY), :] for f in range(5))
                m, u, v, w = at(4), at(1), at(2), at(3)
                cm = CC * m
                grd[0, x, t, pl.ds(0, CY), :] = cm * px + CC * ux + dy(2) + wz
                grd[1, x, t, pl.ds(0, CY), :] = cm * ux + CC * (u * mx + px) + v * dy(4) + w * mz
                grd[2, x, t, pl.ds(0, CY), :] = cm * vx + dy(0)
                grd[3, x, t, pl.ds(0, CY), :] = cm * wx + pz
        return 0

    lax.fori_loop(0, CX // 2, local, 0)

    mark("gather")
    corner = gx * (CX * CY * N_YZ) + yz * CY
    grd_rows = grd.reshape(5, CX * 2 * 64, 128)
    fld_rows = fld.reshape(5, CX * 2 * 64, 128)

    def gather(n, _):
        for k in range(16):
            j = n * 16 + k
            cell = cell_s[0, j]
            line = jnp.maximum(lax.shift_right_logical(cell, 8) - corner, 0)
            x = lax.shift_right_logical(lax.shift_right_logical(line, 7) * 86, 8)
            row = line - 256 * x + (lax.shift_right_logical(cell, 1) & 64)
            for q in range(4):
                stg[q, pl.ds(j, 1), :] = grd_rows[q, pl.ds(row, 1), :]
            for q, f in ((4, 0), (5, 1), (6, 4)):
                stg[q, pl.ds(j, 1), :] = fld_rows[f, pl.ds(row + 8, 1), :]
        return 0

    lax.fori_loop(0, FACES_DEV // 16, gather, 0)

    told(near_sem.at[2], ("gx", 2))
    tell(near_sem.at[4], "gx", 4)
    mark("picks")
    face0 = [pick(stg[q]) for q in range(7)]
    fp, fu, fm = face0[4], face0[5], face0[6]
    fn = [col(3 + k) for k in range(3)]
    to0 = (fm, jnp.ones_like(fm))
    toa = (fn[0], fn[0] * fm, fn[1] * fm, fn[2] * fm, fn[0] * fu)

    def left_of(k, scales):
        out = []
        for scale in scales:
            hi, lo = split2(weights[k] * scale)
            out += [hi, lo, hi]
        return jnp.concatenate(out, axis=1)

    lefts = [(left_of(k, to0), left_of(k, toa[:4]), left_of(k, toa[4:])) for k in range(2)]

    mark("wait_x")
    for way in range(2):
        @pl.when(gets[way])
        def _():
            all_planes[way].wait_recv()

    zwide = lax.broadcasted_iota(jnp.int32, (FACES_DEV, NZ), 1).astype(F32) == zcol
    pad = jnp.zeros((128 - 2 * CY, NZ), BF16)

    def rights(k, fields):
        out = []
        for f in fields:
            hi, lo = split2(hal[f, pl.ds(2 * k, 2)].reshape(2 * CY, NZ))
            out += [hi, pad, hi, pad, lo, pad]
        return out

    def times(a, right):
        return jnp.dot(a, jnp.concatenate(right, axis=0), preferred_element_type=F32)

    def most_at_faces(k):
        right = rights(k, range(4))
        return times(lefts[k][0], right[:12]), times(lefts[k][1], right)

    add0, adda = most_at_faces(1)
    adda = adda + times(lefts[1][2], rights(1, (4,)))
    mark("wait_t")
    for way in range(2):
        @pl.when(gets[way])
        def _():
            all_sums[way][0].wait_recv()
    more0, morea = most_at_faces(0)
    add0, adda = add0 + more0, adda + morea
    mark("wait_u")
    for way in range(2):
        @pl.when(gets[way])
        def _():
            all_sums[way][1].wait_recv()
    mark("near")
    adda = adda + times(lefts[0][2], rights(0, (4,)))
    pickw = lambda a: jnp.sum(jnp.where(zwide, a, 0.0), axis=1, keepdims=True)
    rate0 = -(face0[0] + pickw(add0))
    ratea = -(col(3) * face0[1] + col(4) * face0[2] + col(5) * face0[3] + pickw(adda))
    pnext = fp + TIME_STEP * rate0
    for t in range(4):
        lanes = slice(128 * t, 128 * t + 128)
        geo[0, :, lanes] = ratea * geo[0, :, lanes] + rate0 * geo[1, :, lanes] + pnext * geo[2, :, lanes]

    def patterns(n, _):
        t = n // 8
        block = n - 8 * t
        after = block + 1
        if isinstance(n, int):
            lanes, store = pl.ds(128 * t, 128), 64 * block
            bit = 3 if after % 2 == 1 else (4 if after % 4 == 2 else 5)
        else:
            lanes, store = pl.ds(pl.multiple_of(128 * t, 128), 128), pl.multiple_of(64 * block, 8)
            bit = jnp.where(after % 2 == 1, 3, jnp.where(after % 4 == 2, 4, 5))
        acc = [jnp.zeros((8, 128), F32)] * 8
        for g in range(FACES_DEV // 8):
            rows = pl.ds(8 * g, 8)
            what = geo[0, rows, lanes]
            geo[0, rows, lanes] = what * sgn[bit, rows, lanes]
            parts = [what]
            for k in range(3):
                sign = sgn[k, rows, lanes]
                parts += [part * sign for part in parts]
            acc = [a + part for a, part in zip(acc, parts)]
        for k in range(8):
            binned[t, pl.ds(store + 8 * k, 8), :] = acc[k]
        return 0

    def folded(t):
        out = binned[t, pl.ds(0, BINS, stride=8), :]
        for k in range(1, 8):
            out = out + binned[t, pl.ds(k, BINS, stride=8), :]
        return out

    def acopy(half, k):
        peer = lax.rem(yz + k, N_YZ)
        return pltpu.make_async_remote_copy(
            src_ref=packed.at[half, pl.ds(pl.multiple_of(16 * peer, 16), 16), :], dst_ref=recv_a.at[half, k - 1],
            send_sem=as_sem.at[half], recv_sem=ar_sem.at[half], device_id=(gx, peer), device_id_type=MESH,
        )

    def bcopy(k):
        peer = lax.rem(gx + k, N_GX)
        return pltpu.make_async_remote_copy(
            src_ref=send_b.at[peer], dst_ref=recv_b.at[k - 1],
            send_sem=bs_sem, recv_sem=br_sem, device_id=(peer, yz), device_id_type=MESH,
        )

    def whole(ref, send_sem, recv_sem, to):
        return pltpu.make_async_remote_copy(
            src_ref=ref, dst_ref=ref, send_sem=send_sem, recv_sem=recv_sem, device_id=to, device_id_type=MESH,
        )

    awhole = [whole(recv_a.at[half], as_sem.at[half], ar_sem.at[half], high) for half in range(2)]
    bwhole = whole(recv_b, bs_sem, br_sem, right)

    def pack(half):
        had = had_v[...]
        both = jnp.concatenate([folded(2 * half), folded(2 * half + 1)], axis=0).T
        hi = both.astype(BF16)
        rest = both - hi.astype(F32)
        mid = rest.astype(BF16)
        lo = (rest - mid.astype(F32)).astype(BF16)
        packed[half] = (
            jnp.dot(hi, had, preferred_element_type=F32)
            + jnp.dot(mid, had, preferred_element_type=F32)
            + jnp.dot(lo, had, preferred_element_type=F32)
        )

    def send_half(half):
        for k in (4, 3, 5, 2, 6, 1, 7):
            acopy(half, k).start()

    mark("bins0")
    lax.fori_loop(0, 16, patterns, 0, unroll=4)
    mark("pack0")
    pack(0)
    for n in range(16, 20):
        patterns(n, 0)
    told(near_sem.at[3], ("yz", 4))
    send_half(0)
    told(near_sem.at[4], ("gx", 4))
    tell(near_sem.at[5], "gx", 8)
    mark("bins1")
    lax.fori_loop(20, 32, patterns, 0, unroll=4)
    mark("pack1")
    pack(1)
    send_half(1)

    mark("finish_a")
    def finish(x, _):
        ca, cb = table_s[0, x], table_s[1, x]
        for t in range(2):
            for h in range(2):
                lanes = pl.ds(128 * t, 128)
                ys = pl.ds(24 * h, 24)
                px, ux, vx, wx, mx = (ca * hal[f, 0, ys, lanes] + cb * hal[f, 1, ys, lanes] for f in range(5))
                p, u, v, w, m = (fld[f, x, t, pl.ds(8 + 24 * h, 24), :] for f in range(5))
                n0, n1, n2, n3 = (grd[q, x, t, ys, :] for q in range(4))
                nxt[0, x, ys, lanes] = p - TIME_STEP * (n0 + m * px + ux)
                nxt[1, x, ys, lanes] = u - TIME_STEP * (n1 + m * ux + u * mx + px)
                nxt[2, x, ys, lanes] = v - TIME_STEP * (n2 + m * vx)
                nxt[3, x, ys, lanes] = w - TIME_STEP * (n3 + m * wx)
        return 0

    def edges():
        for x, k, sign in ((0, 2, DD), (CX - 1, 3, -DD)):
            for t in range(2):
                lanes = pl.ds(128 * t, 128)
                px, ux, vx, wx, mx = ((-TIME_STEP * sign) * hal[f, k, :, lanes] for f in range(5))
                u, m = fld[1, x, t, pl.ds(8, CY), :], fld[4, x, t, pl.ds(8, CY), :]
                nxt[0, x, :, lanes] += m * px + ux
                nxt[1, x, :, lanes] += m * ux + u * mx + px
                nxt[2, x, :, lanes] += m * vx
                nxt[3, x, :, lanes] += m * wx

    lax.fori_loop(0, CX // 2, finish, 0)

    mark("wait_a")
    for half in range(2):
        awhole[half].wait_recv()
        total = packed[half, pl.ds(pl.multiple_of(16 * yz, 16), 16), :]
        for k in range(N_YZ - 1):
            total = total + recv_a[half, k]
        for g in range(N_GX):
            send_b[g, pl.ds(half, 1), :] = total[g : g + 1]
    mark("far_wait")
    told(near_sem.at[5], ("gx", 8))
    hops = lambda k: min(k // 4, 4 - k // 4) + min(k % 4, 4 - k % 4)
    for k in sorted(range(1, N_GX), key=hops, reverse=True):
        bcopy(k).start()

    mark("finish_b")
    lax.fori_loop(CX // 2, CX, finish, 0)
    edges()

    mark("wait_b")
    bwhole.wait_recv()
    total = send_b[gx]
    for k in range(N_GX - 1):
        total = total + recv_b[k]
    for h in range(2):
        for h2 in range(2):
            sig[pl.ds(2 * h + h2, 1), :] = total[h : h + 1, BINS * h2 : BINS * h2 + BINS]

    mark("drain")
    for way in range(2):
        @pl.when(sends[way])
        def _():
            for c in (all_planes[way], *all_sums[way]):
                c.wait_send()

        @pl.when(ysends[way])
        def _():
            yall[way].wait_send()
    for c in (*awhole, bwhole):
        c.wait_send()
    mark(None)


def per_device(state, mean_flow, face_cell, face_normal, face_pos, observer_pos, time_bin):
    n = np.arange(CX)
    table = np.zeros((8, 128), np.float32)
    table[0, :CX] = CC * LAM ** (n + 1.0)
    table[1, :CX] = -CC * LAM ** (CX - n * 1.0)
    table[2, 0] = DD
    table[3, CX - 1] = -DD
    dz = operator(NZ).T.astype(np.float32)
    dz_hi, dz_lo = split2(jnp.asarray(dz))
    dz = jnp.concatenate([dz_hi, dz_hi, dz_lo], axis=0)
    ends = closure(CX, CX * N_GX)
    gray = np.arange(BINS) // 8 * 8
    gray = (gray ^ (gray >> 1) & 56) + np.arange(BINS) % 8
    common = gray[:, None] & np.arange(BINS)[None, :]
    parity = sum((common >> k) & 1 for k in range(6)) % 2
    had = np.kron(np.eye(2), (1.0 - 2.0 * parity) / BINS).astype(np.float32)
    anywhere = pl.BlockSpec(memory_space=pltpu.HBM)
    vm = pltpu.VMEM
    dma = pltpu.SemaphoreType.DMA
    nxt, sig = pl.pallas_call(
        functools.partial(kernel, ends),
        out_shape=(
            vm((4, CX, CY, NZ), F32),
            vm((4, BINS), F32),
        ),
        in_specs=[anywhere] * 11,
        out_specs=(pl.BlockSpec(memory_space=pltpu.VMEM), pl.BlockSpec(memory_space=pltpu.VMEM)),
        scratch_shapes=[
            vm((5, CX, 2, 64, 128), F32),
            vm((5, CX, 2, 64, 128), F32),
            vm((3, CX, CY, NZ), F32),
            vm((5, 4, CY, NZ), F32),
            vm((2, 5, CY, NZ), F32),
            vm((7, FACES_DEV, 128), F32),
            vm((3, FACES_DEV, OBS), F32),
            vm((6, FACES_DEV, OBS), F32),
            vm((1, FACES_DEV), jnp.int32),
            vm((3, FACES_DEV), F32),
            vm((3, FACES_DEV), F32),
            vm((3, OBS), F32),
            vm((FACES_DEV, OBS), jnp.int32),
            vm((3 * NZ, NZ), BF16),
            vm((8, 128), F32),
            vm((128, 128), BF16),
            vm((16, 256), F32),
            vm((8, OBS), F32),
            vm((4, 8 * BINS, 128), F32),
            vm((2, 128, 128), F32),
            vm((2, N_YZ - 1, 16, 128), F32),
            vm((N_GX, 2, 128), F32),
            vm((N_GX - 1, 2, 128), F32),
            pltpu.SMEM((4, 128), F32),
            pltpu.SMEM((1, FACES_DEV), jnp.int32),
            dma((5,)), dma((10,)), dma((2, 3)), dma((2, 3)), dma((2,)), dma((2,)),
            dma((2,)), dma((2,)), dma(()), dma(()), pltpu.SemaphoreType.REGULAR((6,)),
        ],
        compiler_params=pltpu.CompilerParams(
            collective_id=0, has_side_effects=True, vmem_limit_bytes=57 * 2**20 + 2**19
        ),
    )(
        state, mean_flow, face_cell.reshape(1, FACES_DEV), face_normal, face_pos, observer_pos, time_bin,
        dz, jnp.asarray(table), jnp.asarray(table[:4]), jnp.asarray(had, BF16),
    )

    def write_out(nxt_ref, sig_ref, nxt_out, sig_out, sem):
        copies = [pltpu.make_async_copy(sig_ref, sig_out, sem.at[1])]
        copies += [pltpu.make_async_copy(nxt_ref.at[k], nxt_out.at[k], sem.at[0]) for k in range(4)]
        for c in copies:
            c.start()
        copies[0].wait()
        pltpu.make_async_copy(nxt_ref, nxt_out, sem.at[0]).wait()

    return pl.pallas_call(
        write_out,
        out_shape=(
            jax.ShapeDtypeStruct((4, CX, CY, NZ), F32),
            jax.ShapeDtypeStruct((4, BINS), F32),
        ),
        in_specs=[pl.BlockSpec(memory_space=pltpu.VMEM)] * 2,
        out_specs=(anywhere, anywhere),
        scratch_shapes=[dma((2,))],
        compiler_params=pltpu.CompilerParams(vmem_limit_bytes=2**20),
    )(pltpu.with_memory_space_constraint(nxt, pltpu.VMEM), pltpu.with_memory_space_constraint(sig, pltpu.VMEM))


def solution(mesh):
    return jax.shard_map(
        per_device,
        mesh=mesh,
        in_specs=(
            P(None, "gx", "yz", None),
            P("gx", "yz", None),
            P(("gx", "yz")),
            P(None, ("gx", "yz")),
            P(None, ("gx", "yz")),
            P(),
            P(("gx", "yz"), None),
        ),
        out_specs=(P(None, "gx", "yz", None), P(("gx", "yz"), None)),
        check_vma=False,
    )
```
